32 devices in a mesh: col: 4 (over z), row: 8 (over y, x, core).
Axes of the slice: x: 2, y: 2, z: 4, core: 2. Of those that a mesh axis runs over, the one named last changes fastest.
Arguments:
- inter_mask: int32 [4096, 65536], P('row', 'col')
- emb_user: bfloat16 [4096, 32], P(('row', 'col'))
- emb_item: bfloat16 [65536, 32], P(('col', 'row'))
- triples: int32 [4096, 3], replicated
Outputs:
- output 1: bfloat16 [4096, 32], P(('row', 'col'))
- output 2: bfloat16 [65536, 32], P(('col', 'row'))
- output 3: float32 [4096], replicated
All inputs are finite; a program needn't handle non-finite values.
Results may differ from the reference program's by a relative error of at most 0.00855594.
Values are sent between devices in bfloat16 or wider.
A program may use at most 1 GiB of HBM per device.

```python
import jax
import jax.numpy as jnp
from jax import lax

EMB = 32
LAYERS = 3
USERS = 4096
ITEMS = 65536
BATCH = 4096
ACT_MAX = 8
DENS_DIV = 256


def draw_mask(base_key):
    key_user, key_item, key_edge = jax.random.split(base_key, 3)
    user_act = jax.random.randint(key_user, (USERS, 1), 1, ACT_MAX + 1)
    item_pop = jax.random.randint(key_item, (1, ITEMS), 1, ACT_MAX + 1)
    edge_draw = jax.random.randint(key_edge, (USERS, ITEMS), 0, DENS_DIV)
    return (edge_draw < user_act * item_pop).astype(jnp.int32)


def draw_triples(base_key):
    key_user, key_pos, key_neg = jax.random.split(base_key, 3)
    user_ids = jax.random.randint(key_user, (BATCH,), 0, USERS)
    pos_ids = jax.random.randint(key_pos, (BATCH,), 0, ITEMS)
    neg_ids = jax.random.randint(key_neg, (BATCH,), 0, ITEMS)
    return jnp.stack([user_ids, pos_ids, neg_ids], axis=1).astype(jnp.int32)


def setup_inputs(seed: int = 0) -> dict:
    sub_keys = jax.random.split(jax.random.key(seed), 8)
    user_mean = jax.random.normal(sub_keys[1], (1, EMB), jnp.float32)
    user_noise = jax.random.normal(sub_keys[2], (USERS, EMB), jnp.float32)
    user_walk = jnp.cumsum(jax.random.normal(sub_keys[6], (USERS, EMB), jnp.float32), axis=0) * (USERS ** -0.5)
    item_mean = jax.random.normal(sub_keys[3], (1, EMB), jnp.float32)
    item_noise = jax.random.normal(sub_keys[4], (ITEMS, EMB), jnp.float32)
    item_walk = jnp.cumsum(jax.random.normal(sub_keys[7], (ITEMS, EMB), jnp.float32), axis=0) * (ITEMS ** -0.5)
    return {
        "inter_mask": draw_mask(sub_keys[0]),
        "emb_user": (0.5 * (user_mean + user_noise + user_walk)).astype(jnp.bfloat16),
        "emb_item": (0.5 * (item_mean + item_noise + item_walk)).astype(jnp.bfloat16),
        "triples": draw_triples(sub_keys[5]),
    }


def reference(inter_mask, emb_user, emb_item, triples):
    deg_user = jnp.maximum(jnp.sum(inter_mask, axis=1), 1).astype(jnp.float32)
    deg_item = jnp.maximum(jnp.sum(inter_mask, axis=0), 1).astype(jnp.float32)
    adj_norm = (inter_mask.astype(jnp.float32) * lax.rsqrt(deg_user)[:, None] * lax.rsqrt(deg_item)[None, :]).astype(jnp.bfloat16)

    def layer_step(carry, unused):
        cur_user, cur_item, total_user, total_item = carry
        next_user = jnp.dot(adj_norm, cur_item, preferred_element_type=jnp.float32).astype(jnp.bfloat16)
        next_item = jnp.dot(adj_norm.T, cur_user, preferred_element_type=jnp.float32).astype(jnp.bfloat16)
        new_carry = (next_user, next_item, total_user + next_user.astype(jnp.float32), total_item + next_item.astype(jnp.float32))
        return new_carry, None

    start_carry = (emb_user, emb_item, emb_user.astype(jnp.float32), emb_item.astype(jnp.float32))
    final_carry, unused_out = lax.scan(layer_step, start_carry, None, length=LAYERS)
    out_user = (final_carry[2] / (LAYERS + 1)).astype(jnp.bfloat16)
    out_item = (final_carry[3] / (LAYERS + 1)).astype(jnp.bfloat16)
    vec_user = out_user[triples[:, 0]].astype(jnp.float32)
    vec_pos = out_item[triples[:, 1]].astype(jnp.float32)
    vec_neg = out_item[triples[:, 2]].astype(jnp.float32)
    margin = jnp.sum(vec_user * vec_pos, axis=1) - jnp.sum(vec_user * vec_neg, axis=1)
    bpr_loss = jax.nn.softplus(-margin)
    return out_user, out_item, bpr_loss
```

```python
import functools

import jax
import jax.numpy as jnp
from jax import lax
from jax.experimental import pallas as pl
from jax.experimental.pallas import tpu as pltpu
from jax.sharding import PartitionSpec as P

LAYERS = 3
ROWS = 8
COLS = 4
SLOTS = 4
CHUNKS = 16
STRIP = 32
MESH_ID = pl.DeviceIdType.MESH
F32 = jnp.float32
BF16 = jnp.bfloat16

DEG = 0
UDEG = 28
AG = 31
ZAG = AG + 21
ZRS = ZAG + 9
RS_D = ZRS + 9
RS_1 = RS_D + 12
RS_2 = RS_1 + 12
OUZ = RS_2 + 6
OUR = OUZ + 3
MGZ = OUR + 7
MGR = MGZ + 3
N_SEM = MGR + 7


def nt_dot(a, b):
    return lax.dot_general(a, b, (((1,), (1,)), ((), ())), preferred_element_type=F32)


def kernel(mask_hbm, eu_ref, ei_ref, ids_ref, outu_ref, outi_ref, margin_ref,
           a_ref, mbuf, deg_own, deg_in, deg_inv, udeg_part, udeg_own, udeg_in, su_ref,
           part, d_in, r1_in, r2_in, eig, eug, pu, pu_in, tot_i, tot_u,
           items_lo, ug, u_rows, mg, mg_z, mg_zsum, mg_r,
           copy_sem, send_sem, recv_sem):
    emb, seg = ei_ref.shape
    users, block = a_ref.shape
    ush = eu_ref.shape[1]
    cw = block // CHUNKS
    dw = block // 32
    row = lax.axis_index("row")
    col = lax.axis_index("col")
    core = lax.rem(row, 2)
    quad = row // 2
    partner = row + 1 - 2 * core
    xq = quad + 1 - 2 * lax.rem(quad, 2)
    yq = lax.rem(quad + 2, 4)
    dq = 3 - quad
    x_row, y_row, d_row = 2 * xq + core, 2 * yq + core, 2 * dq + core
    chip_rows = (x_row, y_row, d_row)
    half = emb // 2
    sent = []

    def remote(src, dst, idx, **where):
        return pltpu.make_async_remote_copy(
            src_ref=src, dst_ref=dst, send_sem=send_sem.at[idx], recv_sem=recv_sem.at[idx],
            device_id=where, device_id_type=MESH_ID)

    def send(src, dst, idx, **where):
        copy = remote(src, dst, idx, **where)
        copy.start()
        sent.append(copy)

    def arrived(dst, idx):
        remote(dst, dst, idx, row=row).wait_recv()

    def mask_copy(j):
        return pltpu.make_async_copy(
            mask_hbm.at[:, pl.ds(j * cw, cw)], mbuf.at[j % SLOTS], copy_sem.at[j % SLOTS])

    for j in range(SLOTS):
        mask_copy(j).start()

    barrier = pltpu.get_barrier_semaphore()
    for k in range(1, ROWS):
        pl.semaphore_signal(barrier, inc=1, device_id={"row": lax.rem(row + k, ROWS)}, device_id_type=MESH_ID)
    for k in range(1, COLS):
        pl.semaphore_signal(barrier, inc=1, device_id={"col": lax.rem(col + k, COLS)}, device_id_type=MESH_ID)
    pl.semaphore_wait(barrier, ROWS + COLS - 2)

    def items_out(layer, src):
        for k in range(3):
            send(src, eig.at[layer, row], AG + 7 * layer + k, row=chip_rows[k])
        send(src, eig.at[layer, row], AG + 7 * layer + 3, row=partner)

    def items_forward(layer):
        for k in range(3):
            ref = eig.at[layer, chip_rows[k]]
            arrived(ref, AG + 7 * layer + k)
            send(ref, ref, AG + 7 * layer + 4 + k, row=partner)

    def items_in(layer):
        for k in range(4):
            arrived(eig.at[layer, 0], AG + 7 * layer + 3 + k)

    def users_out(layer, src):
        for k in range(1, COLS):
            send(src, eug.at[layer, col], ZAG + 3 * layer + k - 1, col=lax.rem(col + k, COLS))

    def users_in(layer):
        for k in range(COLS - 1):
            arrived(eug.at[layer, 0], ZAG + 3 * layer + k)

    eug[0, col] = eu_ref[...]
    eig[0, row] = ei_ref[...]
    users_out(0, eu_ref)
    items_out(0, ei_ref)

    udeg_part[...] = jnp.zeros_like(udeg_part)
    for j in range(CHUNKS):
        mask_copy(j).wait()

        def strip(s, acc, j=j):
            rows = pl.ds(pl.multiple_of(s * STRIP, STRIP), STRIP)
            m = mbuf[j % SLOTS, rows, :].astype(F32)
            a_ref[rows, j * cw:(j + 1) * cw] = m.astype(BF16)
            lanes = m[:, 0:128]
            for t in range(1, cw // 128):
                lanes = lanes + m[:, t * 128:(t + 1) * 128]
            udeg_part[rows, :] = udeg_part[rows, :] + lanes
            for t in range(STRIP // 8):
                acc = acc + m[t * 8:(t + 1) * 8, :]
            return acc

        acc = lax.fori_loop(0, users // STRIP, strip, jnp.zeros((8, cw), F32))
        if j + SLOTS < CHUNKS:
            mask_copy(j + SLOTS).start()
        total = jnp.sum(acc, axis=0, keepdims=True)
        deg_own[2 * j:2 * j + 1, :] = total[:, :dw]
        deg_own[2 * j + 1:2 * j + 2, :] = total[:, dw:]
        if j % 4 == 3:
            g = j // 4
            for k in range(1, ROWS):
                send(deg_own.at[pl.ds(8 * g, 8), :], deg_in.at[k, pl.ds(8 * g, 8), :],
                     DEG + 7 * g + k - 1, row=lax.rem(row + k, ROWS))
        if j == 7:
            items_forward(0)

    udeg_own[...] = nt_dot(jnp.ones((8, 128), BF16), udeg_part[...].astype(BF16))
    for k in range(1, COLS):
        send(udeg_own, udeg_in.at[k], UDEG + k - 1, col=lax.rem(col + k, COLS))
    users_in(0)
    items_in(0)
    for k in range(1, COLS):
        arrived(udeg_in.at[k], UDEG + k - 1)
    du = udeg_own[...] + udeg_in[1] + udeg_in[2] + udeg_in[3]
    su = lax.rsqrt(jnp.maximum(du, 1.0))
    for b in range(users // 128):
        wide = jnp.broadcast_to(su[0:1, b * 128:(b + 1) * 128], (128, 128))
        su_ref[b * 128:(b + 1) * 128, :] = wide.T
    for g in range(4):
        for k in range(1, ROWS):
            arrived(deg_in.at[k, pl.ds(8 * g, 8), :], DEG + 7 * g + k - 1)
    di = deg_own[...]
    for k in range(1, ROWS):
        di = di + deg_in[k]
    deg_inv[...] = lax.rsqrt(jnp.maximum(di, 1.0))

    def users_all(layer):
        return jnp.concatenate([eug[layer, c] for c in range(COLS)], axis=1)

    def seg_lanes(s, h=0, width=None):
        return pl.ds(pl.multiple_of(s * seg + h * cw, 128), width or seg)

    def item_dot(layer, s, eu_all):
        for h in range(2):
            part[layer, s, :, h * cw:(h + 1) * cw] = jnp.dot(
                eu_all, a_ref[:, seg_lanes(s, h, cw)], preferred_element_type=F32)

    def user_dot(layer, s, acc):
        return acc + nt_dot(eig[layer, s], a_ref[:, seg_lanes(s)])

    def d_copy(layer, q):
        return remote(part.at[layer, 2 * q + 1 - core], d_in.at[layer, q], RS_D + 4 * layer + q, row=partner)

    def users_reduce_out(layer, acc):
        for c in range(COLS):
            pu[layer, c] = acc[:, c * ush:(c + 1) * ush]
        for k in range(1, COLS):
            peer = lax.rem(col + k, COLS)
            send(pu.at[layer, peer], pu_in.at[layer, k], ZRS + 3 * layer + k - 1, col=peer)

    def users_reduce_in(layer):
        for k in range(1, COLS):
            arrived(pu_in.at[layer, k], ZRS + 3 * layer + k - 1)
        total = pu[layer, col] + pu_in[layer, 1] + pu_in[layer, 2] + pu_in[layer, 3]
        cur = total.astype(BF16)
        tot_u[...] = tot_u[...] + cur.astype(F32)
        if layer + 1 < LAYERS:
            eug[layer + 1, col] = cur
            users_out(layer + 1, eug.at[layer + 1, col])

    lo, hi = pl.ds(0, half), pl.ds(half, half)

    def combine(layer, q):
        s = 2 * q + core
        remote(d_in.at[layer, q], d_in.at[layer, q], RS_D + 4 * layer + q, row=row).wait_recv()
        part[layer, s] = part[layer, s] + d_in[layer, q]

    def plane_first(layer):
        base = RS_1 + 4 * layer
        combine(layer, dq)
        s = d_row
        send(part.at[layer, s, lo], r1_in.at[layer, 0], base, row=x_row)
        send(part.at[layer, s, hi], r1_in.at[layer, 2], base + 2, row=y_row)
        combine(layer, xq)
        send(part.at[layer, x_row, lo], r1_in.at[layer, 1], base + 1, row=x_row)
        combine(layer, yq)
        send(part.at[layer, y_row, hi], r1_in.at[layer, 3], base + 3, row=y_row)
        combine(layer, quad)

    def plane_second(layer):
        base = RS_1 + 4 * layer
        arrived(r1_in.at[layer, 0], base)
        part[layer, y_row, lo] = part[layer, y_row, lo] + r1_in[layer, 0]
        send(part.at[layer, y_row, lo], r2_in.at[layer, 0], RS_2 + 2 * layer, row=y_row)
        arrived(r1_in.at[layer, 2], base + 2)
        part[layer, x_row, hi] = part[layer, x_row, hi] + r1_in[layer, 2]
        send(part.at[layer, x_row, hi], r2_in.at[layer, 1], RS_2 + 2 * layer + 1, row=x_row)

    def plane_last(layer):
        base = RS_1 + 4 * layer
        arrived(r1_in.at[layer, 1], base + 1)
        arrived(r1_in.at[layer, 3], base + 3)
        arrived(r2_in.at[layer, 0], RS_2 + 2 * layer)
        arrived(r2_in.at[layer, 1], RS_2 + 2 * layer + 1)
        low = part[layer, row, lo] + r1_in[layer, 1] + r2_in[layer, 0]
        high = part[layer, row, hi] + r1_in[layer, 3] + r2_in[layer, 1]
        cur = jnp.concatenate([low, high], axis=0).astype(BF16)
        tot_i[...] = tot_i[...] + cur.astype(F32)
        if layer + 1 < LAYERS:
            eig[layer + 1, row] = cur
            items_out(layer + 1, eig.at[layer + 1, row])

    def item_product(layer):
        eu_all = users_all(layer)

        def other(q, carry):
            item_dot(layer, 2 * q + 1 - core, eu_all)
            d_copy(layer, q).start()
            return carry

        def own(q, carry):
            item_dot(layer, 2 * q + core, eu_all)
            return carry

        lax.fori_loop(0, 4, other, 0)
        lax.fori_loop(0, 4, own, 0)

    def user_product(layer):
        return lax.fori_loop(0, ROWS, lambda s, acc: user_dot(layer, s, acc), jnp.zeros((emb, users), F32))

    def normalize(s):
        for h in range(4):
            inv = deg_inv[pl.ds(4 * s + h, 1), :]

            def strip(t, carry):
                rows = pl.ds(pl.multiple_of(t * STRIP, STRIP), STRIP)
                wide = jnp.concatenate([su_ref[rows, :]] * (dw // 128), axis=1)
                cols = pl.ds(pl.multiple_of(s * seg + h * dw, 128), dw)
                a_ref[rows, cols] = a_ref[rows, cols] * (wide * inv).astype(BF16)
                return carry

            lax.fori_loop(0, users // STRIP, strip, 0)

    eu_first = users_all(0)

    def first_other(q, acc):
        s = 2 * q + 1 - core
        normalize(s)
        item_dot(0, s, eu_first)
        d_copy(0, q).start()
        return user_dot(0, s, acc)

    def first_own(q, acc):
        s = 2 * q + core
        normalize(s)
        item_dot(0, s, eu_first)
        return user_dot(0, s, acc)

    tot_u[...] = eu_ref[...].astype(F32)
    tot_i[...] = ei_ref[...].astype(F32)
    acc = lax.fori_loop(0, 4, first_other, jnp.zeros((emb, users), F32))
    acc = lax.fori_loop(0, 4, first_own, acc)
    users_reduce_out(0, acc)
    plane_first(0)
    users_reduce_in(0)
    plane_second(0)
    users_in(1)
    item_product(1)
    plane_last(0)
    plane_first(1)
    items_forward(1)
    items_in(1)
    users_reduce_out(1, user_product(1))
    plane_second(1)
    users_reduce_in(1)
    plane_last(1)
    users_in(2)
    item_product(2)
    plane_first(2)
    items_forward(2)
    items_in(2)
    users_reduce_out(2, user_product(2))
    plane_second(2)
    users_reduce_in(2)
    scale = 1.0 / (LAYERS + 1)
    out_user = (tot_u[...] * scale).astype(BF16)
    outu_ref[...] = out_user
    u_rows[row, col] = out_user
    for k in range(1, COLS):
        send(u_rows.at[row, col], u_rows.at[row, col], OUZ + k - 1, col=lax.rem(col + k, COLS))
    for k in range(1, COLS):
        arrived(u_rows.at[row, 0], OUZ + k - 1)
    for k in range(1, ROWS):
        send(u_rows.at[row], u_rows.at[row], OUR + k - 1, row=lax.rem(row + k, ROWS))
    for k in range(1, ROWS):
        arrived(u_rows.at[0], OUR + k - 1)

    n_chunks = ids_ref.shape[0] // 3
    tw = ids_ref.shape[1]

    def one_hot(ids):
        low_bits = lax.rem(ids, 128)
        same = lax.broadcasted_iota(jnp.int32, (128, tw), 0) == low_bits
        return jnp.where(same, 1.0, 0.0).astype(BF16)

    def pick(table, count, ids, first):
        hot = one_hot(ids)
        high_bits = ids // 128 - first
        acc = jnp.zeros((emb, tw), F32)
        step = min(8, count)
        for b in range(count // step):
            got = jnp.dot(table(b), hot, preferred_element_type=F32)
            for i in range(step):
                acc = acc + jnp.where(high_bits == b * step + i, got[i * emb:(i + 1) * emb, :], 0.0)
        return acc

    def pick_users(ch, carry):
        ids = ids_ref[pl.ds(ch, 1), :]
        table = lambda b: u_rows[2 * b:2 * b + 2].reshape(8 * emb, 128)
        ug[ch] = pick(table, ROWS * COLS, ids, 0)
        return carry

    lax.fori_loop(0, n_chunks, pick_users, 0)
    plane_last(2)
    out_item = (tot_i[...] * scale).astype(BF16)
    outi_ref[...] = out_item
    n_lo = seg // 128
    for b in range(n_lo):
        items_lo[b] = out_item[:, b * 128:(b + 1) * 128]
    first = (col * ROWS + row) * n_lo

    def score(ch, carry):
        pos = ids_ref[pl.ds(n_chunks + ch, 1), :]
        neg = ids_ref[pl.ds(2 * n_chunks + ch, 1), :]
        table = lambda b: items_lo[8 * b:8 * b + 8].reshape(min(8, n_lo) * emb, 128)
        vec = ug[ch]
        up = jnp.sum(vec * pick(table, n_lo, pos, first), axis=0, keepdims=True)
        down = jnp.sum(vec * pick(table, n_lo, neg, first), axis=0, keepdims=True)
        mg[pl.ds(ch, 1), :] = up - down
        return carry

    lax.fori_loop(0, n_chunks, score, 0)
    for k in range(1, COLS):
        send(mg, mg_z.at[k], MGZ + k - 1, col=lax.rem(col + k, COLS))
    for k in range(1, COLS):
        arrived(mg_z.at[k], MGZ + k - 1)
    mg_zsum[...] = mg[...] + mg_z[1] + mg_z[2] + mg_z[3]
    for k in range(1, ROWS):
        send(mg_zsum, mg_r.at[k], MGR + k - 1, row=lax.rem(row + k, ROWS))
    for k in range(1, ROWS):
        arrived(mg_r.at[k], MGR + k - 1)
    margin = mg_zsum[...]
    for k in range(1, ROWS):
        margin = margin + mg_r[k]
    margin_ref[...] = margin

    for layer in range(LAYERS):
        for q in range(4):
            d_copy(layer, q).wait_send()
    for copy in sent:
        copy.wait_send()


def solution(mesh):
    def device_body(mask_blk, user_shard, item_shard, triples):
        users, block = mask_blk.shape
        emb = user_shard.shape[1]
        ush, seg = user_shard.shape[0], item_shard.shape[0]
        batch = triples.shape[0]
        tw = batch // 8
        dw = block // 32
        ids = triples.T.reshape(3 * 8, tw)
        vmem = pl.BlockSpec(memory_space=pltpu.VMEM)
        out_u, out_i, margin = pl.pallas_call(
            kernel,
            out_shape=(
                jax.ShapeDtypeStruct((emb, ush), BF16),
                jax.ShapeDtypeStruct((emb, seg), BF16),
                jax.ShapeDtypeStruct((8, tw), F32),
            ),
            in_specs=[pl.BlockSpec(memory_space=pl.ANY), vmem, vmem, vmem],
            out_specs=(vmem, vmem, vmem),
            scratch_shapes=[
                pltpu.VMEM((users, block), BF16),
                pltpu.VMEM((SLOTS, users, block // CHUNKS), jnp.int32),
                pltpu.VMEM((32, dw), F32),
                pltpu.VMEM((ROWS, 32, dw), F32),
                pltpu.VMEM((32, dw), F32),
                pltpu.VMEM((users, 128), F32),
                pltpu.VMEM((8, users), F32),
                pltpu.VMEM((COLS, 8, users), F32),
                pltpu.VMEM((users, 128), F32),
                pltpu.VMEM((LAYERS, ROWS, emb, seg), F32),
                pltpu.VMEM((LAYERS, 4, emb, seg), F32),
                pltpu.VMEM((LAYERS, 4, emb // 2, seg), F32),
                pltpu.VMEM((LAYERS, 2, emb // 2, seg), F32),
                pltpu.VMEM((LAYERS, ROWS, emb, seg), BF16),
                pltpu.VMEM((LAYERS, COLS, emb, ush), BF16),
                pltpu.VMEM((LAYERS, COLS, emb, ush), F32),
                pltpu.VMEM((LAYERS, COLS, emb, ush), F32),
                pltpu.VMEM((emb, seg), F32),
                pltpu.VMEM((emb, ush), F32),
                pltpu.VMEM((seg // 128, emb, 128), BF16),
                pltpu.VMEM((8, emb, tw), F32),
                pltpu.VMEM((ROWS, COLS, emb, ush), BF16),
                pltpu.VMEM((8, tw), F32),
                pltpu.VMEM((COLS, 8, tw), F32),
                pltpu.VMEM((8, tw), F32),
                pltpu.VMEM((ROWS, 8, tw), F32),
                pltpu.SemaphoreType.DMA((SLOTS,)),
                pltpu.SemaphoreType.DMA((N_SEM,)),
                pltpu.SemaphoreType.DMA((N_SEM,)),
            ],
            compiler_params=pltpu.CompilerParams(
                collective_id=0, has_side_effects=True, vmem_limit_bytes=62 * 1024 * 1024),
        )(mask_blk, user_shard.T, item_shard.T, ids)
        return out_u.T, out_i.T, jax.nn.softplus(-margin.reshape(batch))

    return jax.shard_map(
        device_body,
        mesh=mesh,
        in_specs=(P("row", "col"), P(("row", "col"), None), P(("col", "row"), None), P()),
        out_specs=(P(("row", "col"), None), P(("col", "row"), None), P()),
        check_vma=False,
    )
```

```python
import functools

import jax
import jax.numpy as jnp
from jax import lax
from jax.experimental import pallas as pl
from jax.experimental.pallas import tpu as pltpu
from jax.sharding import PartitionSpec as P

LAYERS = 3
ROWS = 8
COLS = 4
SLOTS = 4
CHUNKS = 16
STRIP = 32
MESH_ID = pl.DeviceIdType.MESH
F32 = jnp.float32
BF16 = jnp.bfloat16

DEG = 0
UDEG = 28
AG = 31
ZAG = AG + 21
ZRS = ZAG + 9
RS_D = ZRS + 9
RS_1 = RS_D + 12
RS_2 = RS_1 + 12
OUZ = RS_2 + 6
OUR = OUZ + 3
MGZ = OUR + 7
MGR = MGZ + 3
N_SEM = MGR + 7


def nt_dot(a, b):
    return lax.dot_general(a, b, (((1,), (1,)), ((), ())), preferred_element_type=F32)


def kernel(mask_hbm, eu_hbm, ei_hbm, ids_hbm, outu_hbm, outi_hbm, loss_hbm,
           a_ref, mbuf, deg_own, deg_in, deg_inv, udeg_part, udeg_own, udeg_in, su_ref,
           part, d_in, r1_in, r2_in, eig, eug, pu, pu_in, tot_i, tot_u,
           items_lo, up_rows, down_rows, u_rows, mg, mg_z, mg_zsum, mg_r, ids_ref, outi_ref,
           copy_sem, in_sem, send_sem, recv_sem):
    emb, seg = tot_i.shape
    users, block = a_ref.shape
    ush = tot_u.shape[1]
    cw = block // CHUNKS
    dw = block // 32
    row = lax.axis_index("row")
    col = lax.axis_index("col")
    core = lax.rem(row, 2)
    quad = row // 2
    partner = row + 1 - 2 * core
    at_x, at_y = lax.rem(quad, 2), quad // 2
    half = emb // 2
    sent = []

    def flipped(j):
        fx, fy = lax.rem(j, 2), j // 2
        return (at_y + fy - 2 * at_y * fy) * 2 + at_x + fx - 2 * at_x * fx

    x_row, y_row = 2 * flipped(1) + core, 2 * flipped(2) + core

    def remote(src, dst, idx, **where):
        return pltpu.make_async_remote_copy(
            src_ref=src, dst_ref=dst, send_sem=send_sem.at[idx], recv_sem=recv_sem.at[idx],
            device_id=where, device_id_type=MESH_ID)

    def send(src, dst, idx, **where):
        copy = remote(src, dst, idx, **where)
        copy.start()
        sent.append(copy)

    def arrived(dst, idx):
        remote(dst, dst, idx, row=row).wait_recv()

    def mask_copy(j):
        return pltpu.make_async_copy(
            mask_hbm.at[:, pl.ds(j * cw, cw)], mbuf.at[j % SLOTS], copy_sem.at[j % SLOTS])

    small = [
        pltpu.make_async_copy(eu_hbm, eug.at[0, col], in_sem.at[0]),
        pltpu.make_async_copy(ei_hbm, eig.at[0, row], in_sem.at[1]),
        pltpu.make_async_copy(ids_hbm, ids_ref, in_sem.at[2]),
    ]
    small[0].start()
    small[1].start()
    for j in range(SLOTS):
        mask_copy(j).start()
    small[2].start()

    barrier = pltpu.get_barrier_semaphore()
    for k in range(1, ROWS):
        pl.semaphore_signal(barrier, inc=1, device_id={"row": lax.rem(row + k, ROWS)}, device_id_type=MESH_ID)
    for k in range(1, COLS):
        pl.semaphore_signal(barrier, inc=1, device_id={"col": lax.rem(col + k, COLS)}, device_id_type=MESH_ID)
    pl.semaphore_wait(barrier, ROWS + COLS - 2)

    def items_out(layer):
        src = eig.at[layer, row]
        for j in range(1, 4):
            send(src, src, AG + 7 * layer + j - 1, row=2 * flipped(j) + core)
        send(src, src, AG + 7 * layer + 3, row=partner)

    def items_from(layer, j):
        ref = eig.at[layer, 2 * flipped(j) + core]
        arrived(ref, AG + 7 * layer + j - 1)
        remote(ref, ref, AG + 7 * layer + 3 + j, row=partner).start()

    def items_from_partner(layer, j):
        arrived(eig.at[layer, 2 * flipped(j) + 1 - core], AG + 7 * layer + 3 + j)

    def users_out(layer):
        src = eug.at[layer, col]
        for k in range(1, COLS):
            send(src, src, ZAG + 3 * layer + k - 1, col=lax.rem(col + k, COLS))

    def users_in(layer):
        for k in range(COLS - 1):
            arrived(eug.at[layer, 0], ZAG + 3 * layer + k)

    small[0].wait()
    users_out(0)
    small[1].wait()
    items_out(0)
    small[2].wait()

    udeg_part[...] = jnp.zeros_like(udeg_part)
    for j in range(CHUNKS):
        mask_copy(j).wait()

        def strip(s, acc, j=j):
            rows = pl.ds(pl.multiple_of(s * STRIP, STRIP), STRIP)
            m = mbuf[j % SLOTS, rows, :].astype(F32)
            a_ref[rows, j * cw:(j + 1) * cw] = m.astype(BF16)
            lanes = m[:, 0:128]
            for t in range(1, cw // 128):
                lanes = lanes + m[:, t * 128:(t + 1) * 128]
            udeg_part[rows, :] = udeg_part[rows, :] + lanes
            for t in range(STRIP // 8):
                acc = acc + m[t * 8:(t + 1) * 8, :]
            return acc

        acc = lax.fori_loop(0, users // STRIP, strip, jnp.zeros((8, cw), F32))
        if j + SLOTS < CHUNKS:
            mask_copy(j + SLOTS).start()
        total = jnp.sum(acc, axis=0, keepdims=True)
        deg_own[2 * j:2 * j + 1, :] = total[:, :dw]
        deg_own[2 * j + 1:2 * j + 2, :] = total[:, dw:]
        if j % 4 == 3:
            g = j // 4
            for k in range(1, ROWS):
                send(deg_own.at[pl.ds(8 * g, 8), :], deg_in.at[k, pl.ds(8 * g, 8), :],
                     DEG + 7 * g + k - 1, row=lax.rem(row + k, ROWS))
        if j == 7:
            for k in range(1, 4):
                items_from(0, k)

    udeg_own[...] = nt_dot(jnp.ones((8, 128), BF16), udeg_part[...].astype(BF16))
    for k in range(1, COLS):
        send(udeg_own, udeg_in.at[k], UDEG + k - 1, col=lax.rem(col + k, COLS))
    tot_u[...] = eug[0, col].astype(F32)
    tot_i[...] = eig[0, row].astype(F32)
    users_in(0)
    for k in range(4):
        items_from_partner(0, k)
    for k in range(1, COLS):
        arrived(udeg_in.at[k], UDEG + k - 1)
    du = udeg_own[...] + udeg_in[1] + udeg_in[2] + udeg_in[3]
    su = lax.rsqrt(jnp.maximum(du, 1.0))
    for b in range(users // 128):
        wide = jnp.broadcast_to(su[0:1, b * 128:(b + 1) * 128], (128, 128))
        su_ref[b * 128:(b + 1) * 128, :] = wide.T
    for g in range(4):
        for k in range(1, ROWS):
            arrived(deg_in.at[k, pl.ds(8 * g, 8), :], DEG + 7 * g + k - 1)
    di = deg_own[...]
    for k in range(1, ROWS):
        di = di + deg_in[k]
    deg_inv[...] = lax.rsqrt(jnp.maximum(di, 1.0))

    def users_all(layer):
        return jnp.concatenate([eug[layer, c] for c in range(COLS)], axis=1)

    def seg_lanes(s, start=0, width=seg):
        return pl.ds(pl.multiple_of(s * seg + start, 128), width)

    def item_dot(layer, s, eu_all):
        for h in range(2):
            part[layer, s, :, h * cw:(h + 1) * cw] = jnp.dot(
                eu_all, a_ref[:, seg_lanes(s, h * cw, cw)], preferred_element_type=F32)

    def user_dot(layer, s, acc):
        return acc + nt_dot(eig[layer, s], a_ref[:, seg_lanes(s)])

    lo, hi = pl.ds(0, half), pl.ds(half, half)

    def d_copy(layer, i, s):
        return remote(part.at[layer, s], d_in.at[layer, i], RS_D + 4 * layer + i, row=partner)

    def x_first(layer, i, s):
        return remote(part.at[layer, s, lo], r1_in.at[layer, i // 2], RS_1 + 4 * layer + i // 2, row=x_row)

    def y_first(layer, i, s):
        return remote(part.at[layer, s, hi], r1_in.at[layer, 2 + i], RS_1 + 4 * layer + 2 + i, row=y_row)

    def plane_start(layer, i, s):
        arrived(d_in.at[layer, i], RS_D + 4 * layer + i)
        part[layer, s] = part[layer, s] + d_in[layer, i]

        @pl.when(jnp.logical_or(i == 0, i == 2))
        def _():
            x_first(layer, i, s).start()

        @pl.when(i < 2)
        def _():
            y_first(layer, i, s).start()

    def item_product(layer):
        eu_all = users_all(layer)

        def other(i, carry):
            s = 2 * flipped(3 - i) + 1 - core
            item_dot(layer, s, eu_all)
            d_copy(layer, i, s).start()
            return carry

        def own(i, carry):
            s = 2 * flipped(3 - i) + core
            item_dot(layer, s, eu_all)
            plane_start(layer, i, s)
            return carry

        lax.fori_loop(0, 4, other, 0)
        lax.fori_loop(0, 4, own, 0)

    def plane_second(layer):
        base = RS_1 + 4 * layer
        arrived(r1_in.at[layer, 0], base)
        part[layer, y_row, lo] = part[layer, y_row, lo] + r1_in[layer, 0]
        send(part.at[layer, y_row, lo], r2_in.at[layer, 0], RS_2 + 2 * layer, row=y_row)
        arrived(r1_in.at[layer, 2], base + 2)
        part[layer, x_row, hi] = part[layer, x_row, hi] + r1_in[layer, 2]
        send(part.at[layer, x_row, hi], r2_in.at[layer, 1], RS_2 + 2 * layer + 1, row=x_row)

    def plane_last(layer):
        base = RS_1 + 4 * layer
        arrived(r1_in.at[layer, 1], base + 1)
        arrived(r1_in.at[layer, 3], base + 3)
        arrived(r2_in.at[layer, 0], RS_2 + 2 * layer)
        arrived(r2_in.at[layer, 1], RS_2 + 2 * layer + 1)
        low = part[layer, row, lo] + r1_in[layer, 1] + r2_in[layer, 0]
        high = part[layer, row, hi] + r1_in[layer, 3] + r2_in[layer, 1]
        cur = jnp.concatenate([low, high], axis=0).astype(BF16)
        if layer + 1 < LAYERS:
            eig[layer + 1, row] = cur
            items_out(layer + 1)
        tot_i[...] = tot_i[...] + cur.astype(F32)

    def user_product(layer):
        def chip(j, acc):
            @pl.when(j > 0)
            def _():
                items_from(layer, j)

            acc = user_dot(layer, 2 * flipped(j) + core, acc)
            items_from_partner(layer, j)
            return user_dot(layer, 2 * flipped(j) + 1 - core, acc)

        return lax.fori_loop(0, 4, chip, jnp.zeros((emb, users), F32))

    def users_reduce_out(layer, acc):
        for c in range(COLS):
            pu[layer, c] = acc[:, c * ush:(c + 1) * ush]
        for k in range(1, COLS):
            peer = lax.rem(col + k, COLS)
            send(pu.at[layer, peer], pu_in.at[layer, k], ZRS + 3 * layer + k - 1, col=peer)

    def users_reduce_in(layer):
        for k in range(1, COLS):
            arrived(pu_in.at[layer, k], ZRS + 3 * layer + k - 1)
        total = pu[layer, col] + pu_in[layer, 1] + pu_in[layer, 2] + pu_in[layer, 3]
        cur = total.astype(BF16)
        if layer + 1 < LAYERS:
            eug[layer + 1, col] = cur
            users_out(layer + 1)
        tot_u[...] = tot_u[...] + cur.astype(F32)

    tile = 256
    eu_first = users_all(0)
    n_u = users // tile

    def first_segment(s, acc):
        acc = list(acc)
        for h in range(seg // tile):
            cols = seg_lanes(s, h * tile, tile)
            start = h * tile
            inv = deg_inv[pl.ds(s * (seg // dw) + start // dw, 1), start % dw:start % dw + tile]
            items = eig[0, s, :, start:start + tile]
            got = None
            for u in range(n_u):
                rows = slice(u * tile, (u + 1) * tile)
                wide = jnp.concatenate([su_ref[rows, :]] * (tile // 128), axis=1)
                block_a = a_ref[rows, cols] * (wide * inv).astype(BF16)
                a_ref[rows, cols] = block_a
                more = jnp.dot(eu_first[:, rows], block_a, preferred_element_type=F32)
                got = more if got is None else got + more
                acc[u] = acc[u] + nt_dot(items, block_a)
            part[0, s, :, start:start + tile] = got
        return tuple(acc)

    def first_other(i, acc):
        s = 2 * flipped(3 - i) + 1 - core
        acc = first_segment(s, acc)
        d_copy(0, i, s).start()
        return acc

    def first_own(i, acc):
        s = 2 * flipped(3 - i) + core
        acc = first_segment(s, acc)
        plane_start(0, i, s)
        return acc

    acc = tuple(jnp.zeros((emb, tile), F32) for _ in range(n_u))
    acc = lax.fori_loop(0, 4, first_other, acc)
    acc = lax.fori_loop(0, 4, first_own, acc)
    users_reduce_out(0, jnp.concatenate(acc, axis=1))
    plane_second(0)
    users_reduce_in(0)
    plane_last(0)
    users_in(1)
    item_product(1)
    users_reduce_out(1, user_product(1))
    plane_second(1)
    users_reduce_in(1)
    plane_last(1)
    users_in(2)
    item_product(2)
    users_reduce_out(2, user_product(2))
    plane_second(2)
    users_reduce_in(2)
    scale = 1.0 / (LAYERS + 1)
    u_rows[row, col] = (tot_u[...] * scale).astype(BF16)
    for k in range(1, COLS):
        send(u_rows.at[row, col], u_rows.at[row, col], OUZ + k - 1, col=lax.rem(col + k, COLS))
    out_copy = [pltpu.make_async_copy(u_rows.at[row, col], outu_hbm, in_sem.at[0])]
    out_copy[0].start()

    n_chunks = up_rows.shape[0]
    tw = up_rows.shape[2]

    def one_hot(ids):
        low_bits = lax.rem(ids, 128)
        same = lax.broadcasted_iota(jnp.int32, (128, tw), 0) == low_bits
        return jnp.where(same, 1.0, 0.0).astype(BF16)

    def pick(table, count, ids, first):
        hot = one_hot(ids)
        high_bits = ids // 128 - first
        acc = jnp.zeros((emb, tw), F32)
        step = min(8, count)
        for b in range(count // step):
            got = jnp.dot(table(b), hot, preferred_element_type=F32)
            for i in range(step):
                acc = acc + jnp.where(high_bits == b * step + i, got[i * emb:(i + 1) * emb, :], 0.0)
        return acc

    def ids_of(which, ch):
        return ids_ref[which:which + 1, pl.ds(pl.multiple_of(ch * tw, 128), tw)]

    plane_last(2)
    out_item = (tot_i[...] * scale).astype(BF16)
    outi_ref[...] = out_item
    out_copy.append(pltpu.make_async_copy(outi_ref, outi_hbm, in_sem.at[1]))
    out_copy[1].start()
    n_lo = seg // 128
    for b in range(n_lo):
        items_lo[b] = out_item[:, b * 128:(b + 1) * 128]
    first = (col * ROWS + row) * n_lo

    for k in range(1, COLS):
        arrived(u_rows.at[row, 0], OUZ + k - 1)
    for k in range(1, ROWS):
        send(u_rows.at[row], u_rows.at[row], OUR + k - 1, row=lax.rem(row + k, ROWS))

    def pick_items(ch, carry):
        table = lambda b: items_lo[8 * b:8 * b + 8].reshape(min(8, n_lo) * emb, 128)
        up_rows[ch] = pick(table, n_lo, ids_of(1, ch), first)
        down_rows[ch] = pick(table, n_lo, ids_of(2, ch), first)
        return carry

    lax.fori_loop(0, n_chunks, pick_items, 0)
    for k in range(1, ROWS):
        arrived(u_rows.at[0], OUR + k - 1)

    def score(ch, carry):
        table = lambda b: u_rows[2 * b:2 * b + 2].reshape(8 * emb, 128)
        vec = pick(table, ROWS * COLS, ids_of(0, ch), 0)
        up = jnp.sum(vec * up_rows[ch], axis=0, keepdims=True)
        down = jnp.sum(vec * down_rows[ch], axis=0, keepdims=True)
        diff = up - down
        for t in range(tw // 128):
            mg[pl.ds(ch * (tw // 128) + t, 1), :] = diff[:, t * 128:(t + 1) * 128]
        return carry

    lax.fori_loop(0, n_chunks, score, 0)
    for k in range(1, COLS):
        send(mg, mg_z.at[k], MGZ + k - 1, col=lax.rem(col + k, COLS))
    for k in range(1, COLS):
        arrived(mg_z.at[k], MGZ + k - 1)
    mg_zsum[...] = mg[...] + mg_z[1] + mg_z[2] + mg_z[3]
    for k in range(1, ROWS):
        send(mg_zsum, mg_r.at[k], MGR + k - 1, row=lax.rem(row + k, ROWS))
    for k in range(1, ROWS):
        arrived(mg_r.at[k], MGR + k - 1)
    margin = mg_zsum[...]
    for k in range(1, ROWS):
        margin = margin + mg_r[k]
    mg_z[0] = jnp.maximum(-margin, 0.0) + jnp.log1p(jnp.exp(-jnp.abs(margin)))
    out_copy.append(pltpu.make_async_copy(mg_z.at[0], loss_hbm, in_sem.at[2]))
    out_copy[2].start()

    for layer in range(LAYERS):
        for i in range(4):
            d_copy(layer, i, row).wait_send()
        for i in range(2):
            x_first(layer, 2 * i, row).wait_send()
            y_first(layer, i, row).wait_send()
        for j in range(1, 4):
            ref = eig.at[layer, row]
            remote(ref, ref, AG + 7 * layer + 3 + j, row=partner).wait_send()
    for copy in sent:
        copy.wait_send()
    for copy in out_copy:
        copy.wait()


def solution(mesh):
    def device_body(mask_blk, user_shard, item_shard, triples):
        users, block = mask_blk.shape
        emb = user_shard.shape[1]
        ush, seg = user_shard.shape[0], item_shard.shape[0]
        batch = triples.shape[0]
        tw = batch // 8
        dw = block // 32
        hbm = pl.BlockSpec(memory_space=pl.ANY)
        loss_shape = (batch // 128, 128)
        out_u, out_i, loss = pl.pallas_call(
            kernel,
            out_shape=(
                jax.ShapeDtypeStruct((emb, ush), BF16),
                jax.ShapeDtypeStruct((emb, seg), BF16),
                jax.ShapeDtypeStruct(loss_shape, F32),
            ),
            in_specs=[pl.BlockSpec(memory_space=pltpu.HBM)] * 4,
            out_specs=(hbm,) * 3,
            scratch_shapes=[
                pltpu.VMEM((users, block), BF16),
                pltpu.VMEM((SLOTS, users, block // CHUNKS), jnp.int32),
                pltpu.VMEM((32, dw), F32),
                pltpu.VMEM((ROWS, 32, dw), F32),
                pltpu.VMEM((32, dw), F32),
                pltpu.VMEM((users, 128), F32),
                pltpu.VMEM((8, users), F32),
                pltpu.VMEM((COLS, 8, users), F32),
                pltpu.VMEM((users, 128), F32),
                pltpu.VMEM((LAYERS, ROWS, emb, seg), F32),
                pltpu.VMEM((LAYERS, 4, emb, seg), F32),
                pltpu.VMEM((LAYERS, 4, emb // 2, seg), F32),
                pltpu.VMEM((LAYERS, 2, emb // 2, seg), F32),
                pltpu.VMEM((LAYERS, ROWS, emb, seg), BF16),
                pltpu.VMEM((LAYERS, COLS, emb, ush), BF16),
                pltpu.VMEM((LAYERS, COLS, emb, ush), F32),
                pltpu.VMEM((LAYERS, COLS, emb, ush), F32),
                pltpu.VMEM((emb, seg), F32),
                pltpu.VMEM((emb, ush), F32),
                pltpu.VMEM((seg // 128, emb, 128), BF16),
                pltpu.VMEM((8, emb, tw), F32),
                pltpu.VMEM((8, emb, tw), F32),
                pltpu.VMEM((ROWS, COLS, emb, ush), BF16),
                pltpu.VMEM(loss_shape, F32),
                pltpu.VMEM((COLS,) + loss_shape, F32),
                pltpu.VMEM(loss_shape, F32),
                pltpu.VMEM((ROWS,) + loss_shape, F32),
                pltpu.VMEM((3, batch), jnp.int32),
                pltpu.VMEM((emb, seg), BF16),
                pltpu.SemaphoreType.DMA((SLOTS,)),
                pltpu.SemaphoreType.DMA((3,)),
                pltpu.SemaphoreType.DMA((N_SEM,)),
                pltpu.SemaphoreType.DMA((N_SEM,)),
            ],
            compiler_params=pltpu.CompilerParams(
                collective_id=0, has_side_effects=True, vmem_limit_bytes=48 * 1024 * 1024),
        )(mask_blk, user_shard.T, item_shard.T, triples.T)
        return out_u.T, out_i.T, loss.reshape(batch)

    return jax.shard_map(
        device_body,
        mesh=mesh,
        in_specs=(P("row", "col"), P(("row", "col"), None), P(("col", "row"), None), P()),
        out_specs=(P(("row", "col"), None), P(("col", "row"), None), P()),
        check_vma=False,
    )
```

```python
import functools

import jax
import jax.numpy as jnp
from jax import lax
from jax.experimental import pallas as pl
from jax.experimental.pallas import tpu as pltpu
from jax.sharding import PartitionSpec as P

LAYERS = 3
ROWS = 8
COLS = 4
SLOTS = 4
CHUNKS = 16
STRIP = 32
EARLY = 6
GROUP = 256
MESH_ID = pl.DeviceIdType.MESH
F32 = jnp.float32
BF16 = jnp.bfloat16

DEG = 0
UDEG = 28
AG = 31
ZAG = AG + 21
ZRS = ZAG + 9
RS_D = ZRS + 9
RS_1 = RS_D + 12
RS_2 = RS_1 + 12
OUZ = RS_2 + 6
OUR = OUZ + 3
MGZ = OUR + 7
MGR = MGZ + 3
N_SEM = MGR + 7


def nt_dot(a, b):
    return lax.dot_general(a, b, (((1,), (1,)), ((), ())), preferred_element_type=F32)


def kernel(mask_hbm, eu_hbm, ei_hbm, ids_hbm, outu_hbm, outi_hbm, loss_hbm,
           a_ref, mbuf, deg_own, deg_in, deg_inv, udeg_part, udeg_own, udeg_in, su_ref,
           part, d_in, r1_in, r2_in, eig, eug, pu, pu_in, tot_i, tot_u,
           items_lo, up_rows, down_rows, u_rows, mg, mg_z, mg_zsum, mg_r, ids_ref, outi_ref, hot_ref,
           copy_sem, in_sem, send_sem, recv_sem):
    emb, seg = tot_i.shape
    users, block = a_ref.shape
    ush = tot_u.shape[1]
    cw = block // CHUNKS
    dw = block // 32
    row = lax.axis_index("row")
    col = lax.axis_index("col")
    core = lax.rem(row, 2)
    quad = row // 2
    partner = row + 1 - 2 * core
    at_x, at_y = lax.rem(quad, 2), quad // 2
    half = emb // 2
    sent = []

    def flipped(j):
        fx, fy = lax.rem(j, 2), j // 2
        return (at_y + fy - 2 * at_y * fy) * 2 + at_x + fx - 2 * at_x * fx

    x_row, y_row = 2 * flipped(1) + core, 2 * flipped(2) + core

    def remote(src, dst, idx, **where):
        return pltpu.make_async_remote_copy(
            src_ref=src, dst_ref=dst, send_sem=send_sem.at[idx], recv_sem=recv_sem.at[idx],
            device_id=where, device_id_type=MESH_ID)

    def send(src, dst, idx, **where):
        copy = remote(src, dst, idx, **where)
        copy.start()
        sent.append(copy)

    def arrived(dst, idx):
        remote(dst, dst, idx, row=row).wait_recv()

    def mask_copy(j):
        return pltpu.make_async_copy(
            mask_hbm.at[:, pl.ds(j * cw, cw)], mbuf.at[j % SLOTS], copy_sem.at[j % SLOTS])

    small = [
        pltpu.make_async_copy(eu_hbm, eug.at[0, col], in_sem.at[0]),
        pltpu.make_async_copy(ei_hbm, eig.at[0, row], in_sem.at[1]),
        pltpu.make_async_copy(ids_hbm, ids_ref, in_sem.at[2]),
    ]
    small[0].start()
    small[1].start()
    for j in range(SLOTS):
        mask_copy(j).start()
    small[2].start()

    barrier = pltpu.get_barrier_semaphore()
    for k in range(1, ROWS):
        pl.semaphore_signal(barrier, inc=1, device_id={"row": lax.rem(row + k, ROWS)}, device_id_type=MESH_ID)
    for k in range(1, COLS):
        pl.semaphore_signal(barrier, inc=1, device_id={"col": lax.rem(col + k, COLS)}, device_id_type=MESH_ID)

    def items_out(layer):
        src = eig.at[layer, row]
        for j in range(1, 4):
            send(src, src, AG + 7 * layer + j - 1, row=2 * flipped(j) + core)
        send(src, src, AG + 7 * layer + 3, row=partner)

    def items_from(layer, j):
        ref = eig.at[layer, 2 * flipped(j) + core]
        arrived(ref, AG + 7 * layer + j - 1)
        remote(ref, ref, AG + 7 * layer + 3 + j, row=partner).start()

    def items_from_partner(layer, j):
        arrived(eig.at[layer, 2 * flipped(j) + 1 - core], AG + 7 * layer + 3 + j)

    def users_out(layer):
        src = eug.at[layer, col]
        for k in range(1, COLS):
            send(src, src, ZAG + 3 * layer + k - 1, col=lax.rem(col + k, COLS))

    def users_in(layer):
        for k in range(COLS - 1):
            arrived(eug.at[layer, 0], ZAG + 3 * layer + k)

    udeg_part[...] = jnp.zeros_like(udeg_part)
    ready = {max(4 * g + 3, EARLY - 1): (g,) for g in range(4)}
    for j in range(CHUNKS):
        with jax.named_scope("mask_wait"):
            mask_copy(j).wait()

        def strip(s, acc, j=j):
            rows = pl.ds(pl.multiple_of(s * STRIP, STRIP), STRIP)
            m = mbuf[j % SLOTS, rows, :].astype(F32)
            a_ref[rows, j * cw:(j + 1) * cw] = m.astype(BF16)
            lanes = m[:, 0:128]
            for t in range(1, cw // 128):
                lanes = lanes + m[:, t * 128:(t + 1) * 128]
            udeg_part[rows, :] = udeg_part[rows, :] + lanes
            for t in range(STRIP // 8):
                acc = acc + m[t * 8:(t + 1) * 8, :]
            return acc

        acc = lax.fori_loop(0, users // STRIP, strip, jnp.zeros((8, cw), F32))
        if j + SLOTS < CHUNKS:
            mask_copy(j + SLOTS).start()
        total = jnp.sum(acc, axis=0, keepdims=True)
        deg_own[2 * j:2 * j + 1, :] = total[:, :dw]
        deg_own[2 * j + 1:2 * j + 2, :] = total[:, dw:]
        if j == EARLY - 1:
            with jax.named_scope("barrier"):
                pl.semaphore_wait(barrier, ROWS + COLS - 2)
            small[0].wait()
            users_out(0)
            small[1].wait()
            items_out(0)
        for g in ready.get(j, ()):
            for k in range(1, ROWS):
                send(deg_own.at[pl.ds(8 * g, 8), :], deg_in.at[k, pl.ds(8 * g, 8), :],
                     DEG + 7 * g + k - 1, row=lax.rem(row + k, ROWS))

    udeg_own[...] = nt_dot(jnp.ones((8, 128), BF16), udeg_part[...].astype(BF16))
    for k in range(1, COLS):
        send(udeg_own, udeg_in.at[k], UDEG + k - 1, col=lax.rem(col + k, COLS))
    tot_u[...] = eug[0, col].astype(F32)
    tot_i[...] = eig[0, row].astype(F32)
    small[2].wait()
    batch = ids_ref.shape[1]
    n_chunks, tw = up_rows.shape[0], up_rows.shape[2]

    def ids_of(which, ch):
        return ids_ref[which:which + 1, pl.ds(pl.multiple_of(ch * tw, 128), tw)]

    def make_hot(ch, carry):
        for which in range(3):
            low_bits = lax.rem(ids_of(which, ch), GROUP)
            same = lax.broadcasted_iota(jnp.int32, (GROUP, tw), 0) == low_bits
            hot_ref[which, ch] = jnp.where(same, 1.0, 0.0).astype(BF16)
        return carry

    with jax.named_scope("make_hot"):
        lax.fori_loop(0, n_chunks, make_hot, 0)
    users_in(0)
    with jax.named_scope("items0"):
        for k in range(1, 4):
            items_from(0, k)
        for k in range(4):
            items_from_partner(0, k)
    with jax.named_scope("udeg_wait"):
        for k in range(1, COLS):
            arrived(udeg_in.at[k], UDEG + k - 1)
    du = udeg_own[...] + udeg_in[1] + udeg_in[2] + udeg_in[3]
    su = lax.rsqrt(jnp.maximum(du, 1.0))
    for b in range(users // 128):
        wide = jnp.broadcast_to(su[0:1, b * 128:(b + 1) * 128], (128, 128))
        su_ref[b * 128:(b + 1) * 128, :] = wide.T
    with jax.named_scope("ideg_wait"):
        for g in range(4):
            for k in range(1, ROWS):
                arrived(deg_in.at[k, pl.ds(8 * g, 8), :], DEG + 7 * g + k - 1)
    di = deg_own[...]
    for k in range(1, ROWS):
        di = di + deg_in[k]
    deg_inv[...] = lax.rsqrt(jnp.maximum(di, 1.0))

    def users_all(layer):
        return jnp.concatenate([eug[layer, c] for c in range(COLS)], axis=1)

    def seg_lanes(s, start=0, width=seg):
        return pl.ds(pl.multiple_of(s * seg + start, 128), width)

    def item_dot(layer, s, eu_all):
        for h in range(2):
            part[layer, s, :, h * cw:(h + 1) * cw] = jnp.dot(
                eu_all, a_ref[:, seg_lanes(s, h * cw, cw)], preferred_element_type=F32)

    def user_dot(layer, s, acc):
        return acc + nt_dot(eig[layer, s], a_ref[:, seg_lanes(s)])

    lo, hi = pl.ds(0, half), pl.ds(half, half)

    def d_copy(layer, i, s):
        return remote(part.at[layer, s], d_in.at[layer, i], RS_D + 4 * layer + i, row=partner)

    def x_first(layer, i, s):
        return remote(part.at[layer, s, lo], r1_in.at[layer, i // 2], RS_1 + 4 * layer + i // 2, row=x_row)

    def y_first(layer, i, s):
        return remote(part.at[layer, s, hi], r1_in.at[layer, 2 + i], RS_1 + 4 * layer + 2 + i, row=y_row)

    def plane_start(layer, i, s):
        arrived(d_in.at[layer, i], RS_D + 4 * layer + i)
        part[layer, s] = part[layer, s] + d_in[layer, i]

        @pl.when(jnp.logical_or(i == 0, i == 2))
        def _():
            x_first(layer, i, s).start()

        @pl.when(i < 2)
        def _():
            y_first(layer, i, s).start()

    def item_product(layer):
        eu_all = users_all(layer)

        def other(i, carry):
            s = 2 * flipped(3 - i) + 1 - core
            item_dot(layer, s, eu_all)
            d_copy(layer, i, s).start()
            return carry

        def own(i, carry):
            s = 2 * flipped(3 - i) + core
            item_dot(layer, s, eu_all)
            plane_start(layer, i, s)
            return carry

        with jax.named_scope("item_other"):
            lax.fori_loop(0, 4, other, 0)
        with jax.named_scope("item_own"):
            lax.fori_loop(0, 4, own, 0)

    def plane_second(layer):
        base = RS_1 + 4 * layer
        arrived(r1_in.at[layer, 0], base)
        part[layer, y_row, lo] = part[layer, y_row, lo] + r1_in[layer, 0]
        send(part.at[layer, y_row, lo], r2_in.at[layer, 0], RS_2 + 2 * layer, row=y_row)
        arrived(r1_in.at[layer, 2], base + 2)
        part[layer, x_row, hi] = part[layer, x_row, hi] + r1_in[layer, 2]
        send(part.at[layer, x_row, hi], r2_in.at[layer, 1], RS_2 + 2 * layer + 1, row=x_row)

    def plane_last(layer):
        base = RS_1 + 4 * layer
        arrived(r1_in.at[layer, 1], base + 1)
        arrived(r1_in.at[layer, 3], base + 3)
        arrived(r2_in.at[layer, 0], RS_2 + 2 * layer)
        arrived(r2_in.at[layer, 1], RS_2 + 2 * layer + 1)
        low = part[layer, row, lo] + r1_in[layer, 1] + r2_in[layer, 0]
        high = part[layer, row, hi] + r1_in[layer, 3] + r2_in[layer, 1]
        cur = jnp.concatenate([low, high], axis=0).astype(BF16)
        if layer + 1 < LAYERS:
            eig[layer + 1, row] = cur
            items_out(layer + 1)
        tot_i[...] = tot_i[...] + cur.astype(F32)

    def user_product(layer):
        def chip(j, acc):
            @pl.when(j > 0)
            def _():
                items_from(layer, j)

            acc = user_dot(layer, 2 * flipped(j) + core, acc)
            items_from_partner(layer, j)
            return user_dot(layer, 2 * flipped(j) + 1 - core, acc)

        return lax.fori_loop(0, 4, chip, jnp.zeros((emb, users), F32))

    def users_reduce_out(layer, acc):
        for c in range(COLS):
            pu[layer, c] = acc[:, c * ush:(c + 1) * ush]
        for k in range(1, COLS):
            peer = lax.rem(col + k, COLS)
            send(pu.at[layer, peer], pu_in.at[layer, k], ZRS + 3 * layer + k - 1, col=peer)

    def users_reduce_in(layer):
        for k in range(1, COLS):
            arrived(pu_in.at[layer, k], ZRS + 3 * layer + k - 1)
        total = pu[layer, col] + pu_in[layer, 1] + pu_in[layer, 2] + pu_in[layer, 3]
        cur = total.astype(BF16)
        if layer + 1 < LAYERS:
            eug[layer + 1, col] = cur
            users_out(layer + 1)
        tot_u[...] = tot_u[...] + cur.astype(F32)

    tile = 256
    eu_first = users_all(0)
    n_u = users // tile

    def first_segment(s, acc):
        acc = list(acc)
        for h in range(seg // tile):
            cols = seg_lanes(s, h * tile, tile)
            start = h * tile
            inv = deg_inv[pl.ds(s * (seg // dw) + start // dw, 1), start % dw:start % dw + tile]
            items = eig[0, s, :, start:start + tile]
            got = None
            for u in range(n_u):
                rows = slice(u * tile, (u + 1) * tile)
                wide = jnp.concatenate([su_ref[rows, :]] * (tile // 128), axis=1)
                block_a = a_ref[rows, cols] * (wide * inv).astype(BF16)
                a_ref[rows, cols] = block_a
                more = jnp.dot(eu_first[:, rows], block_a, preferred_element_type=F32)
                got = more if got is None else got + more
                acc[u] = acc[u] + nt_dot(items, block_a)
            part[0, s, :, start:start + tile] = got
        return tuple(acc)

    def first_other(i, acc):
        s = 2 * flipped(3 - i) + 1 - core
        acc = first_segment(s, acc)
        d_copy(0, i, s).start()
        return acc

    def first_own(i, acc):
        s = 2 * flipped(3 - i) + core
        acc = first_segment(s, acc)
        plane_start(0, i, s)
        return acc

    acc = tuple(jnp.zeros((emb, tile), F32) for _ in range(n_u))
    with jax.named_scope("first_other"):
        acc = lax.fori_loop(0, 4, first_other, acc)
    with jax.named_scope("first_own"):
        acc = lax.fori_loop(0, 4, first_own, acc)
    users_reduce_out(0, jnp.concatenate(acc, axis=1))
    with jax.named_scope("plane_second0"):
        plane_second(0)
    with jax.named_scope("users_reduce_in0"):
        users_reduce_in(0)
    with jax.named_scope("plane_last0"):
        plane_last(0)
    with jax.named_scope("users_in1"):
        users_in(1)
    item_product(1)
    with jax.named_scope("user_product1"):
        users_reduce_out(1, user_product(1))
    with jax.named_scope("plane_second1"):
        plane_second(1)
    with jax.named_scope("users_reduce_in1"):
        users_reduce_in(1)
    with jax.named_scope("plane_last1"):
        plane_last(1)
    with jax.named_scope("users_in2"):
        users_in(2)
    item_product(2)
    with jax.named_scope("user_product2"):
        users_reduce_out(2, user_product(2))
    with jax.named_scope("plane_second2"):
        plane_second(2)
    with jax.named_scope("users_reduce_in2"):
        users_reduce_in(2)
    scale = 1.0 / (LAYERS + 1)
    u_rows[row, col] = (tot_u[...] * scale).astype(BF16)
    for k in range(1, COLS):
        send(u_rows.at[row, col], u_rows.at[row, col], OUZ + k - 1, col=lax.rem(col + k, COLS))
    out_copy = [pltpu.make_async_copy(u_rows.at[row, col], outu_hbm, in_sem.at[0])]
    out_copy[0].start()

    def pick(tables, which, ch, first):
        hot = hot_ref[which, ch]
        high_bits = ids_of(which, ch) // GROUP - first
        acc = jnp.zeros((emb, tw), F32)
        for b, table in enumerate(tables):
            got = jnp.dot(table(), hot, preferred_element_type=F32)
            for i in range(4):
                acc = acc + jnp.where(high_bits == b * 4 + i, got[i * emb:(i + 1) * emb, :], 0.0)
        return acc

    with jax.named_scope("plane_last2"):
        plane_last(2)
    out_item = (tot_i[...] * scale).astype(BF16)
    outi_ref[...] = out_item
    out_copy.append(pltpu.make_async_copy(outi_ref, outi_hbm, in_sem.at[1]))
    out_copy[1].start()
    n_lo = seg // GROUP
    for b in range(n_lo):
        items_lo[b] = out_item[:, b * GROUP:(b + 1) * GROUP]
    first = (col * ROWS + row) * n_lo

    with jax.named_scope("ouz_wait"):
        for k in range(1, COLS):
            arrived(u_rows.at[row, 0], OUZ + k - 1)
    for k in range(1, ROWS):
        send(u_rows.at[row], u_rows.at[row], OUR + k - 1, row=lax.rem(row + k, ROWS))

    def pick_items(ch, carry):
        tables = [lambda b=b: items_lo[4 * b:4 * b + 4].reshape(4 * emb, GROUP) for b in range(n_lo // 4)]
        up_rows[ch] = pick(tables, 1, ch, first)
        down_rows[ch] = pick(tables, 2, ch, first)
        return carry

    with jax.named_scope("pick_items"):
        lax.fori_loop(0, n_chunks, pick_items, 0)
    with jax.named_scope("our_wait"):
        for k in range(1, ROWS):
            arrived(u_rows.at[0], OUR + k - 1)

    def user_table(b):
        parts = []
        for i in range(4):
            r, c = (4 * b + i) // 2, 2 * (i % 2)
            parts.append(jnp.concatenate([u_rows[r, c], u_rows[r, c + 1]], axis=1))
        return jnp.concatenate(parts, axis=0)

    def score(ch, carry):
        tables = [lambda b=b: user_table(b) for b in range(ROWS * COLS // 8)]
        vec = pick(tables, 0, ch, 0)
        up = jnp.sum(vec * up_rows[ch], axis=0, keepdims=True)
        down = jnp.sum(vec * down_rows[ch], axis=0, keepdims=True)
        diff = up - down
        for t in range(tw // 128):
            mg[pl.ds(ch * (tw // 128) + t, 1), :] = diff[:, t * 128:(t + 1) * 128]
        return carry

    with jax.named_scope("score"):
        lax.fori_loop(0, n_chunks, score, 0)
    for k in range(1, COLS):
        send(mg, mg_z.at[k], MGZ + k - 1, col=lax.rem(col + k, COLS))
    with jax.named_scope("mgz_wait"):
        for k in range(1, COLS):
            arrived(mg_z.at[k], MGZ + k - 1)
    mg_zsum[...] = mg[...] + mg_z[1] + mg_z[2] + mg_z[3]
    for k in range(1, ROWS):
        send(mg_zsum, mg_r.at[k], MGR + k - 1, row=lax.rem(row + k, ROWS))
    with jax.named_scope("mgr_wait"):
        for k in range(1, ROWS):
            arrived(mg_r.at[k], MGR + k - 1)
    margin = mg_zsum[...]
    for k in range(1, ROWS):
        margin = margin + mg_r[k]
    mg_z[0] = jnp.maximum(-margin, 0.0) + jnp.log1p(jnp.exp(-jnp.abs(margin)))
    out_copy.append(pltpu.make_async_copy(mg_z.at[0], loss_hbm, in_sem.at[2]))
    out_copy[2].start()

    for layer in range(LAYERS):
        for i in range(4):
            d_copy(layer, i, row).wait_send()
        for i in range(2):
            x_first(layer, 2 * i, row).wait_send()
            y_first(layer, i, row).wait_send()
        for j in range(1, 4):
            ref = eig.at[layer, row]
            remote(ref, ref, AG + 7 * layer + 3 + j, row=partner).wait_send()
    for copy in sent:
        copy.wait_send()
    for copy in out_copy:
        copy.wait()


def solution(mesh):
    def device_body(mask_blk, user_shard, item_shard, triples):
        users, block = mask_blk.shape
        emb = user_shard.shape[1]
        ush, seg = user_shard.shape[0], item_shard.shape[0]
        batch = triples.shape[0]
        tw = batch // 8
        dw = block // 32
        hbm = pl.BlockSpec(memory_space=pl.ANY)
        loss_shape = (batch // 128, 128)
        out_u, out_i, loss = pl.pallas_call(
            kernel,
            out_shape=(
                jax.ShapeDtypeStruct((emb, ush), BF16),
                jax.ShapeDtypeStruct((emb, seg), BF16),
                jax.ShapeDtypeStruct(loss_shape, F32),
            ),
            in_specs=[pl.BlockSpec(memory_space=pltpu.HBM)] * 4,
            out_specs=(hbm,) * 3,
            scratch_shapes=[
                pltpu.VMEM((users, block), BF16),
                pltpu.VMEM((SLOTS, users, block // CHUNKS), jnp.int32),
                pltpu.VMEM((32, dw), F32),
                pltpu.VMEM((ROWS, 32, dw), F32),
                pltpu.VMEM((32, dw), F32),
                pltpu.VMEM((users, 128), F32),
                pltpu.VMEM((8, users), F32),
                pltpu.VMEM((COLS, 8, users), F32),
                pltpu.VMEM((users, 128), F32),
                pltpu.VMEM((LAYERS, ROWS, emb, seg), F32),
                pltpu.VMEM((LAYERS, 4, emb, seg), F32),
                pltpu.VMEM((LAYERS, 4, emb // 2, seg), F32),
                pltpu.VMEM((LAYERS, 2, emb // 2, seg), F32),
                pltpu.VMEM((LAYERS, ROWS, emb, seg), BF16),
                pltpu.VMEM((LAYERS, COLS, emb, ush), BF16),
                pltpu.VMEM((LAYERS, COLS, emb, ush), F32),
                pltpu.VMEM((LAYERS, COLS, emb, ush), F32),
                pltpu.VMEM((emb, seg), F32),
                pltpu.VMEM((emb, ush), F32),
                pltpu.VMEM((seg // GROUP, emb, GROUP), BF16),
                pltpu.VMEM((8, emb, tw), F32),
                pltpu.VMEM((8, emb, tw), F32),
                pltpu.VMEM((ROWS, COLS, emb, ush), BF16),
                pltpu.VMEM(loss_shape, F32),
                pltpu.VMEM((COLS,) + loss_shape, F32),
                pltpu.VMEM(loss_shape, F32),
                pltpu.VMEM((ROWS,) + loss_shape, F32),
                pltpu.VMEM((3, batch), jnp.int32),
                pltpu.VMEM((emb, seg), BF16),
                pltpu.VMEM((3, 8, GROUP, tw), BF16),
                pltpu.SemaphoreType.DMA((SLOTS,)),
                pltpu.SemaphoreType.DMA((3,)),
                pltpu.SemaphoreType.DMA((N_SEM,)),
                pltpu.SemaphoreType.DMA((N_SEM,)),
            ],
            compiler_params=pltpu.CompilerParams(
                collective_id=0, has_side_effects=True, vmem_limit_bytes=56 * 1024 * 1024),
        )(mask_blk, user_shard.T, item_shard.T, triples.T)
        return out_u.T, out_i.T, loss.reshape(batch)

    return jax.shard_map(
        device_body,
        mesh=mesh,
        in_specs=(P("row", "col"), P(("row", "col"), None), P(("col", "row"), None), P()),
        out_specs=(P(("row", "col"), None), P(("col", "row"), None), P()),
        check_vma=False,
    )
```

```python
import functools

import jax
import jax.numpy as jnp
from jax import lax
from jax.experimental import pallas as pl
from jax.experimental.pallas import tpu as pltpu
from jax.sharding import PartitionSpec as P

LAYERS = 3
ROWS = 8
COLS = 4
SLOTS = 4
CHUNKS = 16
STRIP = 32
EARLY = 6
GROUP = 256
OFFSET = 256.0
MESH_ID = pl.DeviceIdType.MESH
F32 = jnp.float32
BF16 = jnp.bfloat16

DEG = 0
UDEG = 28
AG = 31
ZAG = AG + 21
ZRS = ZAG + 9
RS_D = ZRS + 9
RS_1 = RS_D + 12
RS_2 = RS_1 + 12
OUZ = RS_2 + 6
OUR = OUZ + 3
MGZ = OUR + 7
MGR = MGZ + 3
N_SEM = MGR + 7


def nt_dot(a, b):
    return lax.dot_general(a, b, (((1,), (1,)), ((), ())), preferred_element_type=F32)


def kernel(mask_hbm, eu_hbm, ei_hbm, ids_hbm, outu_hbm, outi_hbm, loss_hbm,
           a_ref, mbuf, deg_own, deg_out, deg_in, deg_inv, udeg_part, udeg_own, udeg_in, su_ref,
           part, d_in, r1_in, r2_in, eig, eug, pu_acc, pu, pu_in, tot_i, tot_u,
           items_lo, up_rows, down_rows, u_rows, mg, mg_z, mg_zsum, mg_r, ids_ref, outi_ref, hot_ref,
           copy_sem, in_sem, send_sem, recv_sem):
    emb, seg = tot_i.shape
    users, block = a_ref.shape
    ush = tot_u.shape[1]
    cw = block // CHUNKS
    dw = block // 32
    row = lax.axis_index("row")
    col = lax.axis_index("col")
    core = lax.rem(row, 2)
    quad = row // 2
    partner = row + 1 - 2 * core
    at_x, at_y = lax.rem(quad, 2), quad // 2
    half = emb // 2
    sent = []

    def flipped(j):
        fx, fy = lax.rem(j, 2), j // 2
        return (at_y + fy - 2 * at_y * fy) * 2 + at_x + fx - 2 * at_x * fx

    x_row, y_row = 2 * flipped(1) + core, 2 * flipped(2) + core

    def remote(src, dst, idx, **where):
        return pltpu.make_async_remote_copy(
            src_ref=src, dst_ref=dst, send_sem=send_sem.at[idx], recv_sem=recv_sem.at[idx],
            device_id=where, device_id_type=MESH_ID)

    def send(src, dst, idx, **where):
        copy = remote(src, dst, idx, **where)
        copy.start()
        sent.append(copy)

    def arrived(dst, idx):
        remote(dst, dst, idx, row=row).wait_recv()

    def mask_copy(j):
        return pltpu.make_async_copy(
            mask_hbm.at[:, pl.ds(j * cw, cw)], mbuf.at[j % SLOTS], copy_sem.at[j % SLOTS])

    small = [
        pltpu.make_async_copy(eu_hbm, eug.at[0, col], in_sem.at[0]),
        pltpu.make_async_copy(ei_hbm, eig.at[0, row], in_sem.at[1]),
        pltpu.make_async_copy(ids_hbm, ids_ref, in_sem.at[2]),
    ]
    small[0].start()
    small[1].start()
    for j in range(SLOTS):
        mask_copy(j).start()
    small[2].start()

    barrier = pltpu.get_barrier_semaphore()
    for k in range(1, ROWS):
        pl.semaphore_signal(barrier, inc=1, device_id={"row": lax.rem(row + k, ROWS)}, device_id_type=MESH_ID)
    for k in range(1, COLS):
        pl.semaphore_signal(barrier, inc=1, device_id={"col": lax.rem(col + k, COLS)}, device_id_type=MESH_ID)

    def items_out(layer):
        src = eig.at[layer, row]
        for j in range(1, 4):
            send(src, src, AG + 7 * layer + j - 1, row=2 * flipped(j) + core)
        send(src, src, AG + 7 * layer + 3, row=partner)

    def items_from(layer, j):
        ref = eig.at[layer, 2 * flipped(j) + core]
        arrived(ref, AG + 7 * layer + j - 1)
        remote(ref, ref, AG + 7 * layer + 3 + j, row=partner).start()

    def items_from_partner(layer, j):
        arrived(eig.at[layer, 2 * flipped(j) + 1 - core], AG + 7 * layer + 3 + j)

    def users_out(layer):
        src = eug.at[layer, col]
        for k in range(1, COLS):
            send(src, src, ZAG + 3 * layer + k - 1, col=lax.rem(col + k, COLS))

    def users_in(layer):
        for k in range(COLS - 1):
            arrived(eug.at[layer, 0], ZAG + 3 * layer + k)

    udeg_part[...] = jnp.zeros_like(udeg_part)
    ready = {max(4 * g + 3, EARLY - 1): (g,) for g in range(4)}
    for j in range(CHUNKS):
        with jax.named_scope("mask_wait"):
            mask_copy(j).wait()

        def strip(s, acc, j=j):
            rows = pl.ds(pl.multiple_of(s * STRIP, STRIP), STRIP)
            m = mbuf[j % SLOTS, rows, :].astype(F32)
            a_ref[rows, j * cw:(j + 1) * cw] = m.astype(BF16)
            lanes = m[:, 0:128]
            for t in range(1, cw // 128):
                lanes = lanes + m[:, t * 128:(t + 1) * 128]
            udeg_part[rows, :] = udeg_part[rows, :] + lanes
            for t in range(STRIP // 8):
                acc = acc + m[t * 8:(t + 1) * 8, :]
            return acc

        acc = lax.fori_loop(0, users // STRIP, strip, jnp.zeros((8, cw), F32))
        if j + SLOTS < CHUNKS:
            mask_copy(j + SLOTS).start()
        total = jnp.sum(acc, axis=0, keepdims=True)
        deg_own[2 * j:2 * j + 1, :] = total[:, :dw]
        deg_own[2 * j + 1:2 * j + 2, :] = total[:, dw:]
        if j == EARLY - 1:
            with jax.named_scope("barrier"):
                pl.semaphore_wait(barrier, ROWS + COLS - 2)
            small[0].wait()
            users_out(0)
            small[1].wait()
            items_out(0)
        for g in ready.get(j, ()):
            deg_out[g] = (deg_own[8 * g:8 * g + 8, :] - OFFSET).astype(BF16)
            for k in range(1, ROWS):
                send(deg_out.at[g], deg_in.at[k, g],
                     DEG + 7 * g + k - 1, row=lax.rem(row + k, ROWS))

    udeg_own[...] = nt_dot(jnp.ones((8, 128), BF16), udeg_part[...].astype(BF16))
    for k in range(1, COLS):
        send(udeg_own, udeg_in.at[k], UDEG + k - 1, col=lax.rem(col + k, COLS))
    tot_u[...] = eug[0, col].astype(F32)
    tot_i[...] = eig[0, row].astype(F32)
    small[2].wait()
    batch = ids_ref.shape[1]
    n_chunks, tw = up_rows.shape[0], up_rows.shape[2]

    def ids_of(which, ch):
        return ids_ref[which:which + 1, pl.ds(pl.multiple_of(ch * tw, 128), tw)]

    def make_hot(ch, carry):
        for which in range(3):
            low_bits = lax.rem(ids_of(which, ch), GROUP)
            same = lax.broadcasted_iota(jnp.int32, (GROUP, tw), 0) == low_bits
            hot_ref[which, ch] = jnp.where(same, 1.0, 0.0).astype(BF16)
        return carry

    with jax.named_scope("make_hot"):
        lax.fori_loop(0, n_chunks, make_hot, 0)
    users_in(0)
    with jax.named_scope("items0"):
        for k in range(1, 4):
            items_from(0, k)
        for k in range(4):
            items_from_partner(0, k)
    with jax.named_scope("udeg_wait"):
        for k in range(1, COLS):
            arrived(udeg_in.at[k], UDEG + k - 1)
    du = udeg_own[...] + udeg_in[1] + udeg_in[2] + udeg_in[3]
    su = lax.rsqrt(jnp.maximum(du, 1.0))
    for b in range(users // 128):
        wide = jnp.broadcast_to(su[0:1, b * 128:(b + 1) * 128], (128, 128))
        su_ref[b * 128:(b + 1) * 128, :] = wide.T
    with jax.named_scope("ideg_wait"):
        for g in range(4):
            for k in range(1, ROWS):
                arrived(deg_in.at[k, g], DEG + 7 * g + k - 1)
    for g in range(4):
        di = deg_own[8 * g:8 * g + 8, :] + OFFSET * (ROWS - 1)
        for k in range(1, ROWS):
            di = di + deg_in[k, g].astype(F32)
        deg_inv[8 * g:8 * g + 8, :] = lax.rsqrt(jnp.maximum(di, 1.0))

    def users_all(layer):
        return jnp.concatenate([eug[layer, c] for c in range(COLS)], axis=1)

    def seg_lanes(s, start=0, width=seg):
        return pl.ds(pl.multiple_of(s * seg + start, 128), width)

    def item_dot(layer, s, eu_all):
        for h in range(2):
            part[layer, s, :, h * cw:(h + 1) * cw] = jnp.dot(
                eu_all, a_ref[:, seg_lanes(s, h * cw, cw)], preferred_element_type=F32)

    def user_dot(layer, s):
        pu_acc[:, 0:emb] = pu_acc[:, 0:emb] + nt_dot(a_ref[:, seg_lanes(s)], eig[layer, s])

    lo, hi = pl.ds(0, half), pl.ds(half, half)

    def d_copy(layer, i, s):
        return remote(part.at[layer, s], d_in.at[layer, i], RS_D + 4 * layer + i, row=partner)

    def x_first(layer, i, s):
        return remote(part.at[layer, s, lo], r1_in.at[layer, i // 2], RS_1 + 4 * layer + i // 2, row=x_row)

    def y_first(layer, i, s):
        return remote(part.at[layer, s, hi], r1_in.at[layer, 2 + i], RS_1 + 4 * layer + 2 + i, row=y_row)

    def plane_start(layer, i, s):
        arrived(d_in.at[layer, i], RS_D + 4 * layer + i)
        part[layer, s] = part[layer, s] + d_in[layer, i]

        @pl.when(jnp.logical_or(i == 0, i == 2))
        def _():
            x_first(layer, i, s).start()

        @pl.when(i < 2)
        def _():
            y_first(layer, i, s).start()

    def item_product(layer):
        eu_all = users_all(layer)

        def other(i, carry):
            s = 2 * flipped(3 - i) + 1 - core
            item_dot(layer, s, eu_all)
            d_copy(layer, i, s).start()
            return carry

        def own(i, carry):
            s = 2 * flipped(3 - i) + core
            item_dot(layer, s, eu_all)
            plane_start(layer, i, s)
            return carry

        with jax.named_scope("item_other"):
            lax.fori_loop(0, 4, other, 0)
        with jax.named_scope("item_own"):
            lax.fori_loop(0, 4, own, 0)

    def plane_second(layer):
        base = RS_1 + 4 * layer
        arrived(r1_in.at[layer, 0], base)
        part[layer, y_row, lo] = part[layer, y_row, lo] + r1_in[layer, 0]
        send(part.at[layer, y_row, lo], r2_in.at[layer, 0], RS_2 + 2 * layer, row=y_row)
        arrived(r1_in.at[layer, 2], base + 2)
        part[layer, x_row, hi] = part[layer, x_row, hi] + r1_in[layer, 2]
        send(part.at[layer, x_row, hi], r2_in.at[layer, 1], RS_2 + 2 * layer + 1, row=x_row)

    def plane_last(layer):
        base = RS_1 + 4 * layer
        arrived(r1_in.at[layer, 1], base + 1)
        arrived(r1_in.at[layer, 3], base + 3)
        arrived(r2_in.at[layer, 0], RS_2 + 2 * layer)
        arrived(r2_in.at[layer, 1], RS_2 + 2 * layer + 1)
        low = part[layer, row, lo] + r1_in[layer, 1] + r2_in[layer, 0]
        high = part[layer, row, hi] + r1_in[layer, 3] + r2_in[layer, 1]
        cur = jnp.concatenate([low, high], axis=0).astype(BF16)
        if layer + 1 < LAYERS:
            eig[layer + 1, row] = cur
            items_out(layer + 1)
        tot_i[...] = tot_i[...] + cur.astype(F32)

    def user_product(layer):
        def chip(j, carry):
            @pl.when(j > 0)
            def _():
                items_from(layer, j)

            user_dot(layer, 2 * flipped(j) + core)
            items_from_partner(layer, j)
            user_dot(layer, 2 * flipped(j) + 1 - core)
            return carry

        pu_acc[...] = jnp.zeros_like(pu_acc)
        lax.fori_loop(0, 4, chip, 0)

    def users_reduce_out(layer):
        for c in range(COLS):
            pu[layer, c] = pu_acc[c * ush:(c + 1) * ush, :].T[:emb, :]
        for k in range(1, COLS):
            peer = lax.rem(col + k, COLS)
            send(pu.at[layer, peer], pu_in.at[layer, k], ZRS + 3 * layer + k - 1, col=peer)

    def users_reduce_in(layer):
        for k in range(1, COLS):
            arrived(pu_in.at[layer, k], ZRS + 3 * layer + k - 1)
        total = pu[layer, col] + pu_in[layer, 1] + pu_in[layer, 2] + pu_in[layer, 3]
        cur = total.astype(BF16)
        if layer + 1 < LAYERS:
            eug[layer + 1, col] = cur
            users_out(layer + 1)
        tot_u[...] = tot_u[...] + cur.astype(F32)

    tile = 256
    eu_first = users_all(0)
    n_u = users // tile

    def first_segment(s):
        for h in range(seg // tile):
            cols = seg_lanes(s, h * tile, tile)
            start = h * tile
            inv = deg_inv[pl.ds(s * (seg // dw) + start // dw, 1), start % dw:start % dw + tile]
            items = eig[0, s, :, start:start + tile]
            got = None
            for u in range(n_u):
                rows = slice(u * tile, (u + 1) * tile)
                wide = jnp.concatenate([su_ref[rows, :]] * (tile // 128), axis=1)
                block_a = a_ref[rows, cols] * (wide * inv).astype(BF16)
                a_ref[rows, cols] = block_a
                more = jnp.dot(eu_first[:, rows], block_a, preferred_element_type=F32)
                got = more if got is None else got + more
                pu_acc[rows, 0:emb] = pu_acc[rows, 0:emb] + nt_dot(block_a, items)
            part[0, s, :, start:start + tile] = got

    def first_other(i, carry):
        s = 2 * flipped(3 - i) + 1 - core
        first_segment(s)
        d_copy(0, i, s).start()
        return carry

    def first_own(i, carry):
        s = 2 * flipped(3 - i) + core
        first_segment(s)
        plane_start(0, i, s)
        return carry

    pu_acc[...] = jnp.zeros_like(pu_acc)
    with jax.named_scope("first_other"):
        lax.fori_loop(0, 4, first_other, 0)
    with jax.named_scope("first_own"):
        lax.fori_loop(0, 4, first_own, 0)
    users_reduce_out(0)
    with jax.named_scope("plane_second0"):
        plane_second(0)
    with jax.named_scope("users_reduce_in0"):
        users_reduce_in(0)
    with jax.named_scope("plane_last0"):
        plane_last(0)
    with jax.named_scope("users_in1"):
        users_in(1)
    item_product(1)
    with jax.named_scope("user_product1"):
        user_product(1)
        users_reduce_out(1)
    with jax.named_scope("plane_second1"):
        plane_second(1)
    with jax.named_scope("users_reduce_in1"):
        users_reduce_in(1)
    with jax.named_scope("plane_last1"):
        plane_last(1)
    with jax.named_scope("users_in2"):
        users_in(2)
    item_product(2)
    with jax.named_scope("user_product2"):
        user_product(2)
        users_reduce_out(2)
    with jax.named_scope("plane_second2"):
        plane_second(2)
    with jax.named_scope("users_reduce_in2"):
        users_reduce_in(2)
    scale = 1.0 / (LAYERS + 1)
    u_rows[row, col] = (tot_u[...] * scale).astype(BF16)
    for k in range(1, COLS):
        send(u_rows.at[row, col], u_rows.at[row, col], OUZ + k - 1, col=lax.rem(col + k, COLS))
    out_copy = [pltpu.make_async_copy(u_rows.at[row, col], outu_hbm, in_sem.at[0])]
    out_copy[0].start()

    def pick(tables, which, ch, first):
        hot = hot_ref[which, ch]
        high_bits = ids_of(which, ch) // GROUP - first
        acc = jnp.zeros((emb, tw), F32)
        for b, table in enumerate(tables):
            got = jnp.dot(table(), hot, preferred_element_type=F32)
            for i in range(4):
                acc = acc + jnp.where(high_bits == b * 4 + i, got[i * emb:(i + 1) * emb, :], 0.0)
        return acc

    with jax.named_scope("plane_last2"):
        plane_last(2)
    out_item = (tot_i[...] * scale).astype(BF16)
    outi_ref[...] = out_item
    out_copy.append(pltpu.make_async_copy(outi_ref, outi_hbm, in_sem.at[1]))
    out_copy[1].start()
    n_lo = seg // GROUP
    for b in range(n_lo):
        items_lo[b] = out_item[:, b * GROUP:(b + 1) * GROUP]
    first = (col * ROWS + row) * n_lo

    with jax.named_scope("ouz_wait"):
        for k in range(1, COLS):
            arrived(u_rows.at[row, 0], OUZ + k - 1)
    for k in range(1, ROWS):
        send(u_rows.at[row], u_rows.at[row], OUR + k - 1, row=lax.rem(row + k, ROWS))

    def pick_items(ch, carry):
        tables = [lambda b=b: items_lo[4 * b:4 * b + 4].reshape(4 * emb, GROUP) for b in range(n_lo // 4)]
        up_rows[ch] = pick(tables, 1, ch, first)
        down_rows[ch] = pick(tables, 2, ch, first)
        return carry

    with jax.named_scope("pick_items"):
        lax.fori_loop(0, n_chunks, pick_items, 0)
    with jax.named_scope("our_wait"):
        for k in range(1, ROWS):
            arrived(u_rows.at[0], OUR + k - 1)

    def user_table(b):
        parts = []
        for i in range(4):
            r, c = (4 * b + i) // 2, 2 * (i % 2)
            parts.append(jnp.concatenate([u_rows[r, c], u_rows[r, c + 1]], axis=1))
        return jnp.concatenate(parts, axis=0)

    def score(ch, carry):
        tables = [lambda b=b: user_table(b) for b in range(ROWS * COLS // 8)]
        vec = pick(tables, 0, ch, 0)
        up = jnp.sum(vec * up_rows[ch], axis=0, keepdims=True)
        down = jnp.sum(vec * down_rows[ch], axis=0, keepdims=True)
        diff = up - down
        for t in range(tw // 128):
            mg[pl.ds(ch * (tw // 128) + t, 1), :] = diff[:, t * 128:(t + 1) * 128]
        return carry

    with jax.named_scope("score"):
        lax.fori_loop(0, n_chunks, score, 0)
    for k in range(1, COLS):
        send(mg, mg_z.at[k], MGZ + k - 1, col=lax.rem(col + k, COLS))
    with jax.named_scope("mgz_wait"):
        for k in range(1, COLS):
            arrived(mg_z.at[k], MGZ + k - 1)
    mg_zsum[...] = mg[...] + mg_z[1] + mg_z[2] + mg_z[3]
    for k in range(1, ROWS):
        send(mg_zsum, mg_r.at[k], MGR + k - 1, row=lax.rem(row + k, ROWS))
    with jax.named_scope("mgr_wait"):
        for k in range(1, ROWS):
            arrived(mg_r.at[k], MGR + k - 1)
    margin = mg_zsum[...]
    for k in range(1, ROWS):
        margin = margin + mg_r[k]
    mg_z[0] = jnp.maximum(-margin, 0.0) + jnp.log1p(jnp.exp(-jnp.abs(margin)))
    out_copy.append(pltpu.make_async_copy(mg_z.at[0], loss_hbm, in_sem.at[2]))
    out_copy[2].start()

    for layer in range(LAYERS):
        for i in range(4):
            d_copy(layer, i, row).wait_send()
        for i in range(2):
            x_first(layer, 2 * i, row).wait_send()
            y_first(layer, i, row).wait_send()
        for j in range(1, 4):
            ref = eig.at[layer, row]
            remote(ref, ref, AG + 7 * layer + 3 + j, row=partner).wait_send()
    for copy in sent:
        copy.wait_send()
    for copy in out_copy:
        copy.wait()


def solution(mesh):
    def device_body(mask_blk, user_shard, item_shard, triples):
        users, block = mask_blk.shape
        assert users <= 2 * OFFSET and block <= 128 * 256
        emb = user_shard.shape[1]
        ush, seg = user_shard.shape[0], item_shard.shape[0]
        batch = triples.shape[0]
        tw = batch // 8
        dw = block // 32
        hbm = pl.BlockSpec(memory_space=pl.ANY)
        loss_shape = (batch // 128, 128)
        out_u, out_i, loss = pl.pallas_call(
            kernel,
            out_shape=(
                jax.ShapeDtypeStruct((emb, ush), BF16),
                jax.ShapeDtypeStruct((emb, seg), BF16),
                jax.ShapeDtypeStruct(loss_shape, F32),
            ),
            in_specs=[pl.BlockSpec(memory_space=pltpu.HBM)] * 4,
            out_specs=(hbm,) * 3,
            scratch_shapes=[
                pltpu.VMEM((users, block), BF16),
                pltpu.VMEM((SLOTS, users, block // CHUNKS), jnp.int32),
                pltpu.VMEM((32, dw), F32),
                pltpu.VMEM((4, 8, dw), BF16),
                pltpu.VMEM((ROWS, 4, 8, dw), BF16),
                pltpu.VMEM((32, dw), F32),
                pltpu.VMEM((users, 128), F32),
                pltpu.VMEM((8, users), F32),
                pltpu.VMEM((COLS, 8, users), F32),
                pltpu.VMEM((users, 128), F32),
                pltpu.VMEM((LAYERS, ROWS, emb, seg), F32),
                pltpu.VMEM((LAYERS, 4, emb, seg), F32),
                pltpu.VMEM((LAYERS, 4, emb // 2, seg), F32),
                pltpu.VMEM((LAYERS, 2, emb // 2, seg), F32),
                pltpu.VMEM((LAYERS, ROWS, emb, seg), BF16),
                pltpu.VMEM((LAYERS, COLS, emb, ush), BF16),
                pltpu.VMEM((users, 128), F32),
                pltpu.VMEM((LAYERS, COLS, emb, ush), F32),
                pltpu.VMEM((LAYERS, COLS, emb, ush), F32),
                pltpu.VMEM((emb, seg), F32),
                pltpu.VMEM((emb, ush), F32),
                pltpu.VMEM((seg // GROUP, emb, GROUP), BF16),
                pltpu.VMEM((8, emb, tw), F32),
                pltpu.VMEM((8, emb, tw), F32),
                pltpu.VMEM((ROWS, COLS, emb, ush), BF16),
                pltpu.VMEM(loss_shape, F32),
                pltpu.VMEM((COLS,) + loss_shape, F32),
                pltpu.VMEM(loss_shape, F32),
                pltpu.VMEM((ROWS,) + loss_shape, F32),
                pltpu.VMEM((3, batch), jnp.int32),
                pltpu.VMEM((emb, seg), BF16),
                pltpu.VMEM((3, 8, GROUP, tw), BF16),
                pltpu.SemaphoreType.DMA((SLOTS,)),
                pltpu.SemaphoreType.DMA((3,)),
                pltpu.SemaphoreType.DMA((N_SEM,)),
                pltpu.SemaphoreType.DMA((N_SEM,)),
            ],
            compiler_params=pltpu.CompilerParams(
                collective_id=0, has_side_effects=True, vmem_limit_bytes=56 * 1024 * 1024),
        )(mask_blk, user_shard.T, item_shard.T, triples.T)
        return out_u.T, out_i.T, loss.reshape(batch)

    return jax.shard_map(
        device_body,
        mesh=mesh,
        in_specs=(P("row", "col"), P(("row", "col"), None), P(("col", "row"), None), P()),
        out_specs=(P(("row", "col"), None), P(("col", "row"), None), P()),
        check_vma=False,
    )
```

```python
import functools

import jax
import jax.numpy as jnp
from jax import lax
from jax.experimental import pallas as pl
from jax.experimental.pallas import tpu as pltpu
from jax.sharding import PartitionSpec as P

LAYERS = 3
ROWS = 8
COLS = 4
SLOTS = 4
CHUNKS = 16
STRIP = 32
EARLY = 6
GROUP = 256
OFFSET = 256.0
MESH_ID = pl.DeviceIdType.MESH
F32 = jnp.float32
BF16 = jnp.bfloat16

DEG = 0
UDEG = 28
AG = 31
ZAG = AG + 21
ZRS = ZAG + 9
RS_D = ZRS + 9
RS_1 = RS_D + 12
RS_2 = RS_1 + 12
OUZ = RS_2 + 6
OUR = OUZ + 3
MGZ = OUR + 7
MGR = MGZ + 3
N_SEM = MGR + 7


def nt_dot(a, b):
    return lax.dot_general(a, b, (((1,), (1,)), ((), ())), preferred_element_type=F32)


def kernel(mask_hbm, eu_hbm, ei_hbm, ids_hbm, outu_hbm, outi_hbm, loss_hbm,
           a_ref, mbuf, deg_own, deg_out, deg_in, deg_inv, udeg_part, udeg_own, udeg_in, su_ref,
           part, d_in, r1_in, r2_in, eig, eug, pu_acc, pu, pu_in, tot_i, tot_u,
           items_lo, up_rows, down_rows, u_rows, mg, mg_z, mg_zsum, mg_r, ids_ref, outi_ref, hot_ref,
           copy_sem, in_sem, send_sem, recv_sem):
    emb, seg = tot_i.shape
    users, block = a_ref.shape
    ush = tot_u.shape[1]
    cw = block // CHUNKS
    dw = block // 32
    row = lax.axis_index("row")
    col = lax.axis_index("col")
    core = lax.rem(row, 2)
    quad = row // 2
    partner = row + 1 - 2 * core
    at_x, at_y = lax.rem(quad, 2), quad // 2
    half = emb // 2
    sent = []

    def flipped(j):
        fx, fy = lax.rem(j, 2), j // 2
        return (at_y + fy - 2 * at_y * fy) * 2 + at_x + fx - 2 * at_x * fx

    x_row, y_row = 2 * flipped(1) + core, 2 * flipped(2) + core

    def remote(src, dst, idx, **where):
        return pltpu.make_async_remote_copy(
            src_ref=src, dst_ref=dst, send_sem=send_sem.at[idx], recv_sem=recv_sem.at[idx],
            device_id=where, device_id_type=MESH_ID)

    def send(src, dst, idx, **where):
        copy = remote(src, dst, idx, **where)
        copy.start()
        sent.append(copy)

    def arrived(dst, idx):
        remote(dst, dst, idx, row=row).wait_recv()

    def mask_copy(j):
        return pltpu.make_async_copy(
            mask_hbm.at[:, pl.ds(j * cw, cw)], mbuf.at[j % SLOTS], copy_sem.at[j % SLOTS])

    small = [
        pltpu.make_async_copy(eu_hbm, eug.at[0, col], in_sem.at[0]),
        pltpu.make_async_copy(ei_hbm, eig.at[0, row], in_sem.at[1]),
        pltpu.make_async_copy(ids_hbm, ids_ref, in_sem.at[2]),
    ]
    small[0].start()
    small[1].start()
    for j in range(SLOTS):
        mask_copy(j).start()
    small[2].start()

    barrier = pltpu.get_barrier_semaphore()
    for k in range(1, ROWS):
        pl.semaphore_signal(barrier, inc=1, device_id={"row": lax.rem(row + k, ROWS)}, device_id_type=MESH_ID)
    for k in range(1, COLS):
        pl.semaphore_signal(barrier, inc=1, device_id={"col": lax.rem(col + k, COLS)}, device_id_type=MESH_ID)

    def items_out(layer):
        src = eig.at[layer, row]
        for j in range(1, 4):
            send(src, src, AG + 7 * layer + j - 1, row=2 * flipped(j) + core)
        send(src, src, AG + 7 * layer + 3, row=partner)

    def items_from(layer, j):
        ref = eig.at[layer, 2 * flipped(j) + core]
        arrived(ref, AG + 7 * layer + j - 1)
        remote(ref, ref, AG + 7 * layer + 3 + j, row=partner).start()

    def items_from_partner(layer, j):
        arrived(eig.at[layer, 2 * flipped(j) + 1 - core], AG + 7 * layer + 3 + j)

    def users_out(layer):
        src = eug.at[layer, col]
        for k in range(1, COLS):
            send(src, src, ZAG + 3 * layer + k - 1, col=lax.rem(col + k, COLS))

    def users_in(layer):
        for k in range(COLS - 1):
            arrived(eug.at[layer, 0], ZAG + 3 * layer + k)

    udeg_part[...] = jnp.zeros_like(udeg_part)
    udeg_own[...] = jnp.zeros_like(udeg_own)
    ready = {max(4 * g + 3, EARLY - 1): (g,) for g in range(4)}
    for j in range(CHUNKS):
        with jax.named_scope("mask_wait"):
            mask_copy(j).wait()

        def strip(s, acc, j=j):
            rows = pl.ds(pl.multiple_of(s * STRIP, STRIP), STRIP)
            m = mbuf[j % SLOTS, rows, :].astype(F32)
            a_ref[rows, j * cw:(j + 1) * cw] = m.astype(BF16)
            lanes = m[:, 0:128]
            for t in range(1, cw // 128):
                lanes = lanes + m[:, t * 128:(t + 1) * 128]
            udeg_part[rows, :] = udeg_part[rows, :] + lanes
            for t in range(STRIP // 8):
                acc = acc + m[t * 8:(t + 1) * 8, :]
            return acc

        acc = lax.fori_loop(0, users // STRIP, strip, jnp.zeros((8, cw), F32))
        if j + SLOTS < CHUNKS:
            mask_copy(j + SLOTS).start()
        total = jnp.sum(acc, axis=0, keepdims=True)
        deg_own[2 * j:2 * j + 1, :] = total[:, :dw]
        deg_own[2 * j + 1:2 * j + 2, :] = total[:, dw:]
        if j == EARLY - 1:
            with jax.named_scope("barrier"):
                pl.semaphore_wait(barrier, ROWS + COLS - 2)
            small[0].wait()
            users_out(0)
            small[1].wait()
            items_out(0)
        for g in ready.get(j, ()):
            deg_out[g] = (deg_own[8 * g:8 * g + 8, :] - OFFSET).astype(BF16)
            for k in range(1, ROWS):
                send(deg_out.at[g], deg_in.at[k, g],
                     DEG + 7 * g + k - 1, row=lax.rem(row + k, ROWS))

    counts = nt_dot(jnp.ones((8, 128), BF16), udeg_part[...].astype(BF16))
    for b in range(users // 128):
        udeg_own[b:b + 1, :] = counts[0:1, b * 128:(b + 1) * 128]
    for k in range(1, COLS):
        send(udeg_own, udeg_in.at[k], UDEG + k - 1, col=lax.rem(col + k, COLS))
    tot_u[...] = eug[0, col].astype(F32)
    tot_i[...] = eig[0, row].astype(F32)
    small[2].wait()
    batch = ids_ref.shape[1]
    n_chunks, tw = up_rows.shape[0], up_rows.shape[2]

    def ids_of(which, ch):
        return ids_ref[which:which + 1, pl.ds(pl.multiple_of(ch * tw, 128), tw)]

    def make_hot(ch, carry):
        for which in range(3):
            low_bits = lax.rem(ids_of(which, ch), GROUP)
            same = lax.broadcasted_iota(jnp.int32, (GROUP, tw), 0) == low_bits
            hot_ref[which, ch] = jnp.where(same, 1.0, 0.0).astype(BF16)
        return carry

    with jax.named_scope("make_hot"):
        lax.fori_loop(0, n_chunks, make_hot, 0)
    users_in(0)
    with jax.named_scope("items0"):
        for k in range(1, 4):
            items_from(0, k)
        for k in range(4):
            items_from_partner(0, k)
    with jax.named_scope("udeg_wait"):
        for k in range(1, COLS):
            arrived(udeg_in.at[k], UDEG + k - 1)
    du = udeg_own[...] + udeg_in[1] + udeg_in[2] + udeg_in[3]
    su = lax.rsqrt(jnp.maximum(du, 1.0))
    for b in range(users // 128):
        wide = jnp.broadcast_to(su[b:b + 1, :], (128, 128))
        su_ref[b * 128:(b + 1) * 128, :] = wide.T
    with jax.named_scope("ideg_wait"):
        for g in range(4):
            for k in range(1, ROWS):
                arrived(deg_in.at[k, g], DEG + 7 * g + k - 1)
    for g in range(4):
        di = deg_own[8 * g:8 * g + 8, :] + OFFSET * (ROWS - 1)
        for k in range(1, ROWS):
            di = di + deg_in[k, g].astype(F32)
        deg_inv[8 * g:8 * g + 8, :] = lax.rsqrt(jnp.maximum(di, 1.0))

    def users_all(layer):
        return jnp.concatenate([eug[layer, c] for c in range(COLS)], axis=1)

    def seg_lanes(s, start=0, width=seg):
        return pl.ds(pl.multiple_of(s * seg + start, 128), width)

    def item_dot(layer, s, eu_all):
        for h in range(2):
            part[layer, s, :, h * cw:(h + 1) * cw] = jnp.dot(
                eu_all, a_ref[:, seg_lanes(s, h * cw, cw)], preferred_element_type=F32)

    lo, hi = pl.ds(0, half), pl.ds(half, half)

    def d_copy(layer, i, s):
        return remote(part.at[layer, s], d_in.at[layer, i], RS_D + 4 * layer + i, row=partner)

    def x_first(layer, i, s):
        return remote(part.at[layer, s, lo], r1_in.at[layer, i // 2], RS_1 + 4 * layer + i // 2, row=x_row)

    def y_first(layer, i, s):
        return remote(part.at[layer, s, hi], r1_in.at[layer, 2 + i], RS_1 + 4 * layer + 2 + i, row=y_row)

    def plane_start(layer, i, s):
        arrived(d_in.at[layer, i], RS_D + 4 * layer + i)
        part[layer, s] = part[layer, s] + d_in[layer, i]

        @pl.when(jnp.logical_or(i == 0, i == 2))
        def _():
            x_first(layer, i, s).start()

        @pl.when(i < 2)
        def _():
            y_first(layer, i, s).start()

    def item_product(layer):
        eu_all = users_all(layer)

        def other(i, carry):
            s0, s1 = 2 * flipped(3 - 2 * i) + 1 - core, 2 * flipped(2 - 2 * i) + 1 - core
            item_dot(layer, s0, eu_all)
            item_dot(layer, s1, eu_all)
            d_copy(layer, 2 * i, s0).start()
            d_copy(layer, 2 * i + 1, s1).start()
            return carry

        def own(i, carry):
            s = 2 * flipped(3 - i) + core
            item_dot(layer, s, eu_all)
            plane_start(layer, i, s)
            return carry

        with jax.named_scope("item_other"):
            lax.fori_loop(0, 2, other, 0)
        with jax.named_scope("item_own"):
            lax.fori_loop(0, 4, own, 0)

    def plane_second(layer):
        base = RS_1 + 4 * layer
        arrived(r1_in.at[layer, 0], base)
        part[layer, y_row, lo] = part[layer, y_row, lo] + r1_in[layer, 0]
        send(part.at[layer, y_row, lo], r2_in.at[layer, 0], RS_2 + 2 * layer, row=y_row)
        arrived(r1_in.at[layer, 2], base + 2)
        part[layer, x_row, hi] = part[layer, x_row, hi] + r1_in[layer, 2]
        send(part.at[layer, x_row, hi], r2_in.at[layer, 1], RS_2 + 2 * layer + 1, row=x_row)

    def plane_last(layer):
        base = RS_1 + 4 * layer
        arrived(r1_in.at[layer, 1], base + 1)
        arrived(r1_in.at[layer, 3], base + 3)
        arrived(r2_in.at[layer, 0], RS_2 + 2 * layer)
        arrived(r2_in.at[layer, 1], RS_2 + 2 * layer + 1)
        low = part[layer, row, lo] + r1_in[layer, 1] + r2_in[layer, 0]
        high = part[layer, row, hi] + r1_in[layer, 3] + r2_in[layer, 1]
        cur = jnp.concatenate([low, high], axis=0).astype(BF16)
        if layer + 1 < LAYERS:
            eig[layer + 1, row] = cur
            items_out(layer + 1)
        tot_i[...] = tot_i[...] + cur.astype(F32)

    def user_dots(layer, j):
        s0 = 2 * flipped(j)
        both = nt_dot(a_ref[:, seg_lanes(s0)], eig[layer, s0])
        both = both + nt_dot(a_ref[:, seg_lanes(s0 + 1)], eig[layer, s0 + 1])
        pu_acc[:, 0:emb] = pu_acc[:, 0:emb] + both

    def user_own_chip(layer):
        pu_acc[...] = jnp.zeros_like(pu_acc)
        items_from_partner(layer, 0)
        user_dots(layer, 0)

    def user_other_chips(layer):
        items_from(layer, 1)
        items_from(layer, 2)

        def chip(j, carry):
            @pl.when(j == 3)
            def _():
                items_from(layer, j)

            items_from_partner(layer, j)
            user_dots(layer, j)
            return carry

        lax.fori_loop(1, 4, chip, 0)

    def users_reduce_out(layer):
        for c in range(COLS):
            pu[layer, c] = pu_acc[c * ush:(c + 1) * ush, :].T[:emb, :]
        for k in range(1, COLS):
            peer = lax.rem(col + k, COLS)
            send(pu.at[layer, peer], pu_in.at[layer, k], ZRS + 3 * layer + k - 1, col=peer)

    def users_reduce_in(layer):
        for k in range(1, COLS):
            arrived(pu_in.at[layer, k], ZRS + 3 * layer + k - 1)
        total = pu[layer, col] + pu_in[layer, 1] + pu_in[layer, 2] + pu_in[layer, 3]
        cur = total.astype(BF16)
        if layer + 1 < LAYERS:
            eug[layer + 1, col] = cur
            users_out(layer + 1)
        tot_u[...] = tot_u[...] + cur.astype(F32)

    tile = 256
    eu_first = users_all(0)
    n_u = users // tile

    def first_segment(s):
        for h in range(seg // tile):
            cols = seg_lanes(s, h * tile, tile)
            start = h * tile
            inv = deg_inv[pl.ds(s * (seg // dw) + start // dw, 1), start % dw:start % dw + tile]
            got = None
            for u in range(n_u):
                rows = slice(u * tile, (u + 1) * tile)
                wide = jnp.concatenate([su_ref[rows, :]] * (tile // 128), axis=1)
                block_a = a_ref[rows, cols] * (wide * inv).astype(BF16)
                a_ref[rows, cols] = block_a
                more = jnp.dot(eu_first[:, rows], block_a, preferred_element_type=F32)
                got = more if got is None else got + more
            part[0, s, :, start:start + tile] = got

    def first_other(i, carry):
        s0, s1 = 2 * flipped(3 - 2 * i) + 1 - core, 2 * flipped(2 - 2 * i) + 1 - core
        first_segment(s0)
        first_segment(s1)
        d_copy(0, 2 * i, s0).start()
        d_copy(0, 2 * i + 1, s1).start()
        return carry

    def first_own(i, carry):
        s = 2 * flipped(3 - i) + core
        first_segment(s)
        plane_start(0, i, s)
        return carry

    pu_acc[...] = jnp.zeros_like(pu_acc)
    with jax.named_scope("first_other"):
        lax.fori_loop(0, 2, first_other, 0)
    with jax.named_scope("first_own"):
        lax.fori_loop(0, 4, first_own, 0)
    with jax.named_scope("user_product0"):
        def chip_first(j, carry):
            user_dots(0, j)
            return carry

        lax.fori_loop(0, 4, chip_first, 0)
        users_reduce_out(0)
    with jax.named_scope("plane_second0"):
        plane_second(0)
    with jax.named_scope("users_reduce_in0"):
        users_reduce_in(0)
    with jax.named_scope("plane_last0"):
        plane_last(0)
    with jax.named_scope("own_chip1"):
        user_own_chip(1)
    with jax.named_scope("users_in1"):
        users_in(1)
    item_product(1)
    with jax.named_scope("user_product1"):
        user_other_chips(1)
        users_reduce_out(1)
    with jax.named_scope("plane_second1"):
        plane_second(1)
    with jax.named_scope("users_reduce_in1"):
        users_reduce_in(1)
    with jax.named_scope("plane_last1"):
        plane_last(1)
    with jax.named_scope("own_chip2"):
        user_own_chip(2)
    with jax.named_scope("users_in2"):
        users_in(2)
    item_product(2)
    with jax.named_scope("user_product2"):
        user_other_chips(2)
        users_reduce_out(2)
    with jax.named_scope("plane_second2"):
        plane_second(2)
    with jax.named_scope("users_reduce_in2"):
        users_reduce_in(2)
    scale = 1.0 / (LAYERS + 1)
    u_rows[row, col] = (tot_u[...] * scale).astype(BF16)
    for k in range(1, COLS):
        send(u_rows.at[row, col], u_rows.at[row, col], OUZ + k - 1, col=lax.rem(col + k, COLS))
    out_copy = [pltpu.make_async_copy(u_rows.at[row, col], outu_hbm, in_sem.at[0])]
    out_copy[0].start()

    def pick(tables, which, ch, first):
        hot = hot_ref[which, ch]
        high_bits = ids_of(which, ch) // GROUP - first
        acc = jnp.zeros((emb, tw), F32)
        for b, table in enumerate(tables):
            got = jnp.dot(table(), hot, preferred_element_type=F32)
            for i in range(4):
                acc = acc + jnp.where(high_bits == b * 4 + i, got[i * emb:(i + 1) * emb, :], 0.0)
        return acc

    with jax.named_scope("plane_last2"):
        plane_last(2)
    out_item = (tot_i[...] * scale).astype(BF16)
    outi_ref[...] = out_item
    out_copy.append(pltpu.make_async_copy(outi_ref, outi_hbm, in_sem.at[1]))
    out_copy[1].start()
    n_lo = seg // GROUP
    for b in range(n_lo):
        items_lo[b] = out_item[:, b * GROUP:(b + 1) * GROUP]
    first = (col * ROWS + row) * n_lo

    with jax.named_scope("ouz_wait"):
        for k in range(1, COLS):
            arrived(u_rows.at[row, 0], OUZ + k - 1)
    for k in range(1, ROWS):
        send(u_rows.at[row], u_rows.at[row], OUR + k - 1, row=lax.rem(row + k, ROWS))

    def pick_items(ch, carry):
        tables = [lambda b=b: items_lo[4 * b:4 * b + 4].reshape(4 * emb, GROUP) for b in range(n_lo // 4)]
        up_rows[ch] = pick(tables, 1, ch, first)
        down_rows[ch] = pick(tables, 2, ch, first)
        return carry

    with jax.named_scope("pick_items"):
        lax.fori_loop(0, n_chunks, pick_items, 0)
    with jax.named_scope("our_wait"):
        for k in range(1, ROWS):
            arrived(u_rows.at[0], OUR + k - 1)

    def user_table(b):
        parts = []
        for i in range(4):
            r, c = (4 * b + i) // 2, 2 * (i % 2)
            parts.append(jnp.concatenate([u_rows[r, c], u_rows[r, c + 1]], axis=1))
        return jnp.concatenate(parts, axis=0)

    def score(pair, carry):
        tables = [lambda b=b: user_table(b) for b in range(ROWS * COLS // 8)]
        for ch in (2 * pair, 2 * pair + 1):
            vec = pick(tables, 0, ch, 0)
            up = jnp.sum(vec * up_rows[ch], axis=0, keepdims=True)
            down = jnp.sum(vec * down_rows[ch], axis=0, keepdims=True)
            diff = up - down
            for t in range(tw // 128):
                mg[pl.ds(ch * (tw // 128) + t, 1), :] = diff[:, t * 128:(t + 1) * 128]
        return carry

    with jax.named_scope("score"):
        lax.fori_loop(0, n_chunks // 2, score, 0)
    for k in range(1, COLS):
        send(mg, mg_z.at[k], MGZ + k - 1, col=lax.rem(col + k, COLS))
    with jax.named_scope("mgz_wait"):
        for k in range(1, COLS):
            arrived(mg_z.at[k], MGZ + k - 1)
    mg_zsum[...] = mg[...] + mg_z[1] + mg_z[2] + mg_z[3]
    for k in range(1, ROWS):
        send(mg_zsum, mg_r.at[k], MGR + k - 1, row=lax.rem(row + k, ROWS))
    with jax.named_scope("mgr_wait"):
        for k in range(1, ROWS):
            arrived(mg_r.at[k], MGR + k - 1)
    margin = mg_zsum[...]
    for k in range(1, ROWS):
        margin = margin + mg_r[k]
    mg_z[0] = jnp.maximum(-margin, 0.0) + jnp.log1p(jnp.exp(-jnp.abs(margin)))
    out_copy.append(pltpu.make_async_copy(mg_z.at[0], loss_hbm, in_sem.at[2]))
    out_copy[2].start()

    for layer in range(LAYERS):
        for i in range(4):
            d_copy(layer, i, row).wait_send()
        for i in range(2):
            x_first(layer, 2 * i, row).wait_send()
            y_first(layer, i, row).wait_send()
        for j in range(1, 4):
            ref = eig.at[layer, row]
            remote(ref, ref, AG + 7 * layer + 3 + j, row=partner).wait_send()
    for copy in sent:
        copy.wait_send()
    for copy in out_copy:
        copy.wait()


def write_out(u_ref, i_ref, l_ref, u_out, i_out, l_out):
    u_out[...] = u_ref[...]
    i_out[...] = i_ref[...]
    l_out[...] = l_ref[...]


def solution(mesh):
    def device_body(mask_blk, user_shard, item_shard, triples):
        users, block = mask_blk.shape
        assert users <= 2 * OFFSET and block <= 128 * 256
        emb = user_shard.shape[1]
        ush, seg = user_shard.shape[0], item_shard.shape[0]
        batch = triples.shape[0]
        tw = batch // 8
        dw = block // 32
        hbm = pl.BlockSpec(memory_space=pl.ANY)
        loss_shape = (batch // 128, 128)
        results = (
            jax.ShapeDtypeStruct((emb, ush), BF16),
            jax.ShapeDtypeStruct((emb, seg), BF16),
            jax.ShapeDtypeStruct(loss_shape, F32),
        )
        found = pl.pallas_call(
            kernel,
            out_shape=results,
            in_specs=[pl.BlockSpec(memory_space=pltpu.HBM)] * 4,
            out_specs=(hbm,) * 3,
            scratch_shapes=[
                pltpu.VMEM((users, block), BF16),
                pltpu.VMEM((SLOTS, users, block // CHUNKS), jnp.int32),
                pltpu.VMEM((32, dw), F32),
                pltpu.VMEM((4, 8, dw), BF16),
                pltpu.VMEM((ROWS, 4, 8, dw), BF16),
                pltpu.VMEM((32, dw), F32),
                pltpu.VMEM((users, 128), F32),
                pltpu.VMEM((8, 128), F32),
                pltpu.VMEM((COLS, 8, 128), F32),
                pltpu.VMEM((users, 128), F32),
                pltpu.VMEM((LAYERS, ROWS, emb, seg), F32),
                pltpu.VMEM((LAYERS, 4, emb, seg), F32),
                pltpu.VMEM((LAYERS, 4, emb // 2, seg), F32),
                pltpu.VMEM((LAYERS, 2, emb // 2, seg), F32),
                pltpu.VMEM((LAYERS, ROWS, emb, seg), BF16),
                pltpu.VMEM((LAYERS, COLS, emb, ush), BF16),
                pltpu.VMEM((users, 128), F32),
                pltpu.VMEM((LAYERS, COLS, emb, ush), F32),
                pltpu.VMEM((LAYERS, COLS, emb, ush), F32),
                pltpu.VMEM((emb, seg), F32),
                pltpu.VMEM((emb, ush), F32),
                pltpu.VMEM((seg // GROUP, emb, GROUP), BF16),
                pltpu.VMEM((8, emb, tw), F32),
                pltpu.VMEM((8, emb, tw), F32),
                pltpu.VMEM((ROWS, COLS, emb, ush), BF16),
                pltpu.VMEM(loss_shape, F32),
                pltpu.VMEM((COLS,) + loss_shape, F32),
                pltpu.VMEM(loss_shape, F32),
                pltpu.VMEM((ROWS,) + loss_shape, F32),
                pltpu.VMEM((3, batch), jnp.int32),
                pltpu.VMEM((emb, seg), BF16),
                pltpu.VMEM((3, 8, GROUP, tw), BF16),
                pltpu.SemaphoreType.DMA((SLOTS,)),
                pltpu.SemaphoreType.DMA((3,)),
                pltpu.SemaphoreType.DMA((N_SEM,)),
                pltpu.SemaphoreType.DMA((N_SEM,)),
            ],
            compiler_params=pltpu.CompilerParams(
                collective_id=0, has_side_effects=True, vmem_limit_bytes=56 * 1024 * 1024),
        )(mask_blk, user_shard.T, item_shard.T, triples.T)
        vmem = pl.BlockSpec(memory_space=pltpu.VMEM)
        out_u, out_i, loss = pl.pallas_call(
            write_out, out_shape=results, in_specs=[vmem] * 3, out_specs=(vmem,) * 3,
        )(*found)
        return out_u.T, out_i.T, loss.reshape(batch)

    return jax.shard_map(
        device_body,
        mesh=mesh,
        in_specs=(P("row", "col"), P(("row", "col"), None), P(("col", "row"), None), P()),
        out_specs=(P(("row", "col"), None), P(("col", "row"), None), P()),
        check_vma=False,
    )
```

```python
import functools

import jax
import jax.numpy as jnp
from jax import lax
from jax.experimental import pallas as pl
from jax.experimental.pallas import tpu as pltpu
from jax.sharding import PartitionSpec as P

LAYERS = 3
ROWS = 8
COLS = 4
SLOTS = 4
CHUNKS = 16
STRIP = 32
EARLY = 6
RELAY0 = 13
GROUP = 256
OFFSET = 256.0
MESH_ID = pl.DeviceIdType.MESH
F32 = jnp.float32
BF16 = jnp.bfloat16

DEG = 0
UDEG = 28
AG = 31
ZAG = AG + 30
ZRS = ZAG + 9
RS_D = ZRS + 9
RS_1 = RS_D + 12
RS_2 = RS_1 + 12
OUZ = RS_2 + 6
OUR = OUZ + 3
MGZ = OUR + 7
MGR = MGZ + 6
N_SEM = MGR + 14


def nt_dot(a, b):
    return lax.dot_general(a, b, (((1,), (1,)), ((), ())), preferred_element_type=F32)


def kernel(mask_hbm, eu_hbm, ei_hbm, ids_hbm, outu_hbm, outi_hbm, loss_hbm,
           a_ref, mbuf, deg_own, deg_out, deg_in, deg_inv, udeg_part, udeg_own, udeg_in, su_ref,
           part, d_in, r1_in, r2_in, eig, eug, pu_acc, pu, pu_in, tot_i, tot_u,
           items_lo, up_rows, down_rows, u_rows, mg, mg_z, mg_zsum, mg_r, ids_ref, outi_ref, hot_ref,
           copy_sem, in_sem, send_sem, recv_sem):
    emb, seg = tot_i.shape
    users, block = a_ref.shape
    ush = tot_u.shape[1]
    cw = block // CHUNKS
    dw = block // 32
    row = lax.axis_index("row")
    col = lax.axis_index("col")
    core = lax.rem(row, 2)
    quad = row // 2
    partner = row + 1 - 2 * core
    at_x, at_y = lax.rem(quad, 2), quad // 2
    half = emb // 2
    sent = []

    def flipped(j):
        fx, fy = (j % 2 if isinstance(j, int) else lax.rem(j, 2)), j // 2
        return (at_y + fy - 2 * at_y * fy) * 2 + at_x + fx - 2 * at_x * fx

    x_row, y_row = 2 * flipped(1) + core, 2 * flipped(2) + core

    def remote(src, dst, idx, **where):
        return pltpu.make_async_remote_copy(
            src_ref=src, dst_ref=dst, send_sem=send_sem.at[idx], recv_sem=recv_sem.at[idx],
            device_id=where, device_id_type=MESH_ID)

    def send(src, dst, idx, **where):
        copy = remote(src, dst, idx, **where)
        copy.start()
        sent.append(copy)

    def arrived(dst, idx):
        remote(dst, dst, idx, row=row).wait_recv()

    def mask_copy(j):
        return pltpu.make_async_copy(
            mask_hbm.at[:, pl.ds(j * cw, cw)], mbuf.at[j % SLOTS], copy_sem.at[j % SLOTS])

    small = [
        pltpu.make_async_copy(eu_hbm, eug.at[0, col], in_sem.at[0]),
        pltpu.make_async_copy(ei_hbm, eig.at[0, row], in_sem.at[1]),
        pltpu.make_async_copy(ids_hbm, ids_ref, in_sem.at[2]),
    ]
    small[0].start()
    small[1].start()
    for j in range(SLOTS):
        mask_copy(j).start()
    small[2].start()

    barrier = pltpu.get_barrier_semaphore()
    for k in range(1, ROWS):
        pl.semaphore_signal(barrier, inc=1, device_id={"row": lax.rem(row + k, ROWS)}, device_id_type=MESH_ID)
    for k in range(1, COLS):
        pl.semaphore_signal(barrier, inc=1, device_id={"col": lax.rem(col + k, COLS)}, device_id_type=MESH_ID)

    lo, hi = pl.ds(0, half), pl.ds(half, half)
    d_row = 2 * flipped(3) + core

    def items_out(layer):
        base = AG + 10 * layer
        low, high = eig.at[layer, row, lo], eig.at[layer, row, hi]
        send(low, low, base, row=x_row)
        send(high, high, base + 1, row=y_row)
        send(high, high, base + 2, row=x_row)
        send(low, low, base + 3, row=y_row)
        send(eig.at[layer, row], eig.at[layer, row], base + 6, row=partner)

    def items_relay(layer):
        base = AG + 10 * layer
        low, high = eig.at[layer, x_row, lo], eig.at[layer, y_row, hi]
        arrived(low, base)
        send(low, low, base + 4, row=y_row)
        arrived(high, base + 1)
        send(high, high, base + 5, row=x_row)

    def items_near(layer):
        base = AG + 10 * layer
        arrived(eig.at[layer, x_row, hi], base + 2)
        send(eig.at[layer, x_row], eig.at[layer, x_row], base + 7, row=partner)
        arrived(eig.at[layer, y_row, lo], base + 3)
        send(eig.at[layer, y_row], eig.at[layer, y_row], base + 8, row=partner)

    def items_far(layer):
        base = AG + 10 * layer
        arrived(eig.at[layer, d_row, lo], base + 4)
        arrived(eig.at[layer, d_row, hi], base + 5)
        remote(eig.at[layer, d_row], eig.at[layer, d_row], base + 9, row=partner).start()

    def items_from_partner(layer, j):
        arrived(eig.at[layer, 2 * flipped(j) + 1 - core], AG + 10 * layer + 6 + j)

    def users_out(layer):
        src = eug.at[layer, col]
        for k in range(1, COLS):
            send(src, src, ZAG + 3 * layer + k - 1, col=lax.rem(col + k, COLS))

    def users_in(layer):
        for k in range(COLS - 1):
            arrived(eug.at[layer, 0], ZAG + 3 * layer + k)

    udeg_part[...] = jnp.zeros_like(udeg_part)
    udeg_own[...] = jnp.zeros_like(udeg_own)
    ready = {max(4 * g + 3, EARLY - 1): (g,) for g in range(4)}
    for j in range(CHUNKS):
        with jax.named_scope("mask_wait"):
            mask_copy(j).wait()

        def strip(s, acc, j=j):
            rows = pl.ds(pl.multiple_of(s * STRIP, STRIP), STRIP)
            m = mbuf[j % SLOTS, rows, :].astype(F32)
            a_ref[rows, j * cw:(j + 1) * cw] = m.astype(BF16)
            lanes = m[:, 0:128]
            for t in range(1, cw // 128):
                lanes = lanes + m[:, t * 128:(t + 1) * 128]
            udeg_part[rows, :] = udeg_part[rows, :] + lanes
            for t in range(STRIP // 8):
                acc = acc + m[t * 8:(t + 1) * 8, :]
            return acc

        acc = lax.fori_loop(0, users // STRIP, strip, jnp.zeros((8, cw), F32))
        if j + SLOTS < CHUNKS:
            mask_copy(j + SLOTS).start()
        total = jnp.sum(acc, axis=0, keepdims=True)
        deg_own[2 * j:2 * j + 1, :] = total[:, :dw]
        deg_own[2 * j + 1:2 * j + 2, :] = total[:, dw:]
        if j == EARLY - 1:
            with jax.named_scope("barrier"):
                pl.semaphore_wait(barrier, ROWS + COLS - 2)
            small[0].wait()
            users_out(0)
            small[1].wait()
            items_out(0)
        if j == RELAY0:
            with jax.named_scope("relay"):
                items_relay(0)
        for g in ready.get(j, ()):
            deg_out[g] = (deg_own[8 * g:8 * g + 8, :] - OFFSET).astype(BF16)
            for k in range(1, ROWS):
                send(deg_out.at[g], deg_in.at[k, g],
                     DEG + 7 * g + k - 1, row=lax.rem(row + k, ROWS))

    counts = nt_dot(jnp.ones((8, 128), BF16), udeg_part[...].astype(BF16))
    for b in range(users // 128):
        udeg_own[b:b + 1, :] = counts[0:1, b * 128:(b + 1) * 128]
    for k in range(1, COLS):
        send(udeg_own, udeg_in.at[k], UDEG + k - 1, col=lax.rem(col + k, COLS))
    tot_u[...] = eug[0, col].astype(F32)
    tot_i[...] = eig[0, row].astype(F32)
    small[2].wait()
    batch = ids_ref.shape[1]
    n_chunks, tw = up_rows.shape[0], up_rows.shape[2]

    def ids_of(which, ch):
        return ids_ref[which:which + 1, pl.ds(pl.multiple_of(ch * tw, 128), tw)]

    def make_hot(ch, carry):
        for which in range(3):
            low_bits = lax.rem(ids_of(which, ch), GROUP)
            same = lax.broadcasted_iota(jnp.int32, (GROUP, tw), 0) == low_bits
            hot_ref[which, ch] = jnp.where(same, 1.0, 0.0).astype(BF16)
        return carry

    with jax.named_scope("make_hot"):
        lax.fori_loop(0, n_chunks, make_hot, 0)
    users_in(0)
    with jax.named_scope("items0"):
        items_near(0)
        items_far(0)
        for k in range(4):
            items_from_partner(0, k)
    with jax.named_scope("udeg_wait"):
        for k in range(1, COLS):
            arrived(udeg_in.at[k], UDEG + k - 1)
    du = udeg_own[...] + udeg_in[1] + udeg_in[2] + udeg_in[3]
    su = lax.rsqrt(jnp.maximum(du, 1.0))
    for b in range(users // 128):
        wide = jnp.broadcast_to(su[b:b + 1, :], (128, 128))
        su_ref[b * 128:(b + 1) * 128, :] = wide.T
    with jax.named_scope("ideg_wait"):
        for g in range(4):
            for k in range(1, ROWS):
                arrived(deg_in.at[k, g], DEG + 7 * g + k - 1)
    for g in range(4):
        di = deg_own[8 * g:8 * g + 8, :] + OFFSET * (ROWS - 1)
        for k in range(1, ROWS):
            di = di + deg_in[k, g].astype(F32)
        deg_inv[8 * g:8 * g + 8, :] = lax.rsqrt(jnp.maximum(di, 1.0))

    def users_all(layer):
        return jnp.concatenate([eug[layer, c] for c in range(COLS)], axis=1)

    def seg_lanes(s, start=0, width=seg):
        return pl.ds(pl.multiple_of(s * seg + start, 128), width)

    def item_dot(layer, s, eu_all):
        for h in range(2):
            part[layer, s, :, h * cw:(h + 1) * cw] = jnp.dot(
                eu_all, a_ref[:, seg_lanes(s, h * cw, cw)], preferred_element_type=F32)

    def d_copy(layer, i, s):
        return remote(part.at[layer, s], d_in.at[layer, i], RS_D + 4 * layer + i, row=partner)

    def x_first(layer, i, s):
        return remote(part.at[layer, s, lo], r1_in.at[layer, i // 2], RS_1 + 4 * layer + i // 2, row=x_row)

    def y_first(layer, i, s):
        return remote(part.at[layer, s, hi], r1_in.at[layer, 2 + i], RS_1 + 4 * layer + 2 + i, row=y_row)

    def plane_start(layer, i, s):
        arrived(d_in.at[layer, i], RS_D + 4 * layer + i)
        part[layer, s] = part[layer, s] + d_in[layer, i]

        @pl.when(jnp.logical_or(i == 0, i == 2))
        def _():
            x_first(layer, i, s).start()

        @pl.when(i < 2)
        def _():
            y_first(layer, i, s).start()

    def item_product(layer, between=None):
        eu_all = users_all(layer)

        def other(i, carry):
            s0, s1 = 2 * flipped(3 - 2 * i) + 1 - core, 2 * flipped(2 - 2 * i) + 1 - core
            item_dot(layer, s0, eu_all)
            item_dot(layer, s1, eu_all)
            d_copy(layer, 2 * i, s0).start()
            d_copy(layer, 2 * i + 1, s1).start()
            return carry

        def own(i, carry):
            s0, s1 = 2 * flipped(3 - 2 * i) + core, 2 * flipped(2 - 2 * i) + core
            item_dot(layer, s0, eu_all)
            item_dot(layer, s1, eu_all)
            plane_start(layer, 2 * i, s0)
            plane_start(layer, 2 * i + 1, s1)
            return carry

        with jax.named_scope("item_other"):
            lax.fori_loop(0, 2, other, 0)
        if between is not None:
            between()
        with jax.named_scope("item_own"):
            lax.fori_loop(0, 2, own, 0)

    def plane_second(layer):
        base = RS_1 + 4 * layer
        arrived(r1_in.at[layer, 0], base)
        part[layer, y_row, lo] = part[layer, y_row, lo] + r1_in[layer, 0]
        send(part.at[layer, y_row, lo], r2_in.at[layer, 0], RS_2 + 2 * layer, row=y_row)
        arrived(r1_in.at[layer, 2], base + 2)
        part[layer, x_row, hi] = part[layer, x_row, hi] + r1_in[layer, 2]
        send(part.at[layer, x_row, hi], r2_in.at[layer, 1], RS_2 + 2 * layer + 1, row=x_row)

    def plane_last(layer):
        base = RS_1 + 4 * layer
        arrived(r1_in.at[layer, 1], base + 1)
        arrived(r1_in.at[layer, 3], base + 3)
        arrived(r2_in.at[layer, 0], RS_2 + 2 * layer)
        arrived(r2_in.at[layer, 1], RS_2 + 2 * layer + 1)
        low = part[layer, row, lo] + r1_in[layer, 1] + r2_in[layer, 0]
        high = part[layer, row, hi] + r1_in[layer, 3] + r2_in[layer, 1]
        cur = jnp.concatenate([low, high], axis=0).astype(BF16)
        if layer + 1 < LAYERS:
            eig[layer + 1, row] = cur
            items_out(layer + 1)
        tot_i[...] = tot_i[...] + cur.astype(F32)

    def user_dots(layer, j):
        s0 = 2 * flipped(j)
        both = nt_dot(a_ref[:, seg_lanes(s0)], eig[layer, s0])
        both = both + nt_dot(a_ref[:, seg_lanes(s0 + 1)], eig[layer, s0 + 1])
        pu_acc[:, 0:emb] = pu_acc[:, 0:emb] + both

    def user_own_chip(layer):
        pu_acc[...] = jnp.zeros_like(pu_acc)
        items_from_partner(layer, 0)
        user_dots(layer, 0)

    def user_other_chips(layer):
        def chip(j, carry):
            @pl.when(j == 3)
            def _():
                items_far(layer)

            items_from_partner(layer, j)
            user_dots(layer, j)
            return carry

        lax.fori_loop(1, 4, chip, 0)

    def users_reduce_out(layer):
        for c in range(COLS):
            pu[layer, c] = pu_acc[c * ush:(c + 1) * ush, :].T[:emb, :]
        for k in range(1, COLS):
            peer = lax.rem(col + k, COLS)
            send(pu.at[layer, peer], pu_in.at[layer, k], ZRS + 3 * layer + k - 1, col=peer)

    def users_reduce_in(layer):
        for k in range(1, COLS):
            arrived(pu_in.at[layer, k], ZRS + 3 * layer + k - 1)
        total = pu[layer, col] + pu_in[layer, 1] + pu_in[layer, 2] + pu_in[layer, 3]
        cur = total.astype(BF16)
        if layer + 1 < LAYERS:
            eug[layer + 1, col] = cur
            users_out(layer + 1)
        tot_u[...] = tot_u[...] + cur.astype(F32)

    tile = 256
    eu_first = users_all(0)
    n_u = users // tile

    def first_segment(s):
        for h in range(seg // tile):
            cols = seg_lanes(s, h * tile, tile)
            start = h * tile
            inv = deg_inv[pl.ds(s * (seg // dw) + start // dw, 1), start % dw:start % dw + tile]
            got = None
            for u in range(n_u):
                rows = slice(u * tile, (u + 1) * tile)
                wide = jnp.concatenate([su_ref[rows, :]] * (tile // 128), axis=1)
                block_a = a_ref[rows, cols] * (wide * inv).astype(BF16)
                a_ref[rows, cols] = block_a
                more = jnp.dot(eu_first[:, rows], block_a, preferred_element_type=F32)
                got = more if got is None else got + more
            part[0, s, :, start:start + tile] = got

    def first_other(i, carry):
        s0, s1 = 2 * flipped(3 - 2 * i) + 1 - core, 2 * flipped(2 - 2 * i) + 1 - core
        first_segment(s0)
        first_segment(s1)
        d_copy(0, 2 * i, s0).start()
        d_copy(0, 2 * i + 1, s1).start()
        return carry

    def first_own(i, carry):
        s0, s1 = 2 * flipped(3 - 2 * i) + core, 2 * flipped(2 - 2 * i) + core
        first_segment(s0)
        first_segment(s1)
        plane_start(0, 2 * i, s0)
        plane_start(0, 2 * i + 1, s1)
        return carry

    pu_acc[...] = jnp.zeros_like(pu_acc)
    with jax.named_scope("first_other"):
        lax.fori_loop(0, 2, first_other, 0)
    with jax.named_scope("first_own"):
        lax.fori_loop(0, 2, first_own, 0)
    def chip_first(j, carry):
        user_dots(0, j)
        return carry

    with jax.named_scope("user_first"):
        lax.fori_loop(0, 2, lambda j, c: chip_first(j, c), 0)
    with jax.named_scope("second0"):
        plane_second(0)
    with jax.named_scope("user_rest"):
        lax.fori_loop(0, 2, lambda j, c: chip_first(j + 2, c), 0)
        users_reduce_out(0)
    with jax.named_scope("last0"):
        plane_last(0)
    with jax.named_scope("own_chip1"):
        user_own_chip(1)
    with jax.named_scope("reduce_in0"):
        users_reduce_in(0)
    with jax.named_scope("relay1"):
        items_relay(1)
    with jax.named_scope("near1"):
        items_near(1)
    with jax.named_scope("users_in1"):
        users_in(1)
    item_product(1)
    with jax.named_scope("other_chips1"):
        user_other_chips(1)
        users_reduce_out(1)
    with jax.named_scope("second1"):
        plane_second(1)
    with jax.named_scope("last1"):
        plane_last(1)
    with jax.named_scope("reduce_in1"):
        users_reduce_in(1)
    with jax.named_scope("own_chip2"):
        user_own_chip(2)
    with jax.named_scope("users_in2"):
        users_in(2)
    with jax.named_scope("relay2"):
        items_relay(2)

    def near():
        with jax.named_scope("near2"):
            items_near(2)

    item_product(2, near)
    with jax.named_scope("other_chips2"):
        user_other_chips(2)
        users_reduce_out(2)
    with jax.named_scope("second2"):
        plane_second(2)
    with jax.named_scope("reduce_in2"):
        users_reduce_in(2)
    scale = 1.0 / (LAYERS + 1)
    u_rows[row, col] = (tot_u[...] * scale).astype(BF16)
    for k in range(1, COLS):
        send(u_rows.at[row, col], u_rows.at[row, col], OUZ + k - 1, col=lax.rem(col + k, COLS))
    out_copy = [pltpu.make_async_copy(u_rows.at[row, col], outu_hbm, in_sem.at[0])]
    out_copy[0].start()

    def pick(tables, which, ch, first):
        hot = hot_ref[which, ch]
        high_bits = ids_of(which, ch) // GROUP - first
        acc = jnp.zeros((emb, tw), F32)
        for b, table in enumerate(tables):
            got = jnp.dot(table(), hot, preferred_element_type=F32)
            for i in range(4):
                acc = acc + jnp.where(high_bits == b * 4 + i, got[i * emb:(i + 1) * emb, :], 0.0)
        return acc

    with jax.named_scope("plane_last2"):
        plane_last(2)
    out_item = (tot_i[...] * scale).astype(BF16)
    outi_ref[...] = out_item
    out_copy.append(pltpu.make_async_copy(outi_ref, outi_hbm, in_sem.at[1]))
    out_copy[1].start()
    n_lo = seg // GROUP
    for b in range(n_lo):
        items_lo[b] = out_item[:, b * GROUP:(b + 1) * GROUP]
    first = (col * ROWS + row) * n_lo

    with jax.named_scope("ouz_wait"):
        for k in range(1, COLS):
            arrived(u_rows.at[row, 0], OUZ + k - 1)
    for k in range(1, ROWS):
        send(u_rows.at[row], u_rows.at[row], OUR + k - 1, row=lax.rem(row + k, ROWS))

    def pick_items(ch, carry):
        tables = [lambda b=b: items_lo[4 * b:4 * b + 4].reshape(4 * emb, GROUP) for b in range(n_lo // 4)]
        up_rows[ch] = pick(tables, 1, ch, first)
        down_rows[ch] = pick(tables, 2, ch, first)
        return carry

    with jax.named_scope("pick_items"):
        lax.fori_loop(0, n_chunks, pick_items, 0)
    with jax.named_scope("our_wait"):
        for k in range(1, ROWS):
            arrived(u_rows.at[0], OUR + k - 1)

    def user_table(b):
        parts = []
        for i in range(4):
            r, c = (4 * b + i) // 2, 2 * (i % 2)
            parts.append(jnp.concatenate([u_rows[r, c], u_rows[r, c + 1]], axis=1))
        return jnp.concatenate(parts, axis=0)

    def score(pair, carry):
        tables = [lambda b=b: user_table(b) for b in range(ROWS * COLS // 8)]
        for ch in (2 * pair, 2 * pair + 1):
            vec = pick(tables, 0, ch, 0)
            up = jnp.sum(vec * up_rows[ch], axis=0, keepdims=True)
            down = jnp.sum(vec * down_rows[ch], axis=0, keepdims=True)
            diff = up - down
            for t in range(tw // 128):
                mg[pl.ds(ch * (tw // 128) + t, 1), :] = diff[:, t * 128:(t + 1) * 128]
        return carry

    n_rows = mg.shape[0] // 2
    halves = [pl.ds(0, n_rows), pl.ds(n_rows, n_rows)]
    for h, rows in enumerate(halves):
        with jax.named_scope("score"):
            lax.fori_loop(0, n_chunks // 4, lambda p, c, h=h: score(p + h * (n_chunks // 4), c), 0)
        for k in range(1, COLS):
            send(mg.at[rows], mg_z.at[k, rows], MGZ + 3 * h + k - 1, col=lax.rem(col + k, COLS))
    for h, rows in enumerate(halves):
        with jax.named_scope("mgz_wait"):
            for k in range(1, COLS):
                arrived(mg_z.at[k, rows], MGZ + 3 * h + k - 1)
        mg_zsum[rows] = mg[rows] + mg_z[1, rows] + mg_z[2, rows] + mg_z[3, rows]
        for k in range(1, ROWS):
            send(mg_zsum.at[rows], mg_r.at[k, rows], MGR + 7 * h + k - 1, row=lax.rem(row + k, ROWS))
    with jax.named_scope("mgr_wait"):
        for h, rows in enumerate(halves):
            for k in range(1, ROWS):
                arrived(mg_r.at[k, rows], MGR + 7 * h + k - 1)
    margin = mg_zsum[...]
    for k in range(1, ROWS):
        margin = margin + mg_r[k]
    mg_z[0] = jnp.maximum(-margin, 0.0) + jnp.log1p(jnp.exp(-jnp.abs(margin)))
    out_copy.append(pltpu.make_async_copy(mg_z.at[0], loss_hbm, in_sem.at[2]))
    out_copy[2].start()

    for layer in range(LAYERS):
        for i in range(4):
            d_copy(layer, i, row).wait_send()
        for i in range(2):
            x_first(layer, 2 * i, row).wait_send()
            y_first(layer, i, row).wait_send()
        remote(eig.at[layer, row], eig.at[layer, row], AG + 10 * layer + 9, row=partner).wait_send()
    for copy in sent:
        copy.wait_send()
    for copy in out_copy:
        copy.wait()


def write_out(u_ref, i_ref, l_ref, u_out, i_out, l_out):
    u_out[...] = u_ref[...]
    i_out[...] = i_ref[...]
    l_out[...] = l_ref[...]


def solution(mesh):
    def device_body(mask_blk, user_shard, item_shard, triples):
        users, block = mask_blk.shape
        assert users <= 2 * OFFSET and block <= 128 * 256
        emb = user_shard.shape[1]
        ush, seg = user_shard.shape[0], item_shard.shape[0]
        batch = triples.shape[0]
        tw = batch // 8
        dw = block // 32
        hbm = pl.BlockSpec(memory_space=pl.ANY)
        loss_shape = (batch // 128, 128)
        results = (
            jax.ShapeDtypeStruct((emb, ush), BF16),
            jax.ShapeDtypeStruct((emb, seg), BF16),
            jax.ShapeDtypeStruct(loss_shape, F32),
        )
        found = pl.pallas_call(
            kernel,
            out_shape=results,
            in_specs=[pl.BlockSpec(memory_space=pltpu.HBM)] * 4,
            out_specs=(hbm,) * 3,
            scratch_shapes=[
                pltpu.VMEM((users, block), BF16),
                pltpu.VMEM((SLOTS, users, block // CHUNKS), jnp.int32),
                pltpu.VMEM((32, dw), F32),
                pltpu.VMEM((4, 8, dw), BF16),
                pltpu.VMEM((ROWS, 4, 8, dw), BF16),
                pltpu.VMEM((32, dw), F32),
                pltpu.VMEM((users, 128), F32),
                pltpu.VMEM((8, 128), F32),
                pltpu.VMEM((COLS, 8, 128), F32),
                pltpu.VMEM((users, 128), F32),
                pltpu.VMEM((LAYERS, ROWS, emb, seg), F32),
                pltpu.VMEM((LAYERS, 4, emb, seg), F32),
                pltpu.VMEM((LAYERS, 4, emb // 2, seg), F32),
                pltpu.VMEM((LAYERS, 2, emb // 2, seg), F32),
                pltpu.VMEM((LAYERS, ROWS, emb, seg), BF16),
                pltpu.VMEM((LAYERS, COLS, emb, ush), BF16),
                pltpu.VMEM((users, 128), F32),
                pltpu.VMEM((LAYERS, COLS, emb, ush), F32),
                pltpu.VMEM((LAYERS, COLS, emb, ush), F32),
                pltpu.VMEM((emb, seg), F32),
                pltpu.VMEM((emb, ush), F32),
                pltpu.VMEM((seg // GROUP, emb, GROUP), BF16),
                pltpu.VMEM((8, emb, tw), F32),
                pltpu.VMEM((8, emb, tw), F32),
                pltpu.VMEM((ROWS, COLS, emb, ush), BF16),
                pltpu.VMEM(loss_shape, F32),
                pltpu.VMEM((COLS,) + loss_shape, F32),
                pltpu.VMEM(loss_shape, F32),
                pltpu.VMEM((ROWS,) + loss_shape, F32),
                pltpu.VMEM((3, batch), jnp.int32),
                pltpu.VMEM((emb, seg), BF16),
                pltpu.VMEM((3, 8, GROUP, tw), BF16),
                pltpu.SemaphoreType.DMA((SLOTS,)),
                pltpu.SemaphoreType.DMA((3,)),
                pltpu.SemaphoreType.DMA((N_SEM,)),
                pltpu.SemaphoreType.DMA((N_SEM,)),
            ],
            compiler_params=pltpu.CompilerParams(
                collective_id=0, has_side_effects=True, vmem_limit_bytes=56 * 1024 * 1024),
        )(mask_blk, user_shard.T, item_shard.T, triples.T)
        vmem = pl.BlockSpec(memory_space=pltpu.VMEM)
        out_u, out_i, loss = pl.pallas_call(
            write_out, out_shape=results, in_specs=[vmem] * 3, out_specs=(vmem,) * 3,
        )(*found)
        return out_u.T, out_i.T, loss.reshape(batch)

    return jax.shard_map(
        device_body,
        mesh=mesh,
        in_specs=(P("row", "col"), P(("row", "col"), None), P(("col", "row"), None), P()),
        out_specs=(P(("row", "col"), None), P(("col", "row"), None), P()),
        check_vma=False,
    )
```

```python
import functools

import jax
import jax.numpy as jnp
from jax import lax
from jax.experimental import pallas as pl
from jax.experimental.pallas import tpu as pltpu
from jax.sharding import PartitionSpec as P

LAYERS = 3
ROWS = 8
COLS = 4
SLOTS = 4
CHUNKS = 16
STRIP = 32
EARLY = 6
RELAY0 = 13
GROUP = 256
OFFSET = 256.0
MESH_ID = pl.DeviceIdType.MESH
F32 = jnp.float32
BF16 = jnp.bfloat16

DEG = 0
UDEG = 28
AG = 31
ZAG = AG + 30
ZRS = ZAG + 9
RS_D = ZRS + 9
RS_1 = RS_D + 12
RS_2 = RS_1 + 12
OUZ = RS_2 + 6
OUR = OUZ + 3
MGZ = OUR + 7
MGR = MGZ + 6
N_SEM = MGR + 14


def nt_dot(a, b):
    return lax.dot_general(a, b, (((1,), (1,)), ((), ())), preferred_element_type=F32)


def kernel(mask_hbm, eu_hbm, ei_hbm, ids_hbm, outu_hbm, outi_hbm, loss_hbm,
           a_ref, mbuf, deg_own, deg_out, deg_in, deg_inv, udeg_part, udeg_own, udeg_in, su_ref,
           part, d_in, r1_in, r2_in, eig, eug, pu_acc, pu, pu_in, tot_i, tot_u,
           items_lo, up_rows, down_rows, u_rows, mg, mg_z, mg_zsum, mg_r, ids_ref, outi_ref, hot_ref,
           copy_sem, in_sem, send_sem, recv_sem):
    emb, seg = tot_i.shape
    users, block = a_ref.shape
    ush = tot_u.shape[1]
    cw = block // CHUNKS
    dw = block // 32
    row = lax.axis_index("row")
    col = lax.axis_index("col")
    core = lax.rem(row, 2)
    quad = row // 2
    partner = row + 1 - 2 * core
    at_x, at_y = lax.rem(quad, 2), quad // 2
    half = emb // 2
    sent = []

    def flipped(j):
        fx, fy = (j % 2 if isinstance(j, int) else lax.rem(j, 2)), j // 2
        return (at_y + fy - 2 * at_y * fy) * 2 + at_x + fx - 2 * at_x * fx

    x_row, y_row = 2 * flipped(1) + core, 2 * flipped(2) + core

    def remote(src, dst, idx, **where):
        return pltpu.make_async_remote_copy(
            src_ref=src, dst_ref=dst, send_sem=send_sem.at[idx], recv_sem=recv_sem.at[idx],
            device_id=where, device_id_type=MESH_ID)

    def send(src, dst, idx, **where):
        copy = remote(src, dst, idx, **where)
        copy.start()
        sent.append(copy)

    def arrived(dst, idx):
        remote(dst, dst, idx, row=row).wait_recv()

    def mask_copy(j):
        return pltpu.make_async_copy(
            mask_hbm.at[:, pl.ds(j * cw, cw)], mbuf.at[j % SLOTS], copy_sem.at[j % SLOTS])

    small = [
        pltpu.make_async_copy(eu_hbm, eug.at[0, col], in_sem.at[0]),
        pltpu.make_async_copy(ei_hbm, eig.at[0, row], in_sem.at[1]),
        pltpu.make_async_copy(ids_hbm, ids_ref, in_sem.at[2]),
    ]
    small[0].start()
    small[1].start()
    for j in range(SLOTS):
        mask_copy(j).start()
    small[2].start()

    barrier = pltpu.get_barrier_semaphore()
    for k in range(1, ROWS):
        pl.semaphore_signal(barrier, inc=1, device_id={"row": lax.rem(row + k, ROWS)}, device_id_type=MESH_ID)
    for k in range(1, COLS):
        pl.semaphore_signal(barrier, inc=1, device_id={"col": lax.rem(col + k, COLS)}, device_id_type=MESH_ID)

    lo, hi = pl.ds(0, half), pl.ds(half, half)
    d_row = 2 * flipped(3) + core

    def items_out(layer):
        base = AG + 10 * layer
        low, high = eig.at[layer, row, lo], eig.at[layer, row, hi]
        send(low, low, base, row=x_row)
        send(high, high, base + 1, row=y_row)
        send(high, high, base + 2, row=x_row)
        send(low, low, base + 3, row=y_row)
        send(eig.at[layer, row], eig.at[layer, row], base + 6, row=partner)

    def items_relay(layer):
        base = AG + 10 * layer
        low, high = eig.at[layer, x_row, lo], eig.at[layer, y_row, hi]
        arrived(low, base)
        send(low, low, base + 4, row=y_row)
        arrived(high, base + 1)
        send(high, high, base + 5, row=x_row)

    def items_near(layer):
        base = AG + 10 * layer
        arrived(eig.at[layer, x_row, hi], base + 2)
        send(eig.at[layer, x_row], eig.at[layer, x_row], base + 7, row=partner)
        arrived(eig.at[layer, y_row, lo], base + 3)
        send(eig.at[layer, y_row], eig.at[layer, y_row], base + 8, row=partner)

    def items_far(layer):
        base = AG + 10 * layer
        arrived(eig.at[layer, d_row, lo], base + 4)
        arrived(eig.at[layer, d_row, hi], base + 5)
        remote(eig.at[layer, d_row], eig.at[layer, d_row], base + 9, row=partner).start()

    def items_from_partner(layer, j):
        arrived(eig.at[layer, 2 * flipped(j) + 1 - core], AG + 10 * layer + 6 + j)

    def users_out(layer):
        src = eug.at[layer, col]
        for k in range(1, COLS):
            send(src, src, ZAG + 3 * layer + k - 1, col=lax.rem(col + k, COLS))

    def users_in(layer):
        for k in range(COLS - 1):
            arrived(eug.at[layer, 0], ZAG + 3 * layer + k)

    udeg_part[...] = jnp.zeros_like(udeg_part)
    udeg_own[...] = jnp.zeros_like(udeg_own)
    ready = {max(4 * g + 3, EARLY - 1): (g,) for g in range(4)}
    for j in range(CHUNKS):
        with jax.named_scope("mask_wait"):
            mask_copy(j).wait()

        def strip(s, acc, j=j):
            rows = pl.ds(pl.multiple_of(s * STRIP, STRIP), STRIP)
            m = mbuf[j % SLOTS, rows, :].astype(F32)
            a_ref[rows, j * cw:(j + 1) * cw] = m.astype(BF16)
            lanes = m[:, 0:128]
            for t in range(1, cw // 128):
                lanes = lanes + m[:, t * 128:(t + 1) * 128]
            udeg_part[rows, :] = udeg_part[rows, :] + lanes
            for t in range(STRIP // 8):
                acc = acc + m[t * 8:(t + 1) * 8, :]
            return acc

        acc = lax.fori_loop(0, users // STRIP, strip, jnp.zeros((8, cw), F32))
        if j + SLOTS < CHUNKS:
            mask_copy(j + SLOTS).start()
        total = jnp.sum(acc, axis=0, keepdims=True)
        deg_own[2 * j:2 * j + 1, :] = total[:, :dw]
        deg_own[2 * j + 1:2 * j + 2, :] = total[:, dw:]
        if j == EARLY - 1:
            with jax.named_scope("barrier"):
                pl.semaphore_wait(barrier, ROWS + COLS - 2)
            small[0].wait()
            users_out(0)
            small[1].wait()
            items_out(0)
        if j == RELAY0:
            with jax.named_scope("relay"):
                items_relay(0)
        for g in ready.get(j, ()):
            deg_out[g] = (deg_own[8 * g:8 * g + 8, :] - OFFSET).astype(BF16)
            for k in range(1, ROWS):
                send(deg_out.at[g], deg_in.at[k, g],
                     DEG + 7 * g + k - 1, row=lax.rem(row + k, ROWS))

    counts = nt_dot(jnp.ones((8, 128), BF16), udeg_part[...].astype(BF16))
    for b in range(users // 128):
        udeg_own[b:b + 1, :] = counts[0:1, b * 128:(b + 1) * 128]
    for k in range(1, COLS):
        send(udeg_own, udeg_in.at[k], UDEG + k - 1, col=lax.rem(col + k, COLS))
    tot_u[...] = eug[0, col].astype(F32)
    tot_i[...] = eig[0, row].astype(F32)
    small[2].wait()
    batch = ids_ref.shape[1]
    n_chunks, tw = up_rows.shape[0], up_rows.shape[2]

    def ids_of(which, ch):
        return ids_ref[which:which + 1, pl.ds(pl.multiple_of(ch * tw, 128), tw)]

    def make_hot(ch, carry):
        for which in range(3):
            low_bits = lax.rem(ids_of(which, ch), GROUP)
            same = lax.broadcasted_iota(jnp.int32, (GROUP, tw), 0) == low_bits
            hot_ref[which, ch] = jnp.where(same, 1.0, 0.0).astype(BF16)
        return carry

    with jax.named_scope("make_hot"):
        lax.fori_loop(0, n_chunks, make_hot, 0)
    users_in(0)
    with jax.named_scope("items0"):
        items_near(0)
        items_far(0)
        for k in range(4):
            items_from_partner(0, k)
    with jax.named_scope("udeg_wait"):
        for k in range(1, COLS):
            arrived(udeg_in.at[k], UDEG + k - 1)
    du = udeg_own[...] + udeg_in[1] + udeg_in[2] + udeg_in[3]
    su = lax.rsqrt(jnp.maximum(du, 1.0))
    for b in range(users // 128):
        wide = jnp.broadcast_to(su[b:b + 1, :], (128, 128))
        su_ref[b * 128:(b + 1) * 128, :] = wide.T
    with jax.named_scope("ideg_wait"):
        for g in range(4):
            for k in range(1, ROWS):
                arrived(deg_in.at[k, g], DEG + 7 * g + k - 1)
    for g in range(4):
        di = deg_own[8 * g:8 * g + 8, :] + OFFSET * (ROWS - 1)
        for k in range(1, ROWS):
            di = di + deg_in[k, g].astype(F32)
        deg_inv[8 * g:8 * g + 8, :] = lax.rsqrt(jnp.maximum(di, 1.0))

    def users_all(layer):
        return jnp.concatenate([eug[layer, c] for c in range(COLS)], axis=1)

    def seg_lanes(s, start=0, width=seg):
        return pl.ds(pl.multiple_of(s * seg + start, 128), width)

    def item_dot(layer, s, eu_all):
        for h in range(2):
            part[layer, s, :, h * cw:(h + 1) * cw] = jnp.dot(
                eu_all, a_ref[:, seg_lanes(s, h * cw, cw)], preferred_element_type=F32)

    def d_copy(layer, i, s):
        return remote(part.at[layer, s], d_in.at[layer, i], RS_D + 4 * layer + i, row=partner)

    def x_first(layer, i, s):
        return remote(part.at[layer, s, lo], r1_in.at[layer, i // 2], RS_1 + 4 * layer + i // 2, row=x_row)

    def y_first(layer, i, s):
        return remote(part.at[layer, s, hi], r1_in.at[layer, 2 + i], RS_1 + 4 * layer + 2 + i, row=y_row)

    def plane_start(layer, i, s):
        arrived(d_in.at[layer, i], RS_D + 4 * layer + i)
        part[layer, s] = part[layer, s] + d_in[layer, i]

        @pl.when(jnp.logical_or(i == 0, i == 2))
        def _():
            x_first(layer, i, s).start()

        @pl.when(i < 2)
        def _():
            y_first(layer, i, s).start()

    def item_product(layer, between=None):
        eu_all = users_all(layer)

        def other(i, carry):
            s0, s1 = 2 * flipped(3 - 2 * i) + 1 - core, 2 * flipped(2 - 2 * i) + 1 - core
            item_dot(layer, s0, eu_all)
            item_dot(layer, s1, eu_all)
            d_copy(layer, 2 * i, s0).start()
            d_copy(layer, 2 * i + 1, s1).start()
            return carry

        def own(i, carry):
            s0, s1 = 2 * flipped(3 - 2 * i) + core, 2 * flipped(2 - 2 * i) + core
            item_dot(layer, s0, eu_all)
            item_dot(layer, s1, eu_all)
            plane_start(layer, 2 * i, s0)
            plane_start(layer, 2 * i + 1, s1)
            return carry

        with jax.named_scope("item_other"):
            lax.fori_loop(0, 2, other, 0)
        if between is not None:
            between()
        with jax.named_scope("item_own"):
            lax.fori_loop(0, 2, own, 0)

    def plane_second(layer):
        base = RS_1 + 4 * layer
        arrived(r1_in.at[layer, 0], base)
        part[layer, y_row, lo] = part[layer, y_row, lo] + r1_in[layer, 0]
        send(part.at[layer, y_row, lo], r2_in.at[layer, 0], RS_2 + 2 * layer, row=y_row)
        arrived(r1_in.at[layer, 2], base + 2)
        part[layer, x_row, hi] = part[layer, x_row, hi] + r1_in[layer, 2]
        send(part.at[layer, x_row, hi], r2_in.at[layer, 1], RS_2 + 2 * layer + 1, row=x_row)

    def plane_last(layer):
        base = RS_1 + 4 * layer
        arrived(r1_in.at[layer, 1], base + 1)
        arrived(r1_in.at[layer, 3], base + 3)
        arrived(r2_in.at[layer, 0], RS_2 + 2 * layer)
        arrived(r2_in.at[layer, 1], RS_2 + 2 * layer + 1)
        low = part[layer, row, lo] + r1_in[layer, 1] + r2_in[layer, 0]
        high = part[layer, row, hi] + r1_in[layer, 3] + r2_in[layer, 1]
        cur = jnp.concatenate([low, high], axis=0).astype(BF16)
        if layer + 1 < LAYERS:
            eig[layer + 1, row] = cur
            items_out(layer + 1)
        tot_i[...] = tot_i[...] + cur.astype(F32)

    def user_dots(layer, j):
        s0 = 2 * flipped(j)
        both = nt_dot(a_ref[:, seg_lanes(s0)], eig[layer, s0])
        both = both + nt_dot(a_ref[:, seg_lanes(s0 + 1)], eig[layer, s0 + 1])
        pu_acc[:, 0:emb] = pu_acc[:, 0:emb] + both

    def user_own_chip(layer):
        pu_acc[...] = jnp.zeros_like(pu_acc)
        items_from_partner(layer, 0)
        user_dots(layer, 0)

    def user_near_chips(layer):
        def chip(j, carry):
            items_from_partner(layer, j)
            user_dots(layer, j)
            return carry

        lax.fori_loop(1, 3, chip, 0)

    def user_far_chip(layer):
        items_far(layer)
        items_from_partner(layer, 3)
        user_dots(layer, 3)

    def users_reduce_out(layer):
        for c in range(COLS):
            pu[layer, c] = pu_acc[c * ush:(c + 1) * ush, :].T[:emb, :]
        for k in range(1, COLS):
            peer = lax.rem(col + k, COLS)
            send(pu.at[layer, peer], pu_in.at[layer, k], ZRS + 3 * layer + k - 1, col=peer)

    def users_reduce_in(layer):
        for k in range(1, COLS):
            arrived(pu_in.at[layer, k], ZRS + 3 * layer + k - 1)
        total = pu[layer, col] + pu_in[layer, 1] + pu_in[layer, 2] + pu_in[layer, 3]
        cur = total.astype(BF16)
        if layer + 1 < LAYERS:
            eug[layer + 1, col] = cur
            users_out(layer + 1)
        tot_u[...] = tot_u[...] + cur.astype(F32)

    tile = 256
    eu_first = users_all(0)
    n_u = users // tile

    def first_segment(s):
        for h in range(seg // tile):
            cols = seg_lanes(s, h * tile, tile)
            start = h * tile
            inv = deg_inv[pl.ds(s * (seg // dw) + start // dw, 1), start % dw:start % dw + tile]
            items = eig[0, s, :, start:start + tile]
            got = None
            for u in range(n_u):
                rows = slice(u * tile, (u + 1) * tile)
                wide = jnp.concatenate([su_ref[rows, :]] * (tile // 128), axis=1)
                block_a = a_ref[rows, cols] * (wide * inv).astype(BF16)
                a_ref[rows, cols] = block_a
                more = jnp.dot(eu_first[:, rows], block_a, preferred_element_type=F32)
                got = more if got is None else got + more
                pu_acc[rows, 0:emb] = pu_acc[rows, 0:emb] + nt_dot(block_a, items)
            part[0, s, :, start:start + tile] = got

    def first_other(i, carry):
        s0, s1 = 2 * flipped(3 - 2 * i) + 1 - core, 2 * flipped(2 - 2 * i) + 1 - core
        first_segment(s0)
        first_segment(s1)
        d_copy(0, 2 * i, s0).start()
        d_copy(0, 2 * i + 1, s1).start()
        return carry

    def first_own(i, carry):
        s0, s1 = 2 * flipped(3 - 2 * i) + core, 2 * flipped(2 - 2 * i) + core
        first_segment(s0)
        first_segment(s1)
        plane_start(0, 2 * i, s0)
        plane_start(0, 2 * i + 1, s1)
        return carry

    pu_acc[...] = jnp.zeros_like(pu_acc)
    with jax.named_scope("first_other"):
        lax.fori_loop(0, 2, first_other, 0)
    with jax.named_scope("first_own"):
        lax.fori_loop(0, 2, first_own, 0)
    with jax.named_scope("reduce_out0"):
        users_reduce_out(0)
    with jax.named_scope("second0"):
        plane_second(0)
    with jax.named_scope("reduce_in0"):
        users_reduce_in(0)
    with jax.named_scope("last0"):
        plane_last(0)
    with jax.named_scope("users_in1"):
        users_in(1)

    def relay_rows():
        with jax.named_scope("relay1"):
            items_relay(1)

    item_product(1, relay_rows)
    with jax.named_scope("own_chip1"):
        user_own_chip(1)
    with jax.named_scope("near1"):
        items_near(1)
    with jax.named_scope("near_chips1"):
        user_near_chips(1)
    with jax.named_scope("second1"):
        plane_second(1)
    with jax.named_scope("far_chip1"):
        user_far_chip(1)
        users_reduce_out(1)
    with jax.named_scope("last1"):
        plane_last(1)
    with jax.named_scope("reduce_in1"):
        users_reduce_in(1)
    with jax.named_scope("own_chip2"):
        user_own_chip(2)
    with jax.named_scope("users_in2"):
        users_in(2)
    with jax.named_scope("relay2"):
        items_relay(2)

    def near_rows():
        with jax.named_scope("near2"):
            items_near(2)

    item_product(2, near_rows)
    with jax.named_scope("near_chips2"):
        user_near_chips(2)
    with jax.named_scope("far_chip2"):
        user_far_chip(2)
        users_reduce_out(2)
    with jax.named_scope("second2"):
        plane_second(2)
    with jax.named_scope("reduce_in2"):
        users_reduce_in(2)
    scale = 1.0 / (LAYERS + 1)
    u_rows[row, col] = (tot_u[...] * scale).astype(BF16)
    for k in range(1, COLS):
        send(u_rows.at[row, col], u_rows.at[row, col], OUZ + k - 1, col=lax.rem(col + k, COLS))
    out_copy = [pltpu.make_async_copy(u_rows.at[row, col], outu_hbm, in_sem.at[0])]
    out_copy[0].start()

    def pick(tables, which, ch, first):
        hot = hot_ref[which, ch]
        high_bits = ids_of(which, ch) // GROUP - first
        acc = jnp.zeros((emb, tw), F32)
        for b, table in enumerate(tables):
            got = jnp.dot(table(), hot, preferred_element_type=F32)
            for i in range(4):
                acc = acc + jnp.where(high_bits == b * 4 + i, got[i * emb:(i + 1) * emb, :], 0.0)
        return acc

    with jax.named_scope("plane_last2"):
        plane_last(2)
    out_item = (tot_i[...] * scale).astype(BF16)
    outi_ref[...] = out_item
    out_copy.append(pltpu.make_async_copy(outi_ref, outi_hbm, in_sem.at[1]))
    out_copy[1].start()
    n_lo = seg // GROUP
    for b in range(n_lo):
        items_lo[b] = out_item[:, b * GROUP:(b + 1) * GROUP]
    first = (col * ROWS + row) * n_lo

    with jax.named_scope("ouz_wait"):
        for k in range(1, COLS):
            arrived(u_rows.at[row, 0], OUZ + k - 1)
    for k in range(1, ROWS):
        send(u_rows.at[row], u_rows.at[row], OUR + k - 1, row=lax.rem(row + k, ROWS))

    def pick_items(ch, carry):
        tables = [lambda b=b: items_lo[4 * b:4 * b + 4].reshape(4 * emb, GROUP) for b in range(n_lo // 4)]
        up_rows[ch] = pick(tables, 1, ch, first)
        down_rows[ch] = pick(tables, 2, ch, first)
        return carry

    with jax.named_scope("pick_items"):
        lax.fori_loop(0, n_chunks, pick_items, 0)
    with jax.named_scope("our_wait"):
        for k in range(1, ROWS):
            arrived(u_rows.at[0], OUR + k - 1)

    def user_table(b):
        parts = []
        for i in range(4):
            r, c = (4 * b + i) // 2, 2 * (i % 2)
            parts.append(jnp.concatenate([u_rows[r, c], u_rows[r, c + 1]], axis=1))
        return jnp.concatenate(parts, axis=0)

    def score(pair, carry):
        tables = [lambda b=b: user_table(b) for b in range(ROWS * COLS // 8)]
        for ch in (2 * pair, 2 * pair + 1):
            vec = pick(tables, 0, ch, 0)
            up = jnp.sum(vec * up_rows[ch], axis=0, keepdims=True)
            down = jnp.sum(vec * down_rows[ch], axis=0, keepdims=True)
            diff = up - down
            for t in range(tw // 128):
                mg[pl.ds(ch * (tw // 128) + t, 1), :] = diff[:, t * 128:(t + 1) * 128]
        return carry

    n_rows = mg.shape[0] // 2
    halves = [pl.ds(0, n_rows), pl.ds(n_rows, n_rows)]
    for h, rows in enumerate(halves):
        with jax.named_scope("score"):
            lax.fori_loop(0, n_chunks // 4, lambda p, c, h=h: score(p + h * (n_chunks // 4), c), 0)
        for k in range(1, COLS):
            send(mg.at[rows], mg_z.at[k, rows], MGZ + 3 * h + k - 1, col=lax.rem(col + k, COLS))
    for h, rows in enumerate(halves):
        with jax.named_scope("mgz_wait"):
            for k in range(1, COLS):
                arrived(mg_z.at[k, rows], MGZ + 3 * h + k - 1)
        mg_zsum[rows] = mg[rows] + mg_z[1, rows] + mg_z[2, rows] + mg_z[3, rows]
        for k in range(1, ROWS):
            send(mg_zsum.at[rows], mg_r.at[k, rows], MGR + 7 * h + k - 1, row=lax.rem(row + k, ROWS))
    with jax.named_scope("mgr_wait"):
        for h, rows in enumerate(halves):
            for k in range(1, ROWS):
                arrived(mg_r.at[k, rows], MGR + 7 * h + k - 1)
    margin = mg_zsum[...]
    for k in range(1, ROWS):
        margin = margin + mg_r[k]
    mg_z[0] = jnp.maximum(-margin, 0.0) + jnp.log1p(jnp.exp(-jnp.abs(margin)))
    out_copy.append(pltpu.make_async_copy(mg_z.at[0], loss_hbm, in_sem.at[2]))
    out_copy[2].start()

    for layer in range(LAYERS):
        for i in range(4):
            d_copy(layer, i, row).wait_send()
        for i in range(2):
            x_first(layer, 2 * i, row).wait_send()
            y_first(layer, i, row).wait_send()
        remote(eig.at[layer, row], eig.at[layer, row], AG + 10 * layer + 9, row=partner).wait_send()
    for copy in sent:
        copy.wait_send()
    for copy in out_copy:
        copy.wait()


def write_out(u_ref, i_ref, l_ref, u_out, i_out, l_out):
    u_out[...] = u_ref[...]
    i_out[...] = i_ref[...]
    l_out[...] = l_ref[...]


def solution(mesh):
    def device_body(mask_blk, user_shard, item_shard, triples):
        users, block = mask_blk.shape
        assert users <= 2 * OFFSET and block <= 128 * 256
        emb = user_shard.shape[1]
        ush, seg = user_shard.shape[0], item_shard.shape[0]
        batch = triples.shape[0]
        tw = batch // 8
        dw = block // 32
        hbm = pl.BlockSpec(memory_space=pl.ANY)
        loss_shape = (batch // 128, 128)
        results = (
            jax.ShapeDtypeStruct((emb, ush), BF16),
            jax.ShapeDtypeStruct((emb, seg), BF16),
            jax.ShapeDtypeStruct(loss_shape, F32),
        )
        found = pl.pallas_call(
            kernel,
            out_shape=results,
            in_specs=[pl.BlockSpec(memory_space=pltpu.HBM)] * 4,
            out_specs=(hbm,) * 3,
            scratch_shapes=[
                pltpu.VMEM((users, block), BF16),
                pltpu.VMEM((SLOTS, users, block // CHUNKS), jnp.int32),
                pltpu.VMEM((32, dw), F32),
                pltpu.VMEM((4, 8, dw), BF16),
                pltpu.VMEM((ROWS, 4, 8, dw), BF16),
                pltpu.VMEM((32, dw), F32),
                pltpu.VMEM((users, 128), F32),
                pltpu.VMEM((8, 128), F32),
                pltpu.VMEM((COLS, 8, 128), F32),
                pltpu.VMEM((users, 128), F32),
                pltpu.VMEM((LAYERS, ROWS, emb, seg), F32),
                pltpu.VMEM((LAYERS, 4, emb, seg), F32),
                pltpu.VMEM((LAYERS, 4, emb // 2, seg), F32),
                pltpu.VMEM((LAYERS, 2, emb // 2, seg), F32),
                pltpu.VMEM((LAYERS, ROWS, emb, seg), BF16),
                pltpu.VMEM((LAYERS, COLS, emb, ush), BF16),
                pltpu.VMEM((users, 128), F32),
                pltpu.VMEM((LAYERS, COLS, emb, ush), F32),
                pltpu.VMEM((LAYERS, COLS, emb, ush), F32),
                pltpu.VMEM((emb, seg), F32),
                pltpu.VMEM((emb, ush), F32),
                pltpu.VMEM((seg // GROUP, emb, GROUP), BF16),
                pltpu.VMEM((8, emb, tw), F32),
                pltpu.VMEM((8, emb, tw), F32),
                pltpu.VMEM((ROWS, COLS, emb, ush), BF16),
                pltpu.VMEM(loss_shape, F32),
                pltpu.VMEM((COLS,) + loss_shape, F32),
                pltpu.VMEM(loss_shape, F32),
                pltpu.VMEM((ROWS,) + loss_shape, F32),
                pltpu.VMEM((3, batch), jnp.int32),
                pltpu.VMEM((emb, seg), BF16),
                pltpu.VMEM((3, 8, GROUP, tw), BF16),
                pltpu.SemaphoreType.DMA((SLOTS,)),
                pltpu.SemaphoreType.DMA((3,)),
                pltpu.SemaphoreType.DMA((N_SEM,)),
                pltpu.SemaphoreType.DMA((N_SEM,)),
            ],
            compiler_params=pltpu.CompilerParams(
                collective_id=0, has_side_effects=True, vmem_limit_bytes=56 * 1024 * 1024),
        )(mask_blk, user_shard.T, item_shard.T, triples.T)
        vmem = pl.BlockSpec(memory_space=pltpu.VMEM)
        out_u, out_i, loss = pl.pallas_call(
            write_out, out_shape=results, in_specs=[vmem] * 3, out_specs=(vmem,) * 3,
        )(*found)
        return out_u.T, out_i.T, loss.reshape(batch)

    return jax.shard_map(
        device_body,
        mesh=mesh,
        in_specs=(P("row", "col"), P(("row", "col"), None), P(("col", "row"), None), P()),
        out_specs=(P(("row", "col"), None), P(("col", "row"), None), P()),
        check_vma=False,
    )
```

```python
import functools

import jax
import jax.numpy as jnp
from jax import lax
from jax.experimental import pallas as pl
from jax.experimental.pallas import tpu as pltpu
from jax.sharding import PartitionSpec as P

LAYERS = 3
ROWS = 8
COLS = 4
SLOTS = 4
CHUNKS = 16
STRIP = 32
EARLY = 6
RELAY0 = 13
GROUP = 256
OFFSET = 256.0
MESH_ID = pl.DeviceIdType.MESH
F32 = jnp.float32
BF16 = jnp.bfloat16

DEG = 0
UDEG = 28
AG = 31
ZAG = AG + 30
ZRS = ZAG + 9
RS_D = ZRS + 9
RS_1 = RS_D + 12
RS_2 = RS_1 + 12
OUZ = RS_2 + 6
OUR = OUZ + 3
MGZ = OUR + 7
MGR = MGZ + 6
N_SEM = MGR + 14


def nt_dot(a, b):
    return lax.dot_general(a, b, (((1,), (1,)), ((), ())), preferred_element_type=F32)


def kernel(mask_hbm, eu_hbm, ei_hbm, ids_hbm, outu_hbm, outi_hbm, loss_hbm,
           a_ref, mbuf, deg_own, deg_out, deg_in, deg_inv, udeg_part, udeg_own, udeg_in, su_ref,
           part, d_in, r1_in, r2_in, eig, eug, pu_acc, pu, pu_in, tot_i, tot_u,
           items_lo, up_rows, down_rows, u_rows, mg, mg_z, mg_zsum, mg_r, ids_ref, outi_ref, hot_ref,
           copy_sem, in_sem, send_sem, recv_sem):
    emb, seg = tot_i.shape
    users, block = a_ref.shape
    ush = tot_u.shape[1]
    cw = block // CHUNKS
    dw = block // 32
    row = lax.axis_index("row")
    col = lax.axis_index("col")
    core = lax.rem(row, 2)
    quad = row // 2
    partner = row + 1 - 2 * core
    at_x, at_y = lax.rem(quad, 2), quad // 2
    half = emb // 2
    sent = []

    def flipped(j):
        fx, fy = (j % 2 if isinstance(j, int) else lax.rem(j, 2)), j // 2
        return (at_y + fy - 2 * at_y * fy) * 2 + at_x + fx - 2 * at_x * fx

    x_row, y_row = 2 * flipped(1) + core, 2 * flipped(2) + core

    def remote(src, dst, idx, **where):
        return pltpu.make_async_remote_copy(
            src_ref=src, dst_ref=dst, send_sem=send_sem.at[idx], recv_sem=recv_sem.at[idx],
            device_id=where, device_id_type=MESH_ID)

    def send(src, dst, idx, **where):
        copy = remote(src, dst, idx, **where)
        copy.start()
        sent.append(copy)

    def arrived(dst, idx):
        remote(dst, dst, idx, row=row).wait_recv()

    def mask_copy(j):
        return pltpu.make_async_copy(
            mask_hbm.at[:, pl.ds(j * cw, cw)], mbuf.at[j % SLOTS], copy_sem.at[j % SLOTS])

    small = [
        pltpu.make_async_copy(eu_hbm, eug.at[0, col], in_sem.at[0]),
        pltpu.make_async_copy(ei_hbm, eig.at[0, row], in_sem.at[1]),
        pltpu.make_async_copy(ids_hbm, ids_ref, in_sem.at[2]),
    ]
    small[0].start()
    small[1].start()
    for j in range(SLOTS):
        mask_copy(j).start()
    small[2].start()

    barrier = pltpu.get_barrier_semaphore()
    for k in range(1, ROWS):
        pl.semaphore_signal(barrier, inc=1, device_id={"row": lax.rem(row + k, ROWS)}, device_id_type=MESH_ID)
    for k in range(1, COLS):
        pl.semaphore_signal(barrier, inc=1, device_id={"col": lax.rem(col + k, COLS)}, device_id_type=MESH_ID)

    lo, hi = pl.ds(0, half), pl.ds(half, half)
    d_row = 2 * flipped(3) + core

    def items_out(layer):
        base = AG + 10 * layer
        low, high = eig.at[layer, row, lo], eig.at[layer, row, hi]
        send(low, low, base, row=x_row)
        send(high, high, base + 1, row=y_row)
        send(high, high, base + 2, row=x_row)
        send(low, low, base + 3, row=y_row)
        send(eig.at[layer, row], eig.at[layer, row], base + 6, row=partner)

    def items_relay(layer):
        base = AG + 10 * layer
        low, high = eig.at[layer, x_row, lo], eig.at[layer, y_row, hi]
        arrived(low, base)
        send(low, low, base + 4, row=y_row)
        arrived(high, base + 1)
        send(high, high, base + 5, row=x_row)

    def items_near(layer):
        base = AG + 10 * layer
        arrived(eig.at[layer, x_row, hi], base + 2)
        send(eig.at[layer, x_row], eig.at[layer, x_row], base + 7, row=partner)
        arrived(eig.at[layer, y_row, lo], base + 3)
        send(eig.at[layer, y_row], eig.at[layer, y_row], base + 8, row=partner)

    def items_far(layer):
        base = AG + 10 * layer
        arrived(eig.at[layer, d_row, lo], base + 4)
        arrived(eig.at[layer, d_row, hi], base + 5)
        remote(eig.at[layer, d_row], eig.at[layer, d_row], base + 9, row=partner).start()

    def items_from_partner(layer, j):
        arrived(eig.at[layer, 2 * flipped(j) + 1 - core], AG + 10 * layer + 6 + j)

    def users_out(layer):
        src = eug.at[layer, col]
        for k in range(1, COLS):
            send(src, src, ZAG + 3 * layer + k - 1, col=lax.rem(col + k, COLS))

    def users_in(layer):
        for k in range(COLS - 1):
            arrived(eug.at[layer, 0], ZAG + 3 * layer + k)

    udeg_part[...] = jnp.zeros_like(udeg_part)
    udeg_own[...] = jnp.zeros_like(udeg_own)
    ready = {max(4 * g + 3, EARLY - 1): (g,) for g in range(4)}
    for j in range(CHUNKS):
        with jax.named_scope("mask_wait"):
            mask_copy(j).wait()

        def strip(s, acc, j=j):
            rows = pl.ds(pl.multiple_of(s * STRIP, STRIP), STRIP)
            m = mbuf[j % SLOTS, rows, :].astype(F32)
            a_ref[rows, j * cw:(j + 1) * cw] = m.astype(BF16)
            lanes = m[:, 0:128]
            for t in range(1, cw // 128):
                lanes = lanes + m[:, t * 128:(t + 1) * 128]
            udeg_part[rows, :] = udeg_part[rows, :] + lanes
            for t in range(STRIP // 8):
                acc = acc + m[t * 8:(t + 1) * 8, :]
            return acc

        acc = lax.fori_loop(0, users // STRIP, strip, jnp.zeros((8, cw), F32))
        if j + SLOTS < CHUNKS:
            mask_copy(j + SLOTS).start()
        total = jnp.sum(acc, axis=0, keepdims=True)
        deg_own[2 * j:2 * j + 1, :] = total[:, :dw]
        deg_own[2 * j + 1:2 * j + 2, :] = total[:, dw:]
        if j == EARLY - 1:
            with jax.named_scope("barrier"):
                pl.semaphore_wait(barrier, ROWS + COLS - 2)
            small[0].wait()
            users_out(0)
            small[1].wait()
            items_out(0)
        if j == RELAY0:
            with jax.named_scope("relay"):
                items_relay(0)
        for g in ready.get(j, ()):
            deg_out[g] = (deg_own[8 * g:8 * g + 8, :] - OFFSET).astype(BF16)
            for k in range(1, ROWS):
                send(deg_out.at[g], deg_in.at[k, g],
                     DEG + 7 * g + k - 1, row=lax.rem(row + k, ROWS))

    counts = nt_dot(jnp.ones((8, 128), BF16), udeg_part[...].astype(BF16))
    for b in range(users // 128):
        udeg_own[b:b + 1, :] = counts[0:1, b * 128:(b + 1) * 128]
    for k in range(1, COLS):
        send(udeg_own, udeg_in.at[k], UDEG + k - 1, col=lax.rem(col + k, COLS))
    tot_u[...] = eug[0, col].astype(F32)
    tot_i[...] = eig[0, row].astype(F32)
    small[2].wait()
    batch = ids_ref.shape[1]
    n_chunks, tw = up_rows.shape[0], up_rows.shape[2]

    def ids_of(which, ch):
        return ids_ref[which:which + 1, pl.ds(pl.multiple_of(ch * tw, 128), tw)]

    def make_hot(ch, carry):
        for which in range(3):
            low_bits = lax.rem(ids_of(which, ch), GROUP)
            same = lax.broadcasted_iota(jnp.int32, (GROUP, tw), 0) == low_bits
            hot_ref[which, ch] = jnp.where(same, 1.0, 0.0).astype(BF16)
        return carry

    with jax.named_scope("make_hot"):
        lax.fori_loop(0, n_chunks, make_hot, 0)
    users_in(0)
    with jax.named_scope("items0"):
        items_near(0)
        items_far(0)
        for k in range(4):
            items_from_partner(0, k)
    with jax.named_scope("udeg_wait"):
        for k in range(1, COLS):
            arrived(udeg_in.at[k], UDEG + k - 1)
    du = udeg_own[...] + udeg_in[1] + udeg_in[2] + udeg_in[3]
    su = lax.rsqrt(jnp.maximum(du, 1.0))
    for b in range(users // 128):
        wide = jnp.broadcast_to(su[b:b + 1, :], (128, 128))
        su_ref[b * 128:(b + 1) * 128, :] = wide.T
    with jax.named_scope("ideg_wait"):
        for g in range(4):
            for k in range(1, ROWS):
                arrived(deg_in.at[k, g], DEG + 7 * g + k - 1)
    for g in range(4):
        di = deg_own[8 * g:8 * g + 8, :] + OFFSET * (ROWS - 1)
        for k in range(1, ROWS):
            di = di + deg_in[k, g].astype(F32)
        deg_inv[8 * g:8 * g + 8, :] = lax.rsqrt(jnp.maximum(di, 1.0))

    def users_all(layer):
        return jnp.concatenate([eug[layer, c] for c in range(COLS)], axis=1)

    def seg_lanes(s, start=0, width=seg):
        return pl.ds(pl.multiple_of(s * seg + start, 128), width)

    def item_dot(layer, s, eu_all):
        for h in range(2):
            part[layer, s, :, h * cw:(h + 1) * cw] = jnp.dot(
                eu_all, a_ref[:, seg_lanes(s, h * cw, cw)], preferred_element_type=F32)

    def d_copy(layer, i, s):
        return remote(part.at[layer, s], d_in.at[layer, i], RS_D + 4 * layer + i, row=partner)

    def x_first(layer, i, s):
        return remote(part.at[layer, s, lo], r1_in.at[layer, i // 2], RS_1 + 4 * layer + i // 2, row=x_row)

    def y_first(layer, i, s):
        return remote(part.at[layer, s, hi], r1_in.at[layer, 2 + i], RS_1 + 4 * layer + 2 + i, row=y_row)

    def plane_start(layer, i, s):
        arrived(d_in.at[layer, i], RS_D + 4 * layer + i)
        part[layer, s] = part[layer, s] + d_in[layer, i]

        @pl.when(jnp.logical_or(i == 0, i == 2))
        def _():
            x_first(layer, i, s).start()

        @pl.when(i < 2)
        def _():
            y_first(layer, i, s).start()

    def item_product(layer, between=None):
        eu_all = users_all(layer)

        def other(i, carry):
            s0, s1 = 2 * flipped(3 - 2 * i) + 1 - core, 2 * flipped(2 - 2 * i) + 1 - core
            item_dot(layer, s0, eu_all)
            item_dot(layer, s1, eu_all)
            d_copy(layer, 2 * i, s0).start()
            d_copy(layer, 2 * i + 1, s1).start()
            return carry

        def own(i, carry):
            s0, s1 = 2 * flipped(3 - 2 * i) + core, 2 * flipped(2 - 2 * i) + core
            item_dot(layer, s0, eu_all)
            item_dot(layer, s1, eu_all)
            plane_start(layer, 2 * i, s0)
            plane_start(layer, 2 * i + 1, s1)
            return carry

        with jax.named_scope("item_other"):
            lax.fori_loop(0, 2, other, 0)
        if between is not None:
            between()
        with jax.named_scope("item_own"):
            lax.fori_loop(0, 2, own, 0)

    def plane_second(layer):
        base = RS_1 + 4 * layer
        arrived(r1_in.at[layer, 0], base)
        part[layer, y_row, lo] = part[layer, y_row, lo] + r1_in[layer, 0]
        send(part.at[layer, y_row, lo], r2_in.at[layer, 0], RS_2 + 2 * layer, row=y_row)
        arrived(r1_in.at[layer, 2], base + 2)
        part[layer, x_row, hi] = part[layer, x_row, hi] + r1_in[layer, 2]
        send(part.at[layer, x_row, hi], r2_in.at[layer, 1], RS_2 + 2 * layer + 1, row=x_row)

    def plane_last(layer):
        base = RS_1 + 4 * layer
        arrived(r1_in.at[layer, 1], base + 1)
        arrived(r1_in.at[layer, 3], base + 3)
        arrived(r2_in.at[layer, 0], RS_2 + 2 * layer)
        arrived(r2_in.at[layer, 1], RS_2 + 2 * layer + 1)
        low = part[layer, row, lo] + r1_in[layer, 1] + r2_in[layer, 0]
        high = part[layer, row, hi] + r1_in[layer, 3] + r2_in[layer, 1]
        cur = jnp.concatenate([low, high], axis=0).astype(BF16)
        if layer + 1 < LAYERS:
            eig[layer + 1, row] = cur
            items_out(layer + 1)
        tot_i[...] = tot_i[...] + cur.astype(F32)

    def user_dots(layer, j):
        s0 = 2 * flipped(j)
        both = nt_dot(a_ref[:, seg_lanes(s0)], eig[layer, s0])
        both = both + nt_dot(a_ref[:, seg_lanes(s0 + 1)], eig[layer, s0 + 1])
        pu_acc[:, 0:emb] = pu_acc[:, 0:emb] + both

    def user_own_chip(layer):
        pu_acc[...] = jnp.zeros_like(pu_acc)
        items_from_partner(layer, 0)
        user_dots(layer, 0)

    def user_chip(layer, j):
        items_from_partner(layer, j)
        user_dots(layer, j)

    def users_reduce_out(layer):
        for c in range(COLS):
            pu[layer, c] = pu_acc[c * ush:(c + 1) * ush, :].T[:emb, :]
        for k in range(1, COLS):
            peer = lax.rem(col + k, COLS)
            send(pu.at[layer, peer], pu_in.at[layer, k], ZRS + 3 * layer + k - 1, col=peer)

    def users_reduce_in(layer):
        for k in range(1, COLS):
            arrived(pu_in.at[layer, k], ZRS + 3 * layer + k - 1)
        total = pu[layer, col] + pu_in[layer, 1] + pu_in[layer, 2] + pu_in[layer, 3]
        cur = total.astype(BF16)
        if layer + 1 < LAYERS:
            eug[layer + 1, col] = cur
            users_out(layer + 1)
        tot_u[...] = tot_u[...] + cur.astype(F32)

    tile = 256
    eu_first = users_all(0)
    n_u = users // tile

    def first_segment(s):
        for h in range(seg // tile):
            cols = seg_lanes(s, h * tile, tile)
            start = h * tile
            inv = deg_inv[pl.ds(s * (seg // dw) + start // dw, 1), start % dw:start % dw + tile]
            items = eig[0, s, :, start:start + tile]
            got = None
            for u in range(n_u):
                rows = slice(u * tile, (u + 1) * tile)
                wide = jnp.concatenate([su_ref[rows, :]] * (tile // 128), axis=1)
                block_a = a_ref[rows, cols] * (wide * inv).astype(BF16)
                a_ref[rows, cols] = block_a
                more = jnp.dot(eu_first[:, rows], block_a, preferred_element_type=F32)
                got = more if got is None else got + more
                pu_acc[rows, 0:emb] = pu_acc[rows, 0:emb] + nt_dot(block_a, items)
            part[0, s, :, start:start + tile] = got

    def first_pair(i, carry):
        theirs, mine = 2 * flipped(3 - i) + 1 - core, 2 * flipped(3 - i) + core
        first_segment(theirs)
        d_copy(0, i, theirs).start()

        @pl.when(i > 0)
        def _():
            plane_start(0, i - 1, 2 * flipped(4 - i) + core)

        first_segment(mine)
        return carry

    pu_acc[...] = jnp.zeros_like(pu_acc)
    with jax.named_scope("first"):
        lax.fori_loop(0, 4, first_pair, 0)
    with jax.named_scope("reduce_out0"):
        users_reduce_out(0)
    with jax.named_scope("second0"):
        plane_start(0, 3, row)
        plane_second(0)
    with jax.named_scope("reduce_in0"):
        users_reduce_in(0)
    with jax.named_scope("last0"):
        plane_last(0)
    with jax.named_scope("users_in1"):
        users_in(1)

    def relay_rows():
        with jax.named_scope("own_chip1"):
            user_own_chip(1)
        with jax.named_scope("relay1"):
            items_relay(1)

    item_product(1, relay_rows)
    with jax.named_scope("near1"):
        items_near(1)
        user_chip(1, 1)
    with jax.named_scope("far1"):
        items_far(1)
    with jax.named_scope("chip1"):
        user_chip(1, 2)
    with jax.named_scope("second1"):
        plane_second(1)
    with jax.named_scope("far_chip1"):
        user_chip(1, 3)
        users_reduce_out(1)
    with jax.named_scope("last1"):
        plane_last(1)
    with jax.named_scope("reduce_in1"):
        users_reduce_in(1)
    with jax.named_scope("own_chip2"):
        user_own_chip(2)
    with jax.named_scope("relay2"):
        items_relay(2)
    with jax.named_scope("users_in2"):
        users_in(2)

    def near_rows():
        with jax.named_scope("near2"):
            items_near(2)

    item_product(2, near_rows)
    with jax.named_scope("far2"):
        items_far(2)
    with jax.named_scope("near_chips2"):
        user_chip(2, 1)
        user_chip(2, 2)
    with jax.named_scope("far_chip2"):
        user_chip(2, 3)
        users_reduce_out(2)
    with jax.named_scope("second2"):
        plane_second(2)
    with jax.named_scope("reduce_in2"):
        users_reduce_in(2)
    scale = 1.0 / (LAYERS + 1)
    u_rows[row, col] = (tot_u[...] * scale).astype(BF16)
    for k in range(1, COLS):
        send(u_rows.at[row, col], u_rows.at[row, col], OUZ + k - 1, col=lax.rem(col + k, COLS))
    out_copy = [pltpu.make_async_copy(u_rows.at[row, col], outu_hbm, in_sem.at[0])]
    out_copy[0].start()

    def pick(tables, which, ch, first):
        hot = hot_ref[which, ch]
        high_bits = ids_of(which, ch) // GROUP - first
        acc = jnp.zeros((emb, tw), F32)
        for b, table in enumerate(tables):
            got = jnp.dot(table(), hot, preferred_element_type=F32)
            for i in range(4):
                acc = acc + jnp.where(high_bits == b * 4 + i, got[i * emb:(i + 1) * emb, :], 0.0)
        return acc

    with jax.named_scope("plane_last2"):
        plane_last(2)
    out_item = (tot_i[...] * scale).astype(BF16)
    outi_ref[...] = out_item
    out_copy.append(pltpu.make_async_copy(outi_ref, outi_hbm, in_sem.at[1]))
    out_copy[1].start()
    n_lo = seg // GROUP
    for b in range(n_lo):
        items_lo[b] = out_item[:, b * GROUP:(b + 1) * GROUP]
    first = (col * ROWS + row) * n_lo

    with jax.named_scope("ouz_wait"):
        for k in range(1, COLS):
            arrived(u_rows.at[row, 0], OUZ + k - 1)
    for k in range(1, ROWS):
        send(u_rows.at[row], u_rows.at[row], OUR + k - 1, row=lax.rem(row + k, ROWS))

    def pick_items(ch, carry):
        tables = [lambda b=b: items_lo[4 * b:4 * b + 4].reshape(4 * emb, GROUP) for b in range(n_lo // 4)]
        up_rows[ch] = pick(tables, 1, ch, first)
        down_rows[ch] = pick(tables, 2, ch, first)
        return carry

    with jax.named_scope("pick_items"):
        lax.fori_loop(0, n_chunks, pick_items, 0)
    with jax.named_scope("our_wait"):
        for k in range(1, ROWS):
            arrived(u_rows.at[0], OUR + k - 1)

    def user_table(b):
        parts = []
        for i in range(4):
            r, c = (4 * b + i) // 2, 2 * (i % 2)
            parts.append(jnp.concatenate([u_rows[r, c], u_rows[r, c + 1]], axis=1))
        return jnp.concatenate(parts, axis=0)

    def score(pair, carry):
        tables = [lambda b=b: user_table(b) for b in range(ROWS * COLS // 8)]
        for ch in (2 * pair, 2 * pair + 1):
            vec = pick(tables, 0, ch, 0)
            up = jnp.sum(vec * up_rows[ch], axis=0, keepdims=True)
            down = jnp.sum(vec * down_rows[ch], axis=0, keepdims=True)
            diff = up - down
            for t in range(tw // 128):
                mg[pl.ds(ch * (tw // 128) + t, 1), :] = diff[:, t * 128:(t + 1) * 128]
        return carry

    n_rows = mg.shape[0] // 2
    halves = [pl.ds(0, n_rows), pl.ds(n_rows, n_rows)]
    for h, rows in enumerate(halves):
        with jax.named_scope("score"):
            lax.fori_loop(0, n_chunks // 4, lambda p, c, h=h: score(p + h * (n_chunks // 4), c), 0)
        for k in range(1, COLS):
            send(mg.at[rows], mg_z.at[k, rows], MGZ + 3 * h + k - 1, col=lax.rem(col + k, COLS))
    for h, rows in enumerate(halves):
        with jax.named_scope("mgz_wait"):
            for k in range(1, COLS):
                arrived(mg_z.at[k, rows], MGZ + 3 * h + k - 1)
        mg_zsum[rows] = mg[rows] + mg_z[1, rows] + mg_z[2, rows] + mg_z[3, rows]
        for k in range(1, ROWS):
            send(mg_zsum.at[rows], mg_r.at[k, rows], MGR + 7 * h + k - 1, row=lax.rem(row + k, ROWS))
    with jax.named_scope("mgr_wait"):
        for h, rows in enumerate(halves):
            for k in range(1, ROWS):
                arrived(mg_r.at[k, rows], MGR + 7 * h + k - 1)
    margin = mg_zsum[...]
    for k in range(1, ROWS):
        margin = margin + mg_r[k]
    mg_z[0] = jnp.maximum(-margin, 0.0) + jnp.log1p(jnp.exp(-jnp.abs(margin)))
    out_copy.append(pltpu.make_async_copy(mg_z.at[0], loss_hbm, in_sem.at[2]))
    out_copy[2].start()

    for layer in range(LAYERS):
        for i in range(4):
            d_copy(layer, i, row).wait_send()
        for i in range(2):
            x_first(layer, 2 * i, row).wait_send()
            y_first(layer, i, row).wait_send()
        remote(eig.at[layer, row], eig.at[layer, row], AG + 10 * layer + 9, row=partner).wait_send()
    for copy in sent:
        copy.wait_send()
    for copy in out_copy:
        copy.wait()


def write_out(u_ref, i_ref, l_ref, u_out, i_out, l_out):
    u_out[...] = u_ref[...]
    i_out[...] = i_ref[...]
    l_out[...] = l_ref[...]


def solution(mesh):
    def device_body(mask_blk, user_shard, item_shard, triples):
        users, block = mask_blk.shape
        assert users <= 2 * OFFSET and block <= 128 * 256
        emb = user_shard.shape[1]
        ush, seg = user_shard.shape[0], item_shard.shape[0]
        batch = triples.shape[0]
        tw = batch // 8
        dw = block // 32
        hbm = pl.BlockSpec(memory_space=pl.ANY)
        loss_shape = (batch // 128, 128)
        results = (
            jax.ShapeDtypeStruct((emb, ush), BF16),
            jax.ShapeDtypeStruct((emb, seg), BF16),
            jax.ShapeDtypeStruct(loss_shape, F32),
        )
        found = pl.pallas_call(
            kernel,
            out_shape=results,
            in_specs=[pl.BlockSpec(memory_space=pltpu.HBM)] * 4,
            out_specs=(hbm,) * 3,
            scratch_shapes=[
                pltpu.VMEM((users, block), BF16),
                pltpu.VMEM((SLOTS, users, block // CHUNKS), jnp.int32),
                pltpu.VMEM((32, dw), F32),
                pltpu.VMEM((4, 8, dw), BF16),
                pltpu.VMEM((ROWS, 4, 8, dw), BF16),
                pltpu.VMEM((32, dw), F32),
                pltpu.VMEM((users, 128), F32),
                pltpu.VMEM((8, 128), F32),
                pltpu.VMEM((COLS, 8, 128), F32),
                pltpu.VMEM((users, 128), F32),
                pltpu.VMEM((LAYERS, ROWS, emb, seg), F32),
                pltpu.VMEM((LAYERS, 4, emb, seg), F32),
                pltpu.VMEM((LAYERS, 4, emb // 2, seg), F32),
                pltpu.VMEM((LAYERS, 2, emb // 2, seg), F32),
                pltpu.VMEM((LAYERS, ROWS, emb, seg), BF16),
                pltpu.VMEM((LAYERS, COLS, emb, ush), BF16),
                pltpu.VMEM((users, 128), F32),
                pltpu.VMEM((LAYERS, COLS, emb, ush), F32),
                pltpu.VMEM((LAYERS, COLS, emb, ush), F32),
                pltpu.VMEM((emb, seg), F32),
                pltpu.VMEM((emb, ush), F32),
                pltpu.VMEM((seg // GROUP, emb, GROUP), BF16),
                pltpu.VMEM((8, emb, tw), F32),
                pltpu.VMEM((8, emb, tw), F32),
                pltpu.VMEM((ROWS, COLS, emb, ush), BF16),
                pltpu.VMEM(loss_shape, F32),
                pltpu.VMEM((COLS,) + loss_shape, F32),
                pltpu.VMEM(loss_shape, F32),
                pltpu.VMEM((ROWS,) + loss_shape, F32),
                pltpu.VMEM((3, batch), jnp.int32),
                pltpu.VMEM((emb, seg), BF16),
                pltpu.VMEM((3, 8, GROUP, tw), BF16),
                pltpu.SemaphoreType.DMA((SLOTS,)),
                pltpu.SemaphoreType.DMA((3,)),
                pltpu.SemaphoreType.DMA((N_SEM,)),
                pltpu.SemaphoreType.DMA((N_SEM,)),
            ],
            compiler_params=pltpu.CompilerParams(
                collective_id=0, has_side_effects=True, vmem_limit_bytes=56 * 1024 * 1024),
        )(mask_blk, user_shard.T, item_shard.T, triples.T)
        vmem = pl.BlockSpec(memory_space=pltpu.VMEM)
        out_u, out_i, loss = pl.pallas_call(
            write_out, out_shape=results, in_specs=[vmem] * 3, out_specs=(vmem,) * 3,
        )(*found)
        return out_u.T, out_i.T, loss.reshape(batch)

    return jax.shard_map(
        device_body,
        mesh=mesh,
        in_specs=(P("row", "col"), P(("row", "col"), None), P(("col", "row"), None), P()),
        out_specs=(P(("row", "col"), None), P(("col", "row"), None), P()),
        check_vma=False,
    )
```

```python
import functools

import jax
import jax.numpy as jnp
from jax import lax
from jax.experimental import pallas as pl
from jax.experimental.pallas import tpu as pltpu
from jax.sharding import PartitionSpec as P

LAYERS = 3
ROWS = 8
COLS = 4
SLOTS = 4
CHUNKS = 16
STRIP = 32
EARLY = 6
RELAY0 = 13
GROUP = 256
OFFSET = 256.0
MESH_ID = pl.DeviceIdType.MESH
F32 = jnp.float32
BF16 = jnp.bfloat16

DEG = 0
UDEG = 28
AG = 31
ZAG = AG + 30
ZRS = ZAG + 9
RS_D = ZRS + 9
RS_1 = RS_D + 12
RS_2 = RS_1 + 12
OUZ = RS_2 + 6
OUR = OUZ + 3
MGZ = OUR + 28
MGR = MGZ + 6
N_SEM = MGR + 14


def nt_dot(a, b):
    return lax.dot_general(a, b, (((1,), (1,)), ((), ())), preferred_element_type=F32)


def kernel(mask_hbm, eu_hbm, ei_hbm, ids_hbm, outu_hbm, outi_hbm, loss_hbm,
           a_ref, mbuf, deg_own, deg_out, deg_in, deg_inv, udeg_part, udeg_own, udeg_in, su_ref,
           part, d_in, r1_in, r2_in, eig, eug, pu_acc, pu, pu_in, tot_i, tot_u,
           items_lo, up_rows, down_rows, u_rows, mg, mg_z, mg_zsum, mg_r, ids_ref, outi_ref, hot_ref,
           copy_sem, in_sem, send_sem, recv_sem):
    emb, seg = tot_i.shape
    users, block = a_ref.shape
    ush = tot_u.shape[1]
    cw = block // CHUNKS
    dw = block // 32
    row = lax.axis_index("row")
    col = lax.axis_index("col")
    core = lax.rem(row, 2)
    quad = row // 2
    partner = row + 1 - 2 * core
    at_x, at_y = lax.rem(quad, 2), quad // 2
    half = emb // 2
    sent = []

    def flipped(j):
        fx, fy = (j % 2 if isinstance(j, int) else lax.rem(j, 2)), j // 2
        return (at_y + fy - 2 * at_y * fy) * 2 + at_x + fx - 2 * at_x * fx

    x_row, y_row = 2 * flipped(1) + core, 2 * flipped(2) + core

    def remote(src, dst, idx, **where):
        return pltpu.make_async_remote_copy(
            src_ref=src, dst_ref=dst, send_sem=send_sem.at[idx], recv_sem=recv_sem.at[idx],
            device_id=where, device_id_type=MESH_ID)

    def send(src, dst, idx, **where):
        copy = remote(src, dst, idx, **where)
        copy.start()
        sent.append(copy)

    def arrived(dst, idx):
        remote(dst, dst, idx, row=row).wait_recv()

    def mask_copy(j):
        return pltpu.make_async_copy(
            mask_hbm.at[:, pl.ds(j * cw, cw)], mbuf.at[j % SLOTS], copy_sem.at[j % SLOTS])

    small = [
        pltpu.make_async_copy(eu_hbm, eug.at[0, col], in_sem.at[0]),
        pltpu.make_async_copy(ei_hbm, eig.at[0, row], in_sem.at[1]),
        pltpu.make_async_copy(ids_hbm, ids_ref, in_sem.at[2]),
    ]
    small[0].start()
    small[1].start()
    for j in range(SLOTS):
        mask_copy(j).start()
    small[2].start()

    barrier = pltpu.get_barrier_semaphore()
    for k in range(1, ROWS):
        pl.semaphore_signal(barrier, inc=1, device_id={"row": lax.rem(row + k, ROWS)}, device_id_type=MESH_ID)
    for k in range(1, COLS):
        pl.semaphore_signal(barrier, inc=1, device_id={"col": lax.rem(col + k, COLS)}, device_id_type=MESH_ID)

    lo, hi = pl.ds(0, half), pl.ds(half, half)
    d_row = 2 * flipped(3) + core

    def items_out(layer):
        base = AG + 10 * layer
        low, high = eig.at[layer, row, lo], eig.at[layer, row, hi]
        send(low, low, base, row=x_row)
        send(high, high, base + 1, row=y_row)
        send(high, high, base + 2, row=x_row)
        send(low, low, base + 3, row=y_row)
        send(eig.at[layer, row], eig.at[layer, row], base + 6, row=partner)

    def items_relay(layer):
        base = AG + 10 * layer
        low, high = eig.at[layer, x_row, lo], eig.at[layer, y_row, hi]
        arrived(low, base)
        send(low, low, base + 4, row=y_row)
        arrived(high, base + 1)
        send(high, high, base + 5, row=x_row)

    def items_near(layer):
        base = AG + 10 * layer
        arrived(eig.at[layer, x_row, hi], base + 2)
        send(eig.at[layer, x_row], eig.at[layer, x_row], base + 7, row=partner)
        arrived(eig.at[layer, y_row, lo], base + 3)
        send(eig.at[layer, y_row], eig.at[layer, y_row], base + 8, row=partner)

    def items_far(layer):
        base = AG + 10 * layer
        arrived(eig.at[layer, d_row, lo], base + 4)
        arrived(eig.at[layer, d_row, hi], base + 5)
        remote(eig.at[layer, d_row], eig.at[layer, d_row], base + 9, row=partner).start()

    def items_from_partner(layer, j):
        arrived(eig.at[layer, 2 * flipped(j) + 1 - core], AG + 10 * layer + 6 + j)

    def users_out(layer):
        src = eug.at[layer, col]
        for k in range(1, COLS):
            send(src, src, ZAG + 3 * layer + k - 1, col=lax.rem(col + k, COLS))

    def users_in(layer):
        for k in range(COLS - 1):
            arrived(eug.at[layer, 0], ZAG + 3 * layer + k)

    udeg_part[...] = jnp.zeros_like(udeg_part)
    udeg_own[...] = jnp.zeros_like(udeg_own)
    ready = {max(4 * g + 3, EARLY - 1): (g,) for g in range(4)}
    for j in range(CHUNKS):
        with jax.named_scope("mask_wait"):
            mask_copy(j).wait()

        def strip(s, acc, j=j):
            rows = pl.ds(pl.multiple_of(s * STRIP, STRIP), STRIP)
            m = mbuf[j % SLOTS, rows, :].astype(F32)
            a_ref[rows, j * cw:(j + 1) * cw] = m.astype(BF16)
            lanes = m[:, 0:128]
            for t in range(1, cw // 128):
                lanes = lanes + m[:, t * 128:(t + 1) * 128]
            udeg_part[rows, :] = udeg_part[rows, :] + lanes
            for t in range(STRIP // 8):
                acc = acc + m[t * 8:(t + 1) * 8, :]
            return acc

        acc = lax.fori_loop(0, users // STRIP, strip, jnp.zeros((8, cw), F32))
        if j + SLOTS < CHUNKS:
            mask_copy(j + SLOTS).start()
        total = jnp.sum(acc, axis=0, keepdims=True)
        deg_own[2 * j:2 * j + 1, :] = total[:, :dw]
        deg_own[2 * j + 1:2 * j + 2, :] = total[:, dw:]
        if j == EARLY - 1:
            with jax.named_scope("barrier"):
                pl.semaphore_wait(barrier, ROWS + COLS - 2)
            small[0].wait()
            users_out(0)
            small[1].wait()
            items_out(0)
        if j == RELAY0:
            with jax.named_scope("relay"):
                items_relay(0)
        for g in ready.get(j, ()):
            deg_out[g] = (deg_own[8 * g:8 * g + 8, :] - OFFSET).astype(BF16)
            for k in range(1, ROWS):
                send(deg_out.at[g], deg_in.at[k, g],
                     DEG + 7 * g + k - 1, row=lax.rem(row + k, ROWS))

    counts = nt_dot(jnp.ones((8, 128), BF16), udeg_part[...].astype(BF16))
    for b in range(users // 128):
        udeg_own[b:b + 1, :] = counts[0:1, b * 128:(b + 1) * 128]
    for k in range(1, COLS):
        send(udeg_own, udeg_in.at[k], UDEG + k - 1, col=lax.rem(col + k, COLS))
    tot_u[...] = eug[0, col].astype(F32)
    tot_i[...] = eig[0, row].astype(F32)
    small[2].wait()
    batch = ids_ref.shape[1]
    n_chunks, tw = up_rows.shape[0], up_rows.shape[2]

    def ids_of(which, ch):
        return ids_ref[which:which + 1, pl.ds(pl.multiple_of(ch * tw, 128), tw)]

    def make_hot(ch, carry):
        for which in range(3):
            low_bits = lax.rem(ids_of(which, ch), GROUP)
            same = lax.broadcasted_iota(jnp.int32, (GROUP, tw), 0) == low_bits
            hot_ref[which, ch] = jnp.where(same, 1.0, 0.0).astype(BF16)
        return carry

    with jax.named_scope("make_hot"):
        lax.fori_loop(0, n_chunks, make_hot, 0)
    users_in(0)
    with jax.named_scope("items0"):
        items_near(0)
        items_far(0)
        for k in range(4):
            items_from_partner(0, k)
    with jax.named_scope("udeg_wait"):
        for k in range(1, COLS):
            arrived(udeg_in.at[k], UDEG + k - 1)
    du = udeg_own[...] + udeg_in[1] + udeg_in[2] + udeg_in[3]
    su = lax.rsqrt(jnp.maximum(du, 1.0))
    for b in range(users // 128):
        wide = jnp.broadcast_to(su[b:b + 1, :], (128, 128))
        su_ref[b * 128:(b + 1) * 128, :] = wide.T
    with jax.named_scope("ideg_wait"):
        for g in range(4):
            for k in range(1, ROWS):
                arrived(deg_in.at[k, g], DEG + 7 * g + k - 1)
    for g in range(4):
        di = deg_own[8 * g:8 * g + 8, :] + OFFSET * (ROWS - 1)
        for k in range(1, ROWS):
            di = di + deg_in[k, g].astype(F32)
        deg_inv[8 * g:8 * g + 8, :] = lax.rsqrt(jnp.maximum(di, 1.0))

    def users_all(layer):
        return jnp.concatenate([eug[layer, c] for c in range(COLS)], axis=1)

    def seg_lanes(s, start=0, width=seg):
        return pl.ds(pl.multiple_of(s * seg + start, 128), width)

    def item_dot(layer, s, eu_all):
        for h in range(2):
            part[layer, s, :, h * cw:(h + 1) * cw] = jnp.dot(
                eu_all, a_ref[:, seg_lanes(s, h * cw, cw)], preferred_element_type=F32)

    def d_copy(layer, i, s):
        return remote(part.at[layer, s], d_in.at[layer, i], RS_D + 4 * layer + i, row=partner)

    def x_first(layer, i, s):
        return remote(part.at[layer, s, lo], r1_in.at[layer, i // 2], RS_1 + 4 * layer + i // 2, row=x_row)

    def y_first(layer, i, s):
        return remote(part.at[layer, s, hi], r1_in.at[layer, 2 + i], RS_1 + 4 * layer + 2 + i, row=y_row)

    def plane_start(layer, i, s):
        arrived(d_in.at[layer, i], RS_D + 4 * layer + i)
        part[layer, s] = part[layer, s] + d_in[layer, i]

        @pl.when(jnp.logical_or(i == 0, i == 2))
        def _():
            x_first(layer, i, s).start()

        @pl.when(i < 2)
        def _():
            y_first(layer, i, s).start()

    def item_product(layer, between=None):
        eu_all = users_all(layer)

        def other(i, carry):
            s0, s1 = 2 * flipped(3 - 2 * i) + 1 - core, 2 * flipped(2 - 2 * i) + 1 - core
            item_dot(layer, s0, eu_all)
            item_dot(layer, s1, eu_all)
            d_copy(layer, 2 * i, s0).start()
            d_copy(layer, 2 * i + 1, s1).start()
            return carry

        def own(i, carry):
            s0, s1 = 2 * flipped(3 - 2 * i) + core, 2 * flipped(2 - 2 * i) + core
            item_dot(layer, s0, eu_all)
            item_dot(layer, s1, eu_all)
            plane_start(layer, 2 * i, s0)
            plane_start(layer, 2 * i + 1, s1)
            return carry

        with jax.named_scope("item_other"):
            lax.fori_loop(0, 2, other, 0)
        if between is not None:
            between()
        with jax.named_scope("item_own"):
            lax.fori_loop(0, 2, own, 0)

    def plane_second(layer):
        base = RS_1 + 4 * layer
        arrived(r1_in.at[layer, 0], base)
        part[layer, y_row, lo] = part[layer, y_row, lo] + r1_in[layer, 0]
        send(part.at[layer, y_row, lo], r2_in.at[layer, 0], RS_2 + 2 * layer, row=y_row)
        arrived(r1_in.at[layer, 2], base + 2)
        part[layer, x_row, hi] = part[layer, x_row, hi] + r1_in[layer, 2]
        send(part.at[layer, x_row, hi], r2_in.at[layer, 1], RS_2 + 2 * layer + 1, row=x_row)

    def plane_last(layer):
        base = RS_1 + 4 * layer
        arrived(r1_in.at[layer, 1], base + 1)
        arrived(r1_in.at[layer, 3], base + 3)
        arrived(r2_in.at[layer, 0], RS_2 + 2 * layer)
        arrived(r2_in.at[layer, 1], RS_2 + 2 * layer + 1)
        low = part[layer, row, lo] + r1_in[layer, 1] + r2_in[layer, 0]
        high = part[layer, row, hi] + r1_in[layer, 3] + r2_in[layer, 1]
        cur = jnp.concatenate([low, high], axis=0).astype(BF16)
        if layer + 1 < LAYERS:
            eig[layer + 1, row] = cur
            items_out(layer + 1)
        tot_i[...] = tot_i[...] + cur.astype(F32)

    def user_dots(layer, j):
        s0 = 2 * flipped(j)
        both = nt_dot(a_ref[:, seg_lanes(s0)], eig[layer, s0])
        both = both + nt_dot(a_ref[:, seg_lanes(s0 + 1)], eig[layer, s0 + 1])
        pu_acc[:, 0:emb] = pu_acc[:, 0:emb] + both

    def user_own_chip(layer):
        pu_acc[...] = jnp.zeros_like(pu_acc)
        items_from_partner(layer, 0)
        user_dots(layer, 0)

    def user_chip(layer, j):
        items_from_partner(layer, j)
        user_dots(layer, j)

    def users_reduce_out(layer):
        for c in range(COLS):
            pu[layer, c] = pu_acc[c * ush:(c + 1) * ush, :].T[:emb, :]
        for k in range(1, COLS):
            peer = lax.rem(col + k, COLS)
            send(pu.at[layer, peer], pu_in.at[layer, k], ZRS + 3 * layer + k - 1, col=peer)

    def users_reduce_in(layer):
        for k in range(1, COLS):
            arrived(pu_in.at[layer, k], ZRS + 3 * layer + k - 1)
        total = pu[layer, col] + pu_in[layer, 1] + pu_in[layer, 2] + pu_in[layer, 3]
        cur = total.astype(BF16)
        if layer + 1 < LAYERS:
            eug[layer + 1, col] = cur
            users_out(layer + 1)
        tot_u[...] = tot_u[...] + cur.astype(F32)

    tile = 256
    eu_first = users_all(0)
    n_u = users // tile

    def first_segment(s):
        for h in range(seg // tile):
            cols = seg_lanes(s, h * tile, tile)
            start = h * tile
            inv = deg_inv[pl.ds(s * (seg // dw) + start // dw, 1), start % dw:start % dw + tile]
            items = eig[0, s, :, start:start + tile]
            got = None
            for u in range(n_u):
                rows = slice(u * tile, (u + 1) * tile)
                wide = jnp.concatenate([su_ref[rows, :]] * (tile // 128), axis=1)
                block_a = a_ref[rows, cols] * (wide * inv).astype(BF16)
                a_ref[rows, cols] = block_a
                more = jnp.dot(eu_first[:, rows], block_a, preferred_element_type=F32)
                got = more if got is None else got + more
                pu_acc[rows, 0:emb] = pu_acc[rows, 0:emb] + nt_dot(block_a, items)
            part[0, s, :, start:start + tile] = got

    def first_pair(i, carry):
        theirs, mine = 2 * flipped(3 - i) + 1 - core, 2 * flipped(3 - i) + core
        first_segment(theirs)
        d_copy(0, i, theirs).start()

        @pl.when(i > 0)
        def _():
            plane_start(0, i - 1, 2 * flipped(4 - i) + core)

        first_segment(mine)
        return carry

    pu_acc[...] = jnp.zeros_like(pu_acc)
    with jax.named_scope("first"):
        lax.fori_loop(0, 4, first_pair, 0)
    with jax.named_scope("reduce_out0"):
        users_reduce_out(0)
    with jax.named_scope("second0"):
        plane_start(0, 3, row)
        plane_second(0)
    with jax.named_scope("reduce_in0"):
        users_reduce_in(0)
    with jax.named_scope("last0"):
        plane_last(0)
    with jax.named_scope("users_in1"):
        users_in(1)

    def relay_rows():
        with jax.named_scope("own_chip1"):
            user_own_chip(1)
        with jax.named_scope("relay1"):
            items_relay(1)

    item_product(1, relay_rows)
    with jax.named_scope("near1"):
        items_near(1)
        user_chip(1, 1)
    with jax.named_scope("far1"):
        items_far(1)
    with jax.named_scope("chip1"):
        user_chip(1, 2)
    with jax.named_scope("second1"):
        plane_second(1)
    with jax.named_scope("far_chip1"):
        user_chip(1, 3)
        users_reduce_out(1)
    with jax.named_scope("last1"):
        plane_last(1)
    with jax.named_scope("reduce_in1"):
        users_reduce_in(1)
    with jax.named_scope("own_chip2"):
        user_own_chip(2)
    with jax.named_scope("relay2"):
        items_relay(2)
    with jax.named_scope("users_in2"):
        users_in(2)

    def near_rows():
        with jax.named_scope("near2"):
            items_near(2)

    item_product(2, near_rows)
    with jax.named_scope("far2"):
        items_far(2)
    with jax.named_scope("near_chips2"):
        user_chip(2, 1)
        user_chip(2, 2)
    with jax.named_scope("far_chip2"):
        user_chip(2, 3)
        users_reduce_out(2)
    with jax.named_scope("second2"):
        plane_second(2)
    with jax.named_scope("reduce_in2"):
        users_reduce_in(2)
    scale = 1.0 / (LAYERS + 1)
    u_rows[row, col] = (tot_u[...] * scale).astype(BF16)
    for k in range(1, COLS):
        send(u_rows.at[row, col], u_rows.at[row, col], OUZ + k - 1, col=lax.rem(col + k, COLS))
    def users_over_plane(piece):
        ref = u_rows.at[row, lax.rem(col + COLS - piece, COLS)]
        for k in range(1, ROWS):
            send(ref, ref, OUR + 7 * piece + k - 1, row=lax.rem(row + k, ROWS))

    users_over_plane(0)
    out_copy = [pltpu.make_async_copy(u_rows.at[row, col], outu_hbm, in_sem.at[0])]
    out_copy[0].start()

    def pick(tables, which, ch, first):
        hot = hot_ref[which, ch]
        high_bits = ids_of(which, ch) // GROUP - first
        acc = jnp.zeros((emb, tw), F32)
        for b, table in enumerate(tables):
            got = jnp.dot(table(), hot, preferred_element_type=F32)
            for i in range(4):
                acc = acc + jnp.where(high_bits == b * 4 + i, got[i * emb:(i + 1) * emb, :], 0.0)
        return acc

    with jax.named_scope("plane_last2"):
        plane_last(2)
    out_item = (tot_i[...] * scale).astype(BF16)
    outi_ref[...] = out_item
    out_copy.append(pltpu.make_async_copy(outi_ref, outi_hbm, in_sem.at[1]))
    out_copy[1].start()
    n_lo = seg // GROUP
    for b in range(n_lo):
        items_lo[b] = out_item[:, b * GROUP:(b + 1) * GROUP]
    first = (col * ROWS + row) * n_lo

    with jax.named_scope("ouz_wait"):
        for k in range(1, COLS):
            arrived(u_rows.at[row, 0], OUZ + k - 1)
            users_over_plane(k)

    def pick_items(ch, carry):
        tables = [lambda b=b: items_lo[4 * b:4 * b + 4].reshape(4 * emb, GROUP) for b in range(n_lo // 4)]
        up_rows[ch] = pick(tables, 1, ch, first)
        down_rows[ch] = pick(tables, 2, ch, first)
        return carry

    with jax.named_scope("pick_items"):
        lax.fori_loop(0, n_chunks, pick_items, 0)
    with jax.named_scope("our_wait"):
        for k in range(7 * COLS):
            arrived(u_rows.at[0, 0], OUR + k)

    def user_table(b):
        parts = []
        for i in range(4):
            r, c = (4 * b + i) // 2, 2 * (i % 2)
            parts.append(jnp.concatenate([u_rows[r, c], u_rows[r, c + 1]], axis=1))
        return jnp.concatenate(parts, axis=0)

    def score(pair, carry):
        tables = [lambda b=b: user_table(b) for b in range(ROWS * COLS // 8)]
        for ch in (2 * pair, 2 * pair + 1):
            vec = pick(tables, 0, ch, 0)
            up = jnp.sum(vec * up_rows[ch], axis=0, keepdims=True)
            down = jnp.sum(vec * down_rows[ch], axis=0, keepdims=True)
            diff = up - down
            for t in range(tw // 128):
                mg[pl.ds(ch * (tw // 128) + t, 1), :] = diff[:, t * 128:(t + 1) * 128]
        return carry

    n_rows = mg.shape[0] // 2
    halves = [pl.ds(0, n_rows), pl.ds(n_rows, n_rows)]
    for h, rows in enumerate(halves):
        with jax.named_scope("score"):
            lax.fori_loop(0, n_chunks // 4, lambda p, c, h=h: score(p + h * (n_chunks // 4), c), 0)
        for k in range(1, COLS):
            send(mg.at[rows], mg_z.at[k, rows], MGZ + 3 * h + k - 1, col=lax.rem(col + k, COLS))
    for h, rows in enumerate(halves):
        with jax.named_scope("mgz_wait"):
            for k in range(1, COLS):
                arrived(mg_z.at[k, rows], MGZ + 3 * h + k - 1)
        mg_zsum[rows] = mg[rows] + mg_z[1, rows] + mg_z[2, rows] + mg_z[3, rows]
        for k in range(1, ROWS):
            send(mg_zsum.at[rows], mg_r.at[k, rows], MGR + 7 * h + k - 1, row=lax.rem(row + k, ROWS))
    with jax.named_scope("mgr_wait"):
        for h, rows in enumerate(halves):
            for k in range(1, ROWS):
                arrived(mg_r.at[k, rows], MGR + 7 * h + k - 1)
    margin = mg_zsum[...]
    for k in range(1, ROWS):
        margin = margin + mg_r[k]
    mg_z[0] = jnp.maximum(-margin, 0.0) + jnp.log1p(jnp.exp(-jnp.abs(margin)))
    out_copy.append(pltpu.make_async_copy(mg_z.at[0], loss_hbm, in_sem.at[2]))
    out_copy[2].start()

    for layer in range(LAYERS):
        for i in range(4):
            d_copy(layer, i, row).wait_send()
        for i in range(2):
            x_first(layer, 2 * i, row).wait_send()
            y_first(layer, i, row).wait_send()
        remote(eig.at[layer, row], eig.at[layer, row], AG + 10 * layer + 9, row=partner).wait_send()
    for copy in sent:
        copy.wait_send()
    for copy in out_copy:
        copy.wait()


def write_out(u_ref, i_ref, l_ref, u_out, i_out, l_out):
    u_out[...] = u_ref[...]
    i_out[...] = i_ref[...]
    l_out[...] = l_ref[...]


def solution(mesh):
    def device_body(mask_blk, user_shard, item_shard, triples):
        users, block = mask_blk.shape
        assert users <= 2 * OFFSET and block <= 128 * 256
        emb = user_shard.shape[1]
        ush, seg = user_shard.shape[0], item_shard.shape[0]
        batch = triples.shape[0]
        tw = batch // 8
        dw = block // 32
        hbm = pl.BlockSpec(memory_space=pl.ANY)
        loss_shape = (batch // 128, 128)
        results = (
            jax.ShapeDtypeStruct((emb, ush), BF16),
            jax.ShapeDtypeStruct((emb, seg), BF16),
            jax.ShapeDtypeStruct(loss_shape, F32),
        )
        found = pl.pallas_call(
            kernel,
            out_shape=results,
            in_specs=[pl.BlockSpec(memory_space=pltpu.HBM)] * 4,
            out_specs=(hbm,) * 3,
            scratch_shapes=[
                pltpu.VMEM((users, block), BF16),
                pltpu.VMEM((SLOTS, users, block // CHUNKS), jnp.int32),
                pltpu.VMEM((32, dw), F32),
                pltpu.VMEM((4, 8, dw), BF16),
                pltpu.VMEM((ROWS, 4, 8, dw), BF16),
                pltpu.VMEM((32, dw), F32),
                pltpu.VMEM((users, 128), F32),
                pltpu.VMEM((8, 128), F32),
                pltpu.VMEM((COLS, 8, 128), F32),
                pltpu.VMEM((users, 128), F32),
                pltpu.VMEM((LAYERS, ROWS, emb, seg), F32),
                pltpu.VMEM((LAYERS, 4, emb, seg), F32),
                pltpu.VMEM((LAYERS, 4, emb // 2, seg), F32),
                pltpu.VMEM((LAYERS, 2, emb // 2, seg), F32),
                pltpu.VMEM((LAYERS, ROWS, emb, seg), BF16),
                pltpu.VMEM((LAYERS, COLS, emb, ush), BF16),
                pltpu.VMEM((users, 128), F32),
                pltpu.VMEM((LAYERS, COLS, emb, ush), F32),
                pltpu.VMEM((LAYERS, COLS, emb, ush), F32),
                pltpu.VMEM((emb, seg), F32),
                pltpu.VMEM((emb, ush), F32),
                pltpu.VMEM((seg // GROUP, emb, GROUP), BF16),
                pltpu.VMEM((8, emb, tw), F32),
                pltpu.VMEM((8, emb, tw), F32),
                pltpu.VMEM((ROWS, COLS, emb, ush), BF16),
                pltpu.VMEM(loss_shape, F32),
                pltpu.VMEM((COLS,) + loss_shape, F32),
                pltpu.VMEM(loss_shape, F32),
                pltpu.VMEM((ROWS,) + loss_shape, F32),
                pltpu.VMEM((3, batch), jnp.int32),
                pltpu.VMEM((emb, seg), BF16),
                pltpu.VMEM((3, 8, GROUP, tw), BF16),
                pltpu.SemaphoreType.DMA((SLOTS,)),
                pltpu.SemaphoreType.DMA((3,)),
                pltpu.SemaphoreType.DMA((N_SEM,)),
                pltpu.SemaphoreType.DMA((N_SEM,)),
            ],
            compiler_params=pltpu.CompilerParams(
                collective_id=0, has_side_effects=True, vmem_limit_bytes=56 * 1024 * 1024),
        )(mask_blk, user_shard.T, item_shard.T, triples.T)
        vmem = pl.BlockSpec(memory_space=pltpu.VMEM)
        out_u, out_i, loss = pl.pallas_call(
            write_out, out_shape=results, in_specs=[vmem] * 3, out_specs=(vmem,) * 3,
        )(*found)
        return out_u.T, out_i.T, loss.reshape(batch)

    return jax.shard_map(
        device_body,
        mesh=mesh,
        in_specs=(P("row", "col"), P(("row", "col"), None), P(("col", "row"), None), P()),
        out_specs=(P(("row", "col"), None), P(("col", "row"), None), P()),
        check_vma=False,
    )
```

```python
import functools

import jax
import jax.numpy as jnp
from jax import lax
from jax.experimental import pallas as pl
from jax.experimental.pallas import tpu as pltpu
from jax.sharding import PartitionSpec as P

LAYERS = 3
ROWS = 8
COLS = 4
SLOTS = 4
CHUNKS = 16
STRIP = 32
EARLY = 6
RELAY0 = 13
GROUP = 256
OFFSET = 256.0
MESH_ID = pl.DeviceIdType.MESH
F32 = jnp.float32
BF16 = jnp.bfloat16

DEG = 0
UDEG = 28
AG = 31
ZAG = AG + 30
ZRS = ZAG + 9
RS_D = ZRS + 9
RS_1 = RS_D + 12
RS_2 = RS_1 + 12
OUZ = RS_2 + 6
OUR = OUZ + 3
MGZ = OUR + 28
MGR = MGZ + 6
N_SEM = MGR + 14


def nt_dot(a, b):
    return lax.dot_general(a, b, (((1,), (1,)), ((), ())), preferred_element_type=F32)


def kernel(mask_hbm, eu_hbm, ei_hbm, ids_hbm, outu_hbm, outi_hbm, loss_hbm,
           a_ref, mbuf, deg_own, deg_out, deg_in, deg_inv, udeg_part, udeg_own, udeg_in, su_ref,
           part, d_in, r1_in, r2_in, eig, eug, pu_acc, pu, pu_in, tot_i, tot_u,
           items_lo, up_rows, down_rows, u_rows, mg, mg_z, mg_zsum, mg_r, ids_ref, outi_ref, hot_ref,
           copy_sem, in_sem, send_sem, recv_sem):
    emb, seg = tot_i.shape
    users, block = a_ref.shape
    ush = tot_u.shape[1]
    cw = block // CHUNKS
    dw = block // 32
    row = lax.axis_index("row")
    col = lax.axis_index("col")
    core = lax.rem(row, 2)
    quad = row // 2
    partner = row + 1 - 2 * core
    at_x, at_y = lax.rem(quad, 2), quad // 2
    half = emb // 2
    sent = []

    def flipped(j):
        fx, fy = (j % 2 if isinstance(j, int) else lax.rem(j, 2)), j // 2
        return (at_y + fy - 2 * at_y * fy) * 2 + at_x + fx - 2 * at_x * fx

    x_row, y_row = 2 * flipped(1) + core, 2 * flipped(2) + core

    def remote(src, dst, idx, **where):
        return pltpu.make_async_remote_copy(
            src_ref=src, dst_ref=dst, send_sem=send_sem.at[idx], recv_sem=recv_sem.at[idx],
            device_id=where, device_id_type=MESH_ID)

    def send(src, dst, idx, **where):
        copy = remote(src, dst, idx, **where)
        copy.start()
        sent.append(copy)

    def arrived(dst, idx):
        remote(dst, dst, idx, row=row).wait_recv()

    def mask_copy(j):
        return pltpu.make_async_copy(
            mask_hbm.at[:, pl.ds(j * cw, cw)], mbuf.at[j % SLOTS], copy_sem.at[j % SLOTS])

    small = [
        pltpu.make_async_copy(eu_hbm, eug.at[0, col], in_sem.at[0]),
        pltpu.make_async_copy(ei_hbm, eig.at[0, row], in_sem.at[1]),
        pltpu.make_async_copy(ids_hbm, ids_ref, in_sem.at[2]),
    ]
    small[0].start()
    small[1].start()
    for j in range(SLOTS):
        mask_copy(j).start()
    small[2].start()

    barrier = pltpu.get_barrier_semaphore()
    for k in range(1, ROWS):
        pl.semaphore_signal(barrier, inc=1, device_id={"row": lax.rem(row + k, ROWS)}, device_id_type=MESH_ID)
    for k in range(1, COLS):
        pl.semaphore_signal(barrier, inc=1, device_id={"col": lax.rem(col + k, COLS)}, device_id_type=MESH_ID)

    lo, hi = pl.ds(0, half), pl.ds(half, half)
    d_row = 2 * flipped(3) + core

    def items_out(layer):
        base = AG + 10 * layer
        low, high = eig.at[layer, row, lo], eig.at[layer, row, hi]
        send(low, low, base, row=x_row)
        send(high, high, base + 1, row=y_row)
        send(high, high, base + 2, row=x_row)
        send(low, low, base + 3, row=y_row)
        send(eig.at[layer, row], eig.at[layer, row], base + 6, row=partner)

    def items_relay(layer):
        base = AG + 10 * layer
        low, high = eig.at[layer, x_row, lo], eig.at[layer, y_row, hi]
        arrived(low, base)
        send(low, low, base + 4, row=y_row)
        arrived(high, base + 1)
        send(high, high, base + 5, row=x_row)

    def items_near(layer):
        base = AG + 10 * layer
        arrived(eig.at[layer, x_row, hi], base + 2)
        send(eig.at[layer, x_row], eig.at[layer, x_row], base + 7, row=partner)
        arrived(eig.at[layer, y_row, lo], base + 3)
        send(eig.at[layer, y_row], eig.at[layer, y_row], base + 8, row=partner)

    def items_far(layer):
        base = AG + 10 * layer
        arrived(eig.at[layer, d_row, lo], base + 4)
        arrived(eig.at[layer, d_row, hi], base + 5)
        remote(eig.at[layer, d_row], eig.at[layer, d_row], base + 9, row=partner).start()

    def items_from_partner(layer, j):
        arrived(eig.at[layer, 2 * flipped(j) + 1 - core], AG + 10 * layer + 6 + j)

    def users_out(layer):
        src = eug.at[layer, col]
        for k in range(1, COLS):
            send(src, src, ZAG + 3 * layer + k - 1, col=lax.rem(col + k, COLS))

    def users_in(layer):
        for k in range(COLS - 1):
            arrived(eug.at[layer, 0], ZAG + 3 * layer + k)

    udeg_part[...] = jnp.zeros_like(udeg_part)
    udeg_own[...] = jnp.zeros_like(udeg_own)
    ready = {max(4 * g + 3, EARLY - 1): (g,) for g in range(4)}
    for j in range(CHUNKS):
        with jax.named_scope("mask_wait"):
            mask_copy(j).wait()

        def strip(s, acc, j=j):
            rows = pl.ds(pl.multiple_of(s * STRIP, STRIP), STRIP)
            m = mbuf[j % SLOTS, rows, :].astype(F32)
            a_ref[rows, j * cw:(j + 1) * cw] = m.astype(BF16)
            lanes = m[:, 0:128]
            for t in range(1, cw // 128):
                lanes = lanes + m[:, t * 128:(t + 1) * 128]
            udeg_part[rows, :] = udeg_part[rows, :] + lanes
            for t in range(STRIP // 8):
                acc = acc + m[t * 8:(t + 1) * 8, :]
            return acc

        acc = lax.fori_loop(0, users // STRIP, strip, jnp.zeros((8, cw), F32))
        if j + SLOTS < CHUNKS:
            mask_copy(j + SLOTS).start()
        total = jnp.sum(acc, axis=0, keepdims=True)
        deg_own[2 * j:2 * j + 1, :] = total[:, :dw]
        deg_own[2 * j + 1:2 * j + 2, :] = total[:, dw:]
        if j == EARLY - 1:
            with jax.named_scope("barrier"):
                pl.semaphore_wait(barrier, ROWS + COLS - 2)
            small[0].wait()
            users_out(0)
            small[1].wait()
            items_out(0)
        if j == RELAY0:
            with jax.named_scope("relay"):
                items_relay(0)
        for g in ready.get(j, ()):
            deg_out[g] = (deg_own[8 * g:8 * g + 8, :] - OFFSET).astype(BF16)
            for k in range(1, ROWS):
                send(deg_out.at[g], deg_in.at[k, g],
                     DEG + 7 * g + k - 1, row=lax.rem(row + k, ROWS))

    counts = nt_dot(jnp.ones((8, 128), BF16), udeg_part[...].astype(BF16))
    for b in range(users // 128):
        udeg_own[b:b + 1, :] = counts[0:1, b * 128:(b + 1) * 128]
    for k in range(1, COLS):
        send(udeg_own, udeg_in.at[k], UDEG + k - 1, col=lax.rem(col + k, COLS))
    tot_u[...] = eug[0, col].astype(F32)
    tot_i[...] = eig[0, row].astype(F32)
    small[2].wait()
    batch = ids_ref.shape[1]
    n_chunks, tw = up_rows.shape[0], up_rows.shape[2]

    def ids_of(which, ch):
        return ids_ref[which:which + 1, pl.ds(pl.multiple_of(ch * tw, 128), tw)]

    def make_hot(ch, carry):
        for which in range(3):
            low_bits = lax.rem(ids_of(which, ch), GROUP)
            same = lax.broadcasted_iota(jnp.int32, (GROUP, tw), 0) == low_bits
            hot_ref[which, ch] = jnp.where(same, 1.0, 0.0).astype(BF16)
        return carry

    with jax.named_scope("make_hot"):
        lax.fori_loop(0, n_chunks, make_hot, 0)
    users_in(0)
    with jax.named_scope("items0"):
        items_near(0)
        items_far(0)
        for k in range(4):
            items_from_partner(0, k)
    with jax.named_scope("udeg_wait"):
        for k in range(1, COLS):
            arrived(udeg_in.at[k], UDEG + k - 1)
    du = udeg_own[...] + udeg_in[1] + udeg_in[2] + udeg_in[3]
    su = lax.rsqrt(jnp.maximum(du, 1.0))
    for b in range(users // 128):
        wide = jnp.broadcast_to(su[b:b + 1, :], (128, 128))
        su_ref[b * 128:(b + 1) * 128, :] = wide.T
    with jax.named_scope("ideg_wait"):
        for g in range(4):
            for k in range(1, ROWS):
                arrived(deg_in.at[k, g], DEG + 7 * g + k - 1)
    for g in range(4):
        di = deg_own[8 * g:8 * g + 8, :] + OFFSET * (ROWS - 1)
        for k in range(1, ROWS):
            di = di + deg_in[k, g].astype(F32)
        deg_inv[8 * g:8 * g + 8, :] = lax.rsqrt(jnp.maximum(di, 1.0))

    def users_all(layer):
        return jnp.concatenate([eug[layer, c] for c in range(COLS)], axis=1)

    def seg_lanes(s, start=0, width=seg):
        return pl.ds(pl.multiple_of(s * seg + start, 128), width)

    def item_dot(layer, s, eu_all):
        for h in range(2):
            part[layer, s, :, h * cw:(h + 1) * cw] = jnp.dot(
                eu_all, a_ref[:, seg_lanes(s, h * cw, cw)], preferred_element_type=F32)

    def d_copy(layer, i, s):
        return remote(part.at[layer, s], d_in.at[layer, i], RS_D + 4 * layer + i, row=partner)

    def x_first(layer, i, s):
        return remote(part.at[layer, s, lo], r1_in.at[layer, i // 2], RS_1 + 4 * layer + i // 2, row=x_row)

    def y_first(layer, i, s):
        return remote(part.at[layer, s, hi], r1_in.at[layer, 2 + i], RS_1 + 4 * layer + 2 + i, row=y_row)

    def plane_start(layer, i, s):
        arrived(d_in.at[layer, i], RS_D + 4 * layer + i)
        part[layer, s] = part[layer, s] + d_in[layer, i]

        @pl.when(jnp.logical_or(i == 0, i == 2))
        def _():
            x_first(layer, i, s).start()

        @pl.when(i < 2)
        def _():
            y_first(layer, i, s).start()

    def item_product(layer, between=None):
        eu_all = users_all(layer)

        def other(i, carry):
            s0, s1 = 2 * flipped(3 - 2 * i) + 1 - core, 2 * flipped(2 - 2 * i) + 1 - core
            item_dot(layer, s0, eu_all)
            item_dot(layer, s1, eu_all)
            d_copy(layer, 2 * i, s0).start()
            d_copy(layer, 2 * i + 1, s1).start()
            return carry

        def own(i, carry):
            s0, s1 = 2 * flipped(3 - 2 * i) + core, 2 * flipped(2 - 2 * i) + core
            item_dot(layer, s0, eu_all)
            item_dot(layer, s1, eu_all)
            plane_start(layer, 2 * i, s0)
            plane_start(layer, 2 * i + 1, s1)
            return carry

        with jax.named_scope("item_other"):
            lax.fori_loop(0, 2, other, 0)
        if between is not None:
            between()
        with jax.named_scope("item_own"):
            lax.fori_loop(0, 2, own, 0)

    def plane_second(layer):
        base = RS_1 + 4 * layer
        arrived(r1_in.at[layer, 0], base)
        part[layer, y_row, lo] = part[layer, y_row, lo] + r1_in[layer, 0]
        send(part.at[layer, y_row, lo], r2_in.at[layer, 0], RS_2 + 2 * layer, row=y_row)
        arrived(r1_in.at[layer, 2], base + 2)
        part[layer, x_row, hi] = part[layer, x_row, hi] + r1_in[layer, 2]
        send(part.at[layer, x_row, hi], r2_in.at[layer, 1], RS_2 + 2 * layer + 1, row=x_row)

    def plane_last(layer):
        base = RS_1 + 4 * layer
        arrived(r1_in.at[layer, 1], base + 1)
        arrived(r1_in.at[layer, 3], base + 3)
        arrived(r2_in.at[layer, 0], RS_2 + 2 * layer)
        arrived(r2_in.at[layer, 1], RS_2 + 2 * layer + 1)
        low = part[layer, row, lo] + r1_in[layer, 1] + r2_in[layer, 0]
        high = part[layer, row, hi] + r1_in[layer, 3] + r2_in[layer, 1]
        cur = jnp.concatenate([low, high], axis=0).astype(BF16)
        if layer + 1 < LAYERS:
            eig[layer + 1, row] = cur
            items_out(layer + 1)
        tot_i[...] = tot_i[...] + cur.astype(F32)

    def user_dots(layer, j):
        s0 = 2 * flipped(j)
        both = nt_dot(a_ref[:, seg_lanes(s0)], eig[layer, s0])
        both = both + nt_dot(a_ref[:, seg_lanes(s0 + 1)], eig[layer, s0 + 1])
        pu_acc[:, 0:emb] = pu_acc[:, 0:emb] + both

    def user_own_chip(layer):
        pu_acc[...] = jnp.zeros_like(pu_acc)
        items_from_partner(layer, 0)
        user_dots(layer, 0)

    def user_chip(layer, j):
        items_from_partner(layer, j)
        user_dots(layer, j)

    def users_reduce_out(layer):
        for c in range(COLS):
            pu[layer, c] = pu_acc[c * ush:(c + 1) * ush, :].T[:emb, :]
        for k in range(1, COLS):
            peer = lax.rem(col + k, COLS)
            send(pu.at[layer, peer], pu_in.at[layer, k], ZRS + 3 * layer + k - 1, col=peer)

    def users_reduce_in(layer):
        for k in range(1, COLS):
            arrived(pu_in.at[layer, k], ZRS + 3 * layer + k - 1)
        total = pu[layer, col] + pu_in[layer, 1] + pu_in[layer, 2] + pu_in[layer, 3]
        cur = total.astype(BF16)
        if layer + 1 < LAYERS:
            eug[layer + 1, col] = cur
            users_out(layer + 1)
        tot_u[...] = tot_u[...] + cur.astype(F32)

    tile = 256
    eu_first = users_all(0)
    n_u = users // tile

    def first_segment(s):
        for h in range(seg // tile):
            cols = seg_lanes(s, h * tile, tile)
            start = h * tile
            inv = deg_inv[pl.ds(s * (seg // dw) + start // dw, 1), start % dw:start % dw + tile]
            items = eig[0, s, :, start:start + tile]
            got = None
            for u in range(n_u):
                rows = slice(u * tile, (u + 1) * tile)
                wide = jnp.concatenate([su_ref[rows, :]] * (tile // 128), axis=1)
                block_a = a_ref[rows, cols] * (wide * inv).astype(BF16)
                a_ref[rows, cols] = block_a
                more = jnp.dot(eu_first[:, rows], block_a, preferred_element_type=F32)
                got = more if got is None else got + more
                pu_acc[rows, 0:emb] = pu_acc[rows, 0:emb] + nt_dot(block_a, items)
            part[0, s, :, start:start + tile] = got

    def first_pair(i, carry):
        theirs, mine = 2 * flipped(3 - i) + 1 - core, 2 * flipped(3 - i) + core
        first_segment(theirs)
        d_copy(0, i, theirs).start()

        @pl.when(i > 0)
        def _():
            plane_start(0, i - 1, 2 * flipped(4 - i) + core)

        first_segment(mine)
        return carry

    pu_acc[...] = jnp.zeros_like(pu_acc)
    with jax.named_scope("first"):
        lax.fori_loop(0, 4, first_pair, 0)
    with jax.named_scope("reduce_out0"):
        users_reduce_out(0)
    with jax.named_scope("second0"):
        plane_start(0, 3, row)
        plane_second(0)
    with jax.named_scope("reduce_in0"):
        users_reduce_in(0)
    with jax.named_scope("last0"):
        plane_last(0)
    with jax.named_scope("users_in1"):
        users_in(1)

    def relay_rows():
        with jax.named_scope("own_chip1"):
            user_own_chip(1)
        with jax.named_scope("relay1"):
            items_relay(1)

    item_product(1, relay_rows)
    with jax.named_scope("near1"):
        items_near(1)
        user_chip(1, 1)
    with jax.named_scope("chip1"):
        user_chip(1, 2)
    with jax.named_scope("far1"):
        items_far(1)
    with jax.named_scope("far_chip1"):
        user_chip(1, 3)
        users_reduce_out(1)
    with jax.named_scope("second1"):
        plane_second(1)
    with jax.named_scope("last1"):
        plane_last(1)
    with jax.named_scope("reduce_in1"):
        users_reduce_in(1)
    with jax.named_scope("own_chip2"):
        user_own_chip(2)
    with jax.named_scope("relay2"):
        items_relay(2)
    with jax.named_scope("users_in2"):
        users_in(2)

    def near_rows():
        with jax.named_scope("near2"):
            items_near(2)

    item_product(2, near_rows)
    with jax.named_scope("far2"):
        items_far(2)
    with jax.named_scope("near_chips2"):
        user_chip(2, 1)
        user_chip(2, 2)
    with jax.named_scope("far_chip2"):
        user_chip(2, 3)
        users_reduce_out(2)
    with jax.named_scope("second2"):
        plane_second(2)
    with jax.named_scope("reduce_in2"):
        users_reduce_in(2)
    scale = 1.0 / (LAYERS + 1)
    u_rows[row, col] = (tot_u[...] * scale).astype(BF16)
    for k in range(1, COLS):
        send(u_rows.at[row, col], u_rows.at[row, col], OUZ + k - 1, col=lax.rem(col + k, COLS))
    def users_over_plane(piece):
        ref = u_rows.at[row, lax.rem(col + COLS - piece, COLS)]
        for k in range(1, ROWS):
            send(ref, ref, OUR + 7 * piece + k - 1, row=lax.rem(row + k, ROWS))

    users_over_plane(0)
    out_copy = [pltpu.make_async_copy(u_rows.at[row, col], outu_hbm, in_sem.at[0])]
    out_copy[0].start()

    def pick(tables, which, ch, first):
        hot = hot_ref[which, ch]
        high_bits = ids_of(which, ch) // GROUP - first
        acc = jnp.zeros((emb, tw), F32)
        for b, table in enumerate(tables):
            got = jnp.dot(table(), hot, preferred_element_type=F32)
            for i in range(4):
                acc = acc + jnp.where(high_bits == b * 4 + i, got[i * emb:(i + 1) * emb, :], 0.0)
        return acc

    with jax.named_scope("plane_last2"):
        plane_last(2)
    out_item = (tot_i[...] * scale).astype(BF16)
    outi_ref[...] = out_item
    out_copy.append(pltpu.make_async_copy(outi_ref, outi_hbm, in_sem.at[1]))
    out_copy[1].start()
    n_lo = seg // GROUP
    for b in range(n_lo):
        items_lo[b] = out_item[:, b * GROUP:(b + 1) * GROUP]
    first = (col * ROWS + row) * n_lo

    with jax.named_scope("ouz_wait"):
        for k in range(1, COLS):
            arrived(u_rows.at[row, 0], OUZ + k - 1)
            users_over_plane(k)

    def pick_items(ch, carry):
        tables = [lambda b=b: items_lo[4 * b:4 * b + 4].reshape(4 * emb, GROUP) for b in range(n_lo // 4)]
        up_rows[ch] = pick(tables, 1, ch, first)
        down_rows[ch] = pick(tables, 2, ch, first)
        return carry

    with jax.named_scope("pick_items"):
        lax.fori_loop(0, n_chunks, pick_items, 0)
    with jax.named_scope("our_wait"):
        for k in range(7 * COLS):
            arrived(u_rows.at[0, 0], OUR + k)

    def user_table(b):
        parts = []
        for i in range(4):
            r, c = (4 * b + i) // 2, 2 * (i % 2)
            parts.append(jnp.concatenate([u_rows[r, c], u_rows[r, c + 1]], axis=1))
        return jnp.concatenate(parts, axis=0)

    def score(pair, carry):
        tables = [lambda b=b: user_table(b) for b in range(ROWS * COLS // 8)]
        for ch in (2 * pair, 2 * pair + 1):
            vec = pick(tables, 0, ch, 0)
            up = jnp.sum(vec * up_rows[ch], axis=0, keepdims=True)
            down = jnp.sum(vec * down_rows[ch], axis=0, keepdims=True)
            diff = up - down
            for t in range(tw // 128):
                mg[pl.ds(ch * (tw // 128) + t, 1), :] = diff[:, t * 128:(t + 1) * 128]
        return carry

    n_rows = mg.shape[0] // 2
    halves = [pl.ds(0, n_rows), pl.ds(n_rows, n_rows)]
    for h, rows in enumerate(halves):
        with jax.named_scope("score"):
            lax.fori_loop(0, n_chunks // 4, lambda p, c, h=h: score(p + h * (n_chunks // 4), c), 0)
        for k in range(1, COLS):
            send(mg.at[rows], mg_z.at[k, rows], MGZ + 3 * h + k - 1, col=lax.rem(col + k, COLS))
    for h, rows in enumerate(halves):
        with jax.named_scope("mgz_wait"):
            for k in range(1, COLS):
                arrived(mg_z.at[k, rows], MGZ + 3 * h + k - 1)
        mg_zsum[rows] = mg[rows] + mg_z[1, rows] + mg_z[2, rows] + mg_z[3, rows]
        for k in range(1, ROWS):
            send(mg_zsum.at[rows], mg_r.at[k, rows], MGR + 7 * h + k - 1, row=lax.rem(row + k, ROWS))
    with jax.named_scope("mgr_wait"):
        for h, rows in enumerate(halves):
            for k in range(1, ROWS):
                arrived(mg_r.at[k, rows], MGR + 7 * h + k - 1)
    margin = mg_zsum[...]
    for k in range(1, ROWS):
        margin = margin + mg_r[k]
    mg_z[0] = jnp.maximum(-margin, 0.0) + jnp.log1p(jnp.exp(-jnp.abs(margin)))
    out_copy.append(pltpu.make_async_copy(mg_z.at[0], loss_hbm, in_sem.at[2]))
    out_copy[2].start()

    for layer in range(LAYERS):
        for i in range(4):
            d_copy(layer, i, row).wait_send()
        for i in range(2):
            x_first(layer, 2 * i, row).wait_send()
            y_first(layer, i, row).wait_send()
        remote(eig.at[layer, row], eig.at[layer, row], AG + 10 * layer + 9, row=partner).wait_send()
    for copy in sent:
        copy.wait_send()
    for copy in out_copy:
        copy.wait()


def write_out(u_ref, i_ref, l_ref, u_out, i_out, l_out):
    u_out[...] = u_ref[...]
    i_out[...] = i_ref[...]
    l_out[...] = l_ref[...]


def solution(mesh):
    def device_body(mask_blk, user_shard, item_shard, triples):
        users, block = mask_blk.shape
        assert users <= 2 * OFFSET and block <= 128 * 256
        emb = user_shard.shape[1]
        ush, seg = user_shard.shape[0], item_shard.shape[0]
        batch = triples.shape[0]
        tw = batch // 8
        dw = block // 32
        hbm = pl.BlockSpec(memory_space=pl.ANY)
        loss_shape = (batch // 128, 128)
        results = (
            jax.ShapeDtypeStruct((emb, ush), BF16),
            jax.ShapeDtypeStruct((emb, seg), BF16),
            jax.ShapeDtypeStruct(loss_shape, F32),
        )
        found = pl.pallas_call(
            kernel,
            out_shape=results,
            in_specs=[pl.BlockSpec(memory_space=pltpu.HBM)] * 4,
            out_specs=(hbm,) * 3,
            scratch_shapes=[
                pltpu.VMEM((users, block), BF16),
                pltpu.VMEM((SLOTS, users, block // CHUNKS), jnp.int32),
                pltpu.VMEM((32, dw), F32),
                pltpu.VMEM((4, 8, dw), BF16),
                pltpu.VMEM((ROWS, 4, 8, dw), BF16),
                pltpu.VMEM((32, dw), F32),
                pltpu.VMEM((users, 128), F32),
                pltpu.VMEM((8, 128), F32),
                pltpu.VMEM((COLS, 8, 128), F32),
                pltpu.VMEM((users, 128), F32),
                pltpu.VMEM((LAYERS, ROWS, emb, seg), F32),
                pltpu.VMEM((LAYERS, 4, emb, seg), F32),
                pltpu.VMEM((LAYERS, 4, emb // 2, seg), F32),
                pltpu.VMEM((LAYERS, 2, emb // 2, seg), F32),
                pltpu.VMEM((LAYERS, ROWS, emb, seg), BF16),
                pltpu.VMEM((LAYERS, COLS, emb, ush), BF16),
                pltpu.VMEM((users, 128), F32),
                pltpu.VMEM((LAYERS, COLS, emb, ush), F32),
                pltpu.VMEM((LAYERS, COLS, emb, ush), F32),
                pltpu.VMEM((emb, seg), F32),
                pltpu.VMEM((emb, ush), F32),
                pltpu.VMEM((seg // GROUP, emb, GROUP), BF16),
                pltpu.VMEM((8, emb, tw), F32),
                pltpu.VMEM((8, emb, tw), F32),
                pltpu.VMEM((ROWS, COLS, emb, ush), BF16),
                pltpu.VMEM(loss_shape, F32),
                pltpu.VMEM((COLS,) + loss_shape, F32),
                pltpu.VMEM(loss_shape, F32),
                pltpu.VMEM((ROWS,) + loss_shape, F32),
                pltpu.VMEM((3, batch), jnp.int32),
                pltpu.VMEM((emb, seg), BF16),
                pltpu.VMEM((3, 8, GROUP, tw), BF16),
                pltpu.SemaphoreType.DMA((SLOTS,)),
                pltpu.SemaphoreType.DMA((3,)),
                pltpu.SemaphoreType.DMA((N_SEM,)),
                pltpu.SemaphoreType.DMA((N_SEM,)),
            ],
            compiler_params=pltpu.CompilerParams(
                collective_id=0, has_side_effects=True, vmem_limit_bytes=56 * 1024 * 1024),
        )(mask_blk, user_shard.T, item_shard.T, triples.T)
        vmem = pl.BlockSpec(memory_space=pltpu.VMEM)
        out_u, out_i, loss = pl.pallas_call(
            write_out, out_shape=results, in_specs=[vmem] * 3, out_specs=(vmem,) * 3,
        )(*found)
        return out_u.T, out_i.T, loss.reshape(batch)

    return jax.shard_map(
        device_body,
        mesh=mesh,
        in_specs=(P("row", "col"), P(("row", "col"), None), P(("col", "row"), None), P()),
        out_specs=(P(("row", "col"), None), P(("col", "row"), None), P()),
        check_vma=False,
    )
```
